128 devices in a mesh: img: 4 (over z), row: 4 (over x_hi, core), col: 8 (over x_lo, y).
Axes of the slice: x: 4 (x_hi: 2, x_lo: 2; x = x_hi * 2 + x_lo), y: 4, z: 4, core: 2. Of those that a mesh axis runs over, the one named last changes fastest.
Arguments:
- edges: int32 [4, 2048, 4096], P('img', 'row', 'col'), parts along dimension 0, may hold values from 0 to 15, as said below
- labels: int32 [4, 2048, 4096], P('img', 'row', 'col'), parts along dimension 0, may hold values from 0 to 2, as said below
- prior: float32 [4, 2048, 4096], P('img', 'row', 'col'), parts along dimension 0, may hold values from 0.05 to 1
- data_weight: float32 [4, 2048, 4096], P('img', 'row', 'col'), parts along dimension 0, may hold values from 0.05 to 1
Outputs:
- labeling: float32 [4, 2048, 4096], P('img', 'row', 'col'), parts along dimension 0
- residual: float32 [4, 2048, 4096], P('img', 'row', 'col'), parts along dimension 0
The draws below stay inside these ranges and needn't reach their ends.
There are 4 independent parts, one for each index of `img`. The reference program is written for one: setup_inputs(seed, part) draws one part's arguments, and reference() takes and returns one part's arrays. A program takes and returns all parts, laid end to end along the dimension named above; each array names one. Nothing has to cross between parts.
Inputs may be any that keep to these rules, and one draw needn't show every extreme that they name: `edges`: bit 1 of a pixel's code marks an edge to the next column, bit 2 to the previous column, bit 4 to the next row, bit 8 to the previous row; both ends of an edge carry it, and no edge leaves the image. `labels`: 0 marks a pixel to be labeled, 1 a foreground seed, 2 a background seed.
All inputs are finite; a program needn't handle non-finite values.
Results may differ from the reference program's by a relative error of at most 0.0002.
Values sent between devices are 32-bit elements; how exact they have to be, the bound alone decides.
No kernel may reach another device: no remote copies, remote signals or barrier semaphores. Data moves between devices by JAX's collectives and lax.ppermute only.
A program may use at most 64 MiB of HBM per device.

```python
import math
import jax
import jax.numpy as jnp

IMGS = 1
ITERS = 8
H = 2048
W = 4096


def draw_edges(key, part):
    key_h = jax.random.fold_in(key, 11)
    key_v = jax.random.fold_in(key, 23)
    horiz = (jax.random.randint(key_h, (IMGS, H, W - 1), 0, 5) < 4).astype(jnp.int32)
    vert = (jax.random.randint(key_v, (IMGS, H - 1, W), 0, 5) < 4).astype(jnp.int32)
    right = jnp.pad(horiz, ((0, 0), (0, 0), (0, 1)))
    left = jnp.pad(horiz, ((0, 0), (0, 0), (1, 0)))
    down = jnp.pad(vert, ((0, 0), (0, 1), (0, 0)))
    upper = jnp.pad(vert, ((0, 0), (1, 0), (0, 0)))
    return right + 2 * left + 4 * down + 8 * upper


def draw_labels(key, part):
    value = jax.random.randint(jax.random.fold_in(key, 37), (IMGS, H, W), 0, 20)
    return jnp.where(value == 0, 1, jnp.where(value == 1, 2, 0)).astype(jnp.int32)


def steps_of(stream_key, extent, cuts, least, largest):
    loudness, own = 1.0, jax.random.fold_in(stream_key, 6)
    for dim, parts in cuts:
        heights = jnp.exp(jax.random.uniform(jax.random.fold_in(own, dim), (parts,), jnp.float32, least / len(cuts), largest / len(cuts)))
        loudness = loudness * jnp.repeat(heights, extent[dim] // parts).reshape([-1 if axis == dim else 1 for axis in range(len(extent))])
    return loudness


def setup_inputs(seed: int = 0, part: int = 0) -> dict:
    keys = jax.random.split(jax.random.key(seed), 5)
    own_keys = jax.random.split(jax.random.fold_in(keys[4], part), 5)
    edges = draw_edges(jax.random.fold_in(jax.random.fold_in(keys[4], part), 71), part)
    labels = draw_labels(jax.random.fold_in(jax.random.fold_in(keys[4], part), 71), part)
    prior = jnp.clip(0.05 + 0.95 * jax.random.uniform(own_keys[2], (IMGS, H, W), jnp.float32) ** steps_of(own_keys[2], (IMGS, H, W), ((1, 4), (2, 8)), -0.2, 0.2), 0.05, 1.0)
    data_weight = jnp.clip(jnp.exp(math.log(1.0) - 2.9957323 * jax.random.uniform(own_keys[3], (IMGS, H, W), jnp.float32) ** steps_of(own_keys[3], (IMGS, H, W), ((1, 4), (2, 8)), -0.2, 0.2)), 0.05, 1.0)
    return dict(edges=edges, labels=labels, prior=prior, data_weight=data_weight)


def neighbours(field, right, left, down, upper):
    padded = jnp.pad(field, ((0, 0), (1, 1), (1, 1)))
    return (right * padded[:, 1:-1, 2:] + left * padded[:, 1:-1, :-2]
            + down * padded[:, 2:, 1:-1] + upper * padded[:, :-2, 1:-1])


def reference(edges, labels, prior, data_weight):
    right = (edges % 2).astype(jnp.float32)
    left = ((edges // 2) % 2).astype(jnp.float32)
    down = ((edges // 4) % 2).astype(jnp.float32)
    upper = ((edges // 8) % 2).astype(jnp.float32)
    degree = right + left + down + upper
    free = (labels == 0).astype(jnp.float32)
    anchor = (labels == 1).astype(jnp.float32)
    diag_term = degree + data_weight

    def operate(field):
        return free * (diag_term * field - neighbours(field, right, left, down, upper))

    rhs = free * (data_weight * prior + neighbours(anchor, right, left, down, upper))
    solution = jnp.zeros_like(rhs)
    residual = rhs
    direction = rhs
    norm_now = jnp.sum(residual * residual, axis=(1, 2))
    for step in range(ITERS):
        image_v = operate(direction)
        alpha = norm_now / jnp.sum(direction * image_v, axis=(1, 2))
        solution = solution + alpha[:, None, None] * direction
        residual = residual - alpha[:, None, None] * image_v
        norm_next = jnp.sum(residual * residual, axis=(1, 2))
        direction = residual + (norm_next / norm_now)[:, None, None] * direction
        norm_now = norm_next
    return anchor + solution, residual
```

```python
import functools
import jax
import jax.numpy as jnp
from jax import lax
from jax.experimental import pallas as pl
from jax.experimental.pallas import tpu as pltpu
from jax.sharding import PartitionSpec as P

ITERS = 8
HALO = 8
LANES = 128
LOW, HIGH = 0.05, 7.5
CENTRE, RADIUS = (HIGH + LOW) / 2, (HIGH - LOW) / 2
AMPLIFICATION = 24.0
VMEM = pl.BlockSpec(memory_space=pltpu.VMEM)
ANY = pl.BlockSpec(memory_space=pl.ANY)


def with_halo(array, sides, width):
    edges = {}
    for axis, dim in sides:
        count, length = (lax.axis_size(axis), array.shape[dim])
        up = [(i, (i + 1) % count) for i in range(count - 1)]
        last = lax.slice_in_dim(array, length - width, length, axis=dim)
        first = lax.slice_in_dim(array, 0, width, axis=dim)
        edges[dim] = (
            lax.ppermute(last, axis, up),
            lax.ppermute(first, axis, [(b, a) for a, b in up]),
        )
    done = []
    for _, dim in sides:
        low, high = edges[dim]
        around = [(width, width) if d in done else (0, 0) for d in range(array.ndim)]
        array = jnp.concatenate([jnp.pad(low, around), array, jnp.pad(high, around)], axis=dim)
        done.append(dim)
    return array


def total(value, axis):
    count = lax.axis_size(axis)
    flat = value.reshape(1, 1, 1)
    every = lax.all_to_all(jnp.broadcast_to(flat, (count, 1, 1)), axis, 0, 0, tiled=True)
    return every.sum()


def neighbours(field, right, left, down, upper):
    padded = with_halo(field, (("row", 1), ("col", 2)), 1)
    return (
        right * padded[:, 1:-1, 2:]
        + left * padded[:, 1:-1, :-2]
        + down * padded[:, 2:, 1:-1]
        + upper * padded[:, :-2, 1:-1]
    )


def plain(edges, labels, prior, data_weight):
    right = (edges % 2).astype(jnp.float32)
    left = (edges // 2 % 2).astype(jnp.float32)
    down = (edges // 4 % 2).astype(jnp.float32)
    upper = (edges // 8 % 2).astype(jnp.float32)
    degree = right + left + down + upper
    free = (labels == 0).astype(jnp.float32)
    anchor = (labels == 1).astype(jnp.float32)
    diag_term = degree + data_weight

    def nearby(field):
        return neighbours(field, right, left, down, upper)

    rhs = free * (data_weight * prior + nearby(anchor))

    def step(_, carry):
        result, residual, direction, norm_now = carry
        image_v = free * (diag_term * direction - nearby(direction))
        alpha = norm_now / total(jnp.sum(direction * image_v), ("row", "col"))
        result = result + alpha * direction
        residual = residual - alpha * image_v
        norm_next = total(jnp.sum(residual * residual), ("row", "col"))
        direction = residual + (norm_next / norm_now) * direction
        return result, residual, direction, norm_next

    start = (jnp.zeros_like(rhs), rhs, rhs, total(jnp.sum(rhs * rhs), ("row", "col")))
    result, residual, _, _ = lax.fori_loop(0, ITERS, step, start)
    return anchor + result, residual


def lane_ids(rows):
    return lax.broadcasted_iota(jnp.int32, (rows, LANES), 1)


def col_pack(*refs):
    first, last, to_left, to_right = refs[:4], refs[4:8], refs[8], refs[9]
    rows = first[0].shape[1]
    width = HALO + 1
    lane = lane_ids(rows)
    for side, out, base in ((first, to_left, 0), (last, to_right, LANES - width)):
        packed = None
        for a, ref in enumerate(side):
            x = ref[0].astype(jnp.float32)
            x = pltpu.roll(x, (a * width - base) % LANES, 1) if (a * width - base) % LANES else x
            packed = x if packed is None else jnp.where(lane < a * width, packed, x)
        out[...] = jnp.swapaxes(packed, 0, 1)[: out.shape[0]]


def side_tiles(from_right, from_left, rows_at, count):
    width = HALO + 1
    pad = jnp.zeros((LANES - from_right.shape[0], count), jnp.float32)
    r = jnp.swapaxes(jnp.concatenate([from_right[:, pl.ds(rows_at, count)], pad], 0), 0, 1)
    l = jnp.swapaxes(jnp.concatenate([from_left[:, pl.ds(rows_at, count)], pad], 0), 0, 1)
    lane = lane_ids(count)
    tiles = []
    for a in range(4):
        right = pltpu.roll(r, (-a * width) % LANES, 1) if a else r
        left = pltpu.roll(l, (LANES - width - a * width) % LANES, 1)
        outside = 2.0 if a == 1 else 0.0
        x = jnp.where(lane < width, right, jnp.where(lane >= LANES - width, left, outside))
        tiles.append(x)
    return tiles


def row_pack(*refs):
    top, bottom = refs[:4], refs[4:8]
    from_right, from_left, to_upper, to_lower = refs[8:]
    rows = from_right.shape[1]
    inner = top[0].shape[2]
    for side, out, at, narrow in (
        (top, to_upper, 0, 0),
        (bottom, to_lower, rows - LANES, HALO),
    ):
        tiles = side_tiles(from_right, from_left, at, LANES)
        shift = 0 if at == 0 else LANES - 2 * HALO
        for a, row, lo, n in ((0, 0, narrow, 8), (2, 8, narrow, 8), (3, 16, narrow, 8), (1, 24, 0, 16)):
            out[row : row + n, :inner] = side[a][0, lo : lo + n, :].astype(jnp.float32)
            out[row : row + n, inner:] = tiles[a][shift + lo : shift + lo + n]


def shifted(tiles, lane, by):
    count = len(tiles)
    turned = [pltpu.roll(t, by % LANES, 1) for t in tiles]
    if by > 0:
        return [jnp.where(lane == 0, turned[j - 1], turned[j]) for j in range(count)]
    return [jnp.where(lane == LANES - 1, turned[(j + 1) % count], turned[j]) for j in range(count)]


def basis(
    edges, labels, prior, weight, from_right, from_left, from_lower, from_upper,
    field, sums, code_s, lab_s, prior_s, weight_s, er_s, ed_s, eu_s, diag_s, sem,
):
    rows, cols = edges.shape[1], edges.shape[2]
    inner = cols // LANES
    tiles = inner + 1
    top = 2 * HALO
    copies = []
    for a, (src, dst) in enumerate(((edges, code_s), (labels, lab_s), (prior, prior_s), (weight, weight_s))):
        for j in range(inner):
            copy = pltpu.make_async_copy(
                src.at[0, :, pl.ds(j * LANES, LANES)],
                dst.at[j, pl.ds(top, rows), :],
                sem.at[a * inner + j],
            )
            copy.start()
            copies.append(copy)
    order = (code_s, lab_s, prior_s, weight_s)
    for at in range(0, rows, LANES):
        side = side_tiles(from_right, from_left, at, LANES)
        for a, dst in enumerate(order):
            dst[inner, top + at : top + at + LANES, :] = side[a].astype(dst.dtype)
    for a, row, n in ((0, 0, 8), (2, 8, 8), (3, 16, 8), (1, 24, 16)):
        dst = order[a]
        for j in range(tiles):
            lanes = slice(j * LANES, (j + 1) * LANES)
            dst[j, top - n : top, :] = from_upper[row : row + n, lanes].astype(dst.dtype)
            dst[j, top + rows : top + rows + n, :] = from_lower[row : row + n, lanes].astype(dst.dtype)
    zero = jnp.zeros((HALO, LANES), jnp.float32)
    for k in range(ITERS):
        for j in range(tiles):
            field[k, j, 0:HALO, :] = zero
            field[k, j, top + rows + HALO : top + rows + 2 * HALO, :] = zero
    for copy in copies:
        copy.wait()

    lane = lane_ids(8)
    scale = 2.0 / RADIUS

    def decode(i, _):
        s = pl.multiple_of(HALO + 8 * i, 8)
        here = pl.ds(s, 8)
        lab = [lab_s[j, here, :] for j in range(tiles)]
        lab_r = shifted(lab, lane, -1)
        lab_l = shifted(lab, lane, 1)
        for j in range(tiles):
            code = code_s[j, here, :]
            r = (code & 1).astype(jnp.float32)
            l = ((code >> 1) & 1).astype(jnp.float32)
            d = ((code >> 2) & 1).astype(jnp.float32)
            u = ((code >> 3) & 1).astype(jnp.float32)
            lab_d = lab_s[j, pl.ds(s + 1, 8), :]
            lab_u = lab_s[j, pl.ds(s - 1, 8), :]
            w = weight_s[j, here, :]
            free = lab[j] == 0
            one = jnp.where(free, scale, 0.0)
            er_s[j, here, :] = jnp.where(lab_r[j] == 0, one, 0.0) * r
            ed_s[j, here, :] = one * d
            eu_s[j, here, :] = one * u
            diag_s[j, here, :] = scale * ((r + l + d + u) + w - CENTRE)
            near = (
                jnp.where(lab_r[j] == 1, r, 0.0)
                + jnp.where(lab_l[j] == 1, l, 0.0)
                + jnp.where(lab_d == 1, d, 0.0)
                + jnp.where(lab_u == 1, u, 0.0)
            )
            rhs = jnp.where(free, w * prior_s[j, here, :] + near, 0.0)
            field[0, j, here, :] = rhs
        return 0

    lax.fori_loop(0, (rows + 2 * HALO) // 8, decode, 0)

    def advance(k, s):
        here = pl.ds(s, 8)
        v = [field[k, j, here, :] for j in range(tiles)]
        er = [er_s[j, here, :] for j in range(tiles)]
        v_r = shifted(v, lane, -1)
        g = shifted([er[j] * v[j] for j in range(tiles)], lane, 1)
        new = []
        for j in range(tiles):
            x = diag_s[j, here, :] * v[j] - (er[j] * v_r[j] + g[j])
            x = x - (
                ed_s[j, here, :] * field[k, j, pl.ds(s + 1, 8), :]
                + eu_s[j, here, :] * field[k, j, pl.ds(s - 1, 8), :]
            )
            x = 0.5 * x if k == 0 else x - field[k - 1, j, here, :]
            field[k + 1, j, here, :] = x
            new.append(x)
        return v, new

    parts = []
    for k in range(ITERS):
        last = k == ITERS - 1

        def body(i, carry, k=k, last=last):
            s = pl.multiple_of(top + 8 * i, 8)
            v, new = advance(k, s)
            pairs = [(v, v), (v, new)] + ([(new, new)] if last else [])
            out = []
            for acc, (a, b) in zip(carry, pairs):
                t = [a[j] * b[j] for j in range(inner)]
                while len(t) > 1:
                    t = [t[q] + t[q + 1] for q in range(0, len(t) - 1, 2)] + ([t[-1]] if len(t) % 2 else [])
                out.append(acc + t[0])
            return tuple(out)

        if not last:
            advance(k, HALO)
            advance(k, top + rows)
        acc = tuple(jnp.zeros((8, LANES), jnp.float32) for _ in range(3 if last else 2))
        parts.extend(lax.fori_loop(0, rows // 8, body, acc))

    out = jnp.zeros((1, LANES), jnp.float32)
    for n, acc in enumerate(parts):
        one = jnp.sum(jnp.sum(acc, axis=0, keepdims=True), axis=1, keepdims=True)
        out = jnp.where(lane_ids(1) == n, one, out)
    sums[...] = jnp.broadcast_to(out[None], sums.shape)


def coefficients(dots):
    n = ITERS
    inv = 1.0 / dots[0]
    moment = [jnp.ones_like(dots[0]), dots[1] * inv]
    for k in range(1, n + 1):
        moment.append(2.0 * (dots[2 * k] * inv) - moment[0])
        if k < n:
            moment.append(2.0 * (dots[2 * k + 1] * inv) - moment[1])
    gram = [[0.5 * (moment[i + j] + moment[abs(i - j)]) for j in range(n + 1)] for i in range(n + 1)]

    def image(p):
        q = [CENTRE * x for x in p] + [jnp.zeros_like(p[0])]
        for i, x in enumerate(p):
            if i == 0:
                q[1] = q[1] + RADIUS * x
            else:
                q[i + 1] = q[i + 1] + (RADIUS / 2) * x
                q[i - 1] = q[i - 1] + (RADIUS / 2) * x
        return q

    def product(a, b):
        sums = None
        for i, x in enumerate(a):
            t = gram[i][0] * b[0]
            for j in range(1, len(b)):
                t = t + gram[i][j] * b[j]
            sums = x * t if sums is None else sums + x * t
        return sums

    zero = jnp.zeros_like(inv)
    x, r, p = [], [moment[0]], [moment[0]]
    now = moment[0]
    for _ in range(n):
        q = image(p)
        alpha = now / product(p, q)
        x = [(x[i] if i < len(x) else zero) + alpha * p[i] for i in range(len(p))]
        r = [(r[i] if i < len(r) else zero) - alpha * q[i] for i in range(len(q))]
        following = product(r, r)
        beta = following / now
        p = [r[i] + (beta * p[i] if i < len(p) else zero) for i in range(len(r))]
        now = following
    size = zero
    for i in range(n + 1):
        size = size + jnp.abs(r[i]) * jnp.sqrt(jnp.maximum(gram[i][i], 0.0))
    good = (size * size <= (AMPLIFICATION * AMPLIFICATION) * now) & (now > 0.0)
    return x, r, good


def combine(every, labels, field, labeling, residual, flag):
    rows, cols = labels.shape[1], labels.shape[2]
    inner = cols // LANES
    top = 2 * HALO
    g = jnp.sum(every[:, 0, :], axis=0, keepdims=True)
    dots = [jnp.broadcast_to(g[:, n : n + 1], (8, LANES)) for n in range(2 * ITERS + 1)]
    x, r, good = coefficients(dots)
    flag[...] = good.astype(jnp.int32)

    def body(i, _):
        s = pl.multiple_of(8 * i, 8)
        for j in range(inner):
            lanes = slice(j * LANES, (j + 1) * LANES)
            sol = jnp.where(labels[0, pl.ds(s, 8), lanes] == 1, 1.0, 0.0)
            res = None
            for k in range(ITERS + 1):
                t = field[k, j, pl.ds(s + top, 8), :]
                res = r[k] * t if res is None else res + r[k] * t
                if k < ITERS:
                    sol = sol + x[k] * t
            labeling[0, pl.ds(s, 8), lanes] = sol
            residual[0, pl.ds(s, 8), lanes] = res
        return 0

    lax.fori_loop(0, rows // 8, body, 0)


def fixed(shape, at):
    return pl.BlockSpec(shape, lambda *_: at)


def per_device(edges, labels, prior, data_weight):
    arrays = (edges, labels, prior, data_weight)
    _, rows, cols = edges.shape
    f32 = jnp.float32
    tiles = cols // LANES + 1
    deep = rows + 4 * HALO

    to_left, to_right = pl.pallas_call(
        col_pack,
        grid=(1,),
        in_specs=[fixed((1, rows, LANES), (0, 0, 0))] * 4
        + [fixed((1, rows, LANES), (0, 0, cols // LANES - 1))] * 4,
        out_specs=[fixed((40, rows), (0, 0))] * 2,
        out_shape=[jax.ShapeDtypeStruct((40, rows), f32)] * 2,
    )(*arrays, *arrays)
    count = lax.axis_size("col")
    up = [(i, i + 1) for i in range(count - 1)]
    back = [(b, a) for a, b in up]
    from_right = lax.ppermute(to_left, "col", back)
    from_left = lax.ppermute(to_right, "col", up)

    to_upper, to_lower = pl.pallas_call(
        row_pack,
        grid=(1,),
        in_specs=[fixed((1, 2 * HALO, cols), (0, 0, 0))] * 4
        + [fixed((1, 2 * HALO, cols), (0, rows // (2 * HALO) - 1, 0))] * 4
        + [fixed((40, rows), (0, 0))] * 2,
        out_specs=[fixed((40, tiles * LANES), (0, 0))] * 2,
        out_shape=[jax.ShapeDtypeStruct((40, tiles * LANES), f32)] * 2,
    )(*arrays, *arrays, from_right, from_left)
    count = lax.axis_size("row")
    up = [(i, i + 1) for i in range(count - 1)]
    back = [(b, a) for a, b in up]
    from_lower = lax.ppermute(to_upper, "row", back)
    from_upper = lax.ppermute(to_lower, "row", up)

    group = lax.axis_size(("row", "col"))
    grid_s = lambda dtype: pltpu.VMEM((tiles, deep, LANES), dtype)
    field, sums = pl.pallas_call(
        basis,
        in_specs=[ANY] * 4 + [VMEM] * 4,
        out_specs=[VMEM, VMEM],
        out_shape=[
            jax.ShapeDtypeStruct((ITERS + 1, tiles, deep, LANES), f32),
            jax.ShapeDtypeStruct((group, 1, LANES), f32),
        ],
        scratch_shapes=[grid_s(jnp.int32), grid_s(jnp.int32)]
        + [grid_s(f32)] * 6
        + [pltpu.SemaphoreType.DMA((4 * (tiles - 1),))],
        compiler_params=pltpu.CompilerParams(vmem_limit_bytes=32 * 1024 * 1024),
    )(*arrays, from_right, from_left, from_lower, from_upper)

    every = lax.all_to_all(sums, ("row", "col"), 0, 0, tiled=True)

    labeling, residual, flag = pl.pallas_call(
        combine,
        in_specs=[VMEM] * 3,
        out_specs=[VMEM] * 3,
        out_shape=[jax.ShapeDtypeStruct(edges.shape, f32)] * 2
        + [jax.ShapeDtypeStruct((8, LANES), jnp.int32)],
        compiler_params=pltpu.CompilerParams(vmem_limit_bytes=32 * 1024 * 1024),
    )(every, labels, field)

    def again(carry):
        return (jnp.int32(1), *plain(edges, labels, prior, data_weight))

    _, labeling, residual = lax.while_loop(
        lambda carry: carry[0] == 0, again, (flag[0, 0], labeling, residual)
    )
    return labeling, residual


def solution(mesh):
    spec = P("img", "row", "col")
    return jax.shard_map(
        per_device, mesh=mesh, in_specs=(spec,) * 4, out_specs=(spec,) * 2, check_vma=False
    )
```

```python
import functools
import jax
import jax.numpy as jnp
from jax import lax
from jax.experimental import pallas as pl
from jax.experimental.pallas import tpu as pltpu
from jax.sharding import PartitionSpec as P

ITERS = 8
HALO = 8
LANES = 128
LOW, HIGH = 0.05, 7.5
CENTRE, RADIUS = (HIGH + LOW) / 2, (HIGH - LOW) / 2
AMPLIFICATION = 24.0
VMEM = pl.BlockSpec(memory_space=pltpu.VMEM)
ANY = pl.BlockSpec(memory_space=pl.ANY)


def with_halo(array, sides, width):
    edges = {}
    for axis, dim in sides:
        count, length = (lax.axis_size(axis), array.shape[dim])
        up = [(i, (i + 1) % count) for i in range(count - 1)]
        last = lax.slice_in_dim(array, length - width, length, axis=dim)
        first = lax.slice_in_dim(array, 0, width, axis=dim)
        edges[dim] = (
            lax.ppermute(last, axis, up),
            lax.ppermute(first, axis, [(b, a) for a, b in up]),
        )
    done = []
    for _, dim in sides:
        low, high = edges[dim]
        around = [(width, width) if d in done else (0, 0) for d in range(array.ndim)]
        array = jnp.concatenate([jnp.pad(low, around), array, jnp.pad(high, around)], axis=dim)
        done.append(dim)
    return array


def total(value, axis):
    count = lax.axis_size(axis)
    flat = value.reshape(1, 1, 1)
    every = lax.all_to_all(jnp.broadcast_to(flat, (count, 1, 1)), axis, 0, 0, tiled=True)
    return every.sum()


def neighbours(field, right, left, down, upper):
    padded = with_halo(field, (("row", 1), ("col", 2)), 1)
    return (
        right * padded[:, 1:-1, 2:]
        + left * padded[:, 1:-1, :-2]
        + down * padded[:, 2:, 1:-1]
        + upper * padded[:, :-2, 1:-1]
    )


def plain(edges, labels, prior, data_weight):
    right = (edges % 2).astype(jnp.float32)
    left = (edges // 2 % 2).astype(jnp.float32)
    down = (edges // 4 % 2).astype(jnp.float32)
    upper = (edges // 8 % 2).astype(jnp.float32)
    degree = right + left + down + upper
    free = (labels == 0).astype(jnp.float32)
    anchor = (labels == 1).astype(jnp.float32)
    diag_term = degree + data_weight

    def nearby(field):
        return neighbours(field, right, left, down, upper)

    rhs = free * (data_weight * prior + nearby(anchor))

    def step(_, carry):
        result, residual, direction, norm_now = carry
        image_v = free * (diag_term * direction - nearby(direction))
        alpha = norm_now / total(jnp.sum(direction * image_v), ("row", "col"))
        result = result + alpha * direction
        residual = residual - alpha * image_v
        norm_next = total(jnp.sum(residual * residual), ("row", "col"))
        direction = residual + (norm_next / norm_now) * direction
        return result, residual, direction, norm_next

    start = (jnp.zeros_like(rhs), rhs, rhs, total(jnp.sum(rhs * rhs), ("row", "col")))
    result, residual, _, _ = lax.fori_loop(0, ITERS, step, start)
    return anchor + result, residual


def lane_ids(rows):
    return lax.broadcasted_iota(jnp.int32, (rows, LANES), 1)


def col_pack(*refs):
    first, last, to_left, to_right = refs[:4], refs[4:8], refs[8], refs[9]
    rows = first[0].shape[1]
    width = HALO + 1
    lane = lane_ids(rows)
    for side, out, base in ((first, to_left, 0), (last, to_right, LANES - width)):
        packed = None
        for a, ref in enumerate(side):
            x = ref[0].astype(jnp.float32)
            x = pltpu.roll(x, (a * width - base) % LANES, 1) if (a * width - base) % LANES else x
            packed = x if packed is None else jnp.where(lane < a * width, packed, x)
        out[...] = jnp.swapaxes(packed, 0, 1)[: out.shape[0]]


def side_tiles(from_right, from_left, rows_at, count):
    width = HALO + 1
    pad = jnp.zeros((LANES - from_right.shape[0], count), jnp.float32)
    r = jnp.swapaxes(jnp.concatenate([from_right[:, pl.ds(rows_at, count)], pad], 0), 0, 1)
    l = jnp.swapaxes(jnp.concatenate([from_left[:, pl.ds(rows_at, count)], pad], 0), 0, 1)
    lane = lane_ids(count)
    tiles = []
    for a in range(4):
        right = pltpu.roll(r, (-a * width) % LANES, 1) if a else r
        left = pltpu.roll(l, (LANES - width - a * width) % LANES, 1)
        outside = 2.0 if a == 1 else 0.0
        x = jnp.where(lane < width, right, jnp.where(lane >= LANES - width, left, outside))
        tiles.append(x)
    return tiles


def row_pack(*refs):
    top, bottom = refs[:4], refs[4:8]
    from_right, from_left, to_upper, to_lower = refs[8:]
    rows = from_right.shape[1]
    inner = top[0].shape[2]
    for side, out, at, narrow in (
        (top, to_upper, 0, 0),
        (bottom, to_lower, rows - LANES, HALO),
    ):
        tiles = side_tiles(from_right, from_left, at, LANES)
        shift = 0 if at == 0 else LANES - 2 * HALO
        for a, row, lo, n in ((0, 0, narrow, 8), (2, 8, narrow, 8), (3, 16, narrow, 8), (1, 24, 0, 16)):
            out[row : row + n, :inner] = side[a][0, lo : lo + n, :].astype(jnp.float32)
            out[row : row + n, inner:] = tiles[a][shift + lo : shift + lo + n]


def shifted(tiles, lane, by):
    count = len(tiles)
    turned = [pltpu.roll(t, by % LANES, 1) for t in tiles]
    if by > 0:
        return [jnp.where(lane == 0, turned[j - 1], turned[j]) for j in range(count)]
    return [jnp.where(lane == LANES - 1, turned[(j + 1) % count], turned[j]) for j in range(count)]


def basis(
    edges, labels, prior, weight, from_right, from_left, from_lower, from_upper,
    *refs,
):
    field, sums = refs[: ITERS + 1], refs[ITERS + 1]
    code_s, lab_s, prior_s, weight_s, er_s, ed_s, eu_s, diag_s, sem = refs[ITERS + 2 :]
    rows, cols = edges.shape[1], edges.shape[2]
    inner = cols // LANES
    tiles = inner + 1
    top = 2 * HALO
    copies = []
    for a, (src, dst) in enumerate(((edges, code_s), (labels, lab_s), (prior, prior_s), (weight, weight_s))):
        for j in range(inner):
            copy = pltpu.make_async_copy(
                src.at[0, :, pl.ds(j * LANES, LANES)],
                dst.at[j, pl.ds(top, rows), :],
                sem.at[a * inner + j],
            )
            copy.start()
            copies.append(copy)
    order = (code_s, lab_s, prior_s, weight_s)
    for at in range(0, rows, LANES):
        side = side_tiles(from_right, from_left, at, LANES)
        for a, dst in enumerate(order):
            dst[inner, top + at : top + at + LANES, :] = side[a].astype(dst.dtype)
    for a, row, n in ((0, 0, 8), (2, 8, 8), (3, 16, 8), (1, 24, 16)):
        dst = order[a]
        for j in range(tiles):
            lanes = slice(j * LANES, (j + 1) * LANES)
            dst[j, top - n : top, :] = from_upper[row : row + n, lanes].astype(dst.dtype)
            dst[j, top + rows : top + rows + n, :] = from_lower[row : row + n, lanes].astype(dst.dtype)
    zero = jnp.zeros((HALO, LANES), jnp.float32)
    for k in range(ITERS):
        for j in range(tiles):
            field[k][j, 0:HALO, :] = zero
            field[k][j, top + rows + HALO : top + rows + 2 * HALO, :] = zero
    for copy in copies:
        copy.wait()

    lane = lane_ids(8)
    scale = 2.0 / RADIUS

    def decode(i, _):
        s = pl.multiple_of(HALO + 8 * i, 8)
        here = pl.ds(s, 8)
        lab = [lab_s[j, here, :] for j in range(tiles)]
        lab_r = shifted(lab, lane, -1)
        lab_l = shifted(lab, lane, 1)
        for j in range(tiles):
            code = code_s[j, here, :]
            r = (code & 1).astype(jnp.float32)
            l = ((code >> 1) & 1).astype(jnp.float32)
            d = ((code >> 2) & 1).astype(jnp.float32)
            u = ((code >> 3) & 1).astype(jnp.float32)
            lab_d = lab_s[j, pl.ds(s + 1, 8), :]
            lab_u = lab_s[j, pl.ds(s - 1, 8), :]
            w = weight_s[j, here, :]
            free = lab[j] == 0
            one = jnp.where(free, scale, 0.0)
            er_s[j, here, :] = jnp.where(lab_r[j] == 0, one, 0.0) * r
            ed_s[j, here, :] = one * d
            eu_s[j, here, :] = one * u
            diag_s[j, here, :] = scale * ((r + l + d + u) + w - CENTRE)
            near = (
                jnp.where(lab_r[j] == 1, r, 0.0)
                + jnp.where(lab_l[j] == 1, l, 0.0)
                + jnp.where(lab_d == 1, d, 0.0)
                + jnp.where(lab_u == 1, u, 0.0)
            )
            rhs = jnp.where(free, w * prior_s[j, here, :] + near, 0.0)
            field[0][j, here, :] = rhs
        return 0

    lax.fori_loop(0, (rows + 2 * HALO) // 8, decode, 0, unroll=6)

    def advance(k, s):
        here = pl.ds(s, 8)
        v = [field[k][j, here, :] for j in range(tiles)]
        er = [er_s[j, here, :] for j in range(tiles)]
        v_r = shifted(v, lane, -1)
        g = shifted([er[j] * v[j] for j in range(tiles)], lane, 1)
        new = []
        for j in range(tiles):
            x = diag_s[j, here, :] * v[j] - (er[j] * v_r[j] + g[j])
            x = x - (
                ed_s[j, here, :] * field[k][j, pl.ds(s + 1, 8), :]
                + eu_s[j, here, :] * field[k][j, pl.ds(s - 1, 8), :]
            )
            x = 0.5 * x if k == 0 else x - field[k - 1][j, here, :]
            field[k + 1][j, here, :] = x
            new.append(x)
        return v, new

    parts = []
    for k in range(ITERS):
        last = k == ITERS - 1

        def body(i, carry, k=k, last=last):
            s = pl.multiple_of(top + 8 * i, 8)
            v, new = advance(k, s)
            pairs = [(v, v), (v, new)] + ([(new, new)] if last else [])
            out = []
            for acc, (a, b) in zip(carry, pairs):
                t = [a[j] * b[j] for j in range(inner)]
                while len(t) > 1:
                    t = [t[q] + t[q + 1] for q in range(0, len(t) - 1, 2)] + ([t[-1]] if len(t) % 2 else [])
                out.append(acc + t[0])
            return tuple(out)

        if not last:
            advance(k, HALO)
            advance(k, top + rows)
        acc = tuple(jnp.zeros((8, LANES), jnp.float32) for _ in range(3 if last else 2))
        parts.extend(lax.fori_loop(0, rows // 8, body, acc, unroll=16))

    out = jnp.zeros((1, LANES), jnp.float32)
    for n, acc in enumerate(parts):
        one = jnp.sum(jnp.sum(acc, axis=0, keepdims=True), axis=1, keepdims=True)
        out = jnp.where(lane_ids(1) == n, one, out)
    sums[...] = jnp.broadcast_to(out[None], sums.shape)


def coefficients(dots):
    n = ITERS
    inv = 1.0 / dots[0]
    moment = [jnp.ones_like(dots[0]), dots[1] * inv]
    for k in range(1, n + 1):
        moment.append(2.0 * (dots[2 * k] * inv) - moment[0])
        if k < n:
            moment.append(2.0 * (dots[2 * k + 1] * inv) - moment[1])
    gram = [[0.5 * (moment[i + j] + moment[abs(i - j)]) for j in range(n + 1)] for i in range(n + 1)]

    def image(p):
        q = [CENTRE * x for x in p] + [jnp.zeros_like(p[0])]
        for i, x in enumerate(p):
            if i == 0:
                q[1] = q[1] + RADIUS * x
            else:
                q[i + 1] = q[i + 1] + (RADIUS / 2) * x
                q[i - 1] = q[i - 1] + (RADIUS / 2) * x
        return q

    def product(a, b):
        sums = None
        for i, x in enumerate(a):
            t = gram[i][0] * b[0]
            for j in range(1, len(b)):
                t = t + gram[i][j] * b[j]
            sums = x * t if sums is None else sums + x * t
        return sums

    zero = jnp.zeros_like(inv)
    x, r, p = [], [moment[0]], [moment[0]]
    now = moment[0]
    for _ in range(n):
        q = image(p)
        alpha = now / product(p, q)
        x = [(x[i] if i < len(x) else zero) + alpha * p[i] for i in range(len(p))]
        r = [(r[i] if i < len(r) else zero) - alpha * q[i] for i in range(len(q))]
        following = product(r, r)
        beta = following / now
        p = [r[i] + (beta * p[i] if i < len(p) else zero) for i in range(len(r))]
        now = following
    size = zero
    for i in range(n + 1):
        size = size + jnp.abs(r[i]) * jnp.sqrt(jnp.maximum(gram[i][i], 0.0))
    good = (size * size <= (AMPLIFICATION * AMPLIFICATION) * now) & (now > 0.0)
    return x, r, good


def combine(every, labels, *refs):
    field, (labeling, residual, flag) = refs[: ITERS + 1], refs[ITERS + 1 :]
    rows, cols = labels.shape[1], labels.shape[2]
    inner = cols // LANES
    top = 2 * HALO
    g = jnp.sum(every[:, 0, :], axis=0, keepdims=True)
    dots = [jnp.broadcast_to(g[:, n : n + 1], (8, LANES)) for n in range(2 * ITERS + 1)]
    x, r, good = coefficients(dots)
    flag[...] = good.astype(jnp.int32)

    def body(i, _):
        s = pl.multiple_of(8 * i, 8)
        for j in range(inner):
            lanes = slice(j * LANES, (j + 1) * LANES)
            sol = jnp.where(labels[0, pl.ds(s, 8), lanes] == 1, 1.0, 0.0)
            res = None
            for k in range(ITERS + 1):
                t = field[k][j, pl.ds(s + top, 8), :]
                res = r[k] * t if res is None else res + r[k] * t
                if k < ITERS:
                    sol = sol + x[k] * t
            labeling[0, pl.ds(s, 8), lanes] = sol
            residual[0, pl.ds(s, 8), lanes] = res
        return 0

    lax.fori_loop(0, rows // 8, body, 0, unroll=8)


def fixed(shape, at):
    return pl.BlockSpec(shape, lambda *_: at)


def per_device(edges, labels, prior, data_weight):
    arrays = (edges, labels, prior, data_weight)
    _, rows, cols = edges.shape
    f32 = jnp.float32
    tiles = cols // LANES + 1
    deep = rows + 4 * HALO

    to_left, to_right = pl.pallas_call(
        col_pack,
        grid=(1,),
        in_specs=[fixed((1, rows, LANES), (0, 0, 0))] * 4
        + [fixed((1, rows, LANES), (0, 0, cols // LANES - 1))] * 4,
        out_specs=[fixed((40, rows), (0, 0))] * 2,
        out_shape=[jax.ShapeDtypeStruct((40, rows), f32)] * 2,
    )(*arrays, *arrays)
    count = lax.axis_size("col")
    up = [(i, i + 1) for i in range(count - 1)]
    back = [(b, a) for a, b in up]
    from_right = lax.ppermute(to_left, "col", back)
    from_left = lax.ppermute(to_right, "col", up)

    to_upper, to_lower = pl.pallas_call(
        row_pack,
        grid=(1,),
        in_specs=[fixed((1, 2 * HALO, cols), (0, 0, 0))] * 4
        + [fixed((1, 2 * HALO, cols), (0, rows // (2 * HALO) - 1, 0))] * 4
        + [fixed((40, rows), (0, 0))] * 2,
        out_specs=[fixed((40, tiles * LANES), (0, 0))] * 2,
        out_shape=[jax.ShapeDtypeStruct((40, tiles * LANES), f32)] * 2,
    )(*arrays, *arrays, from_right, from_left)
    count = lax.axis_size("row")
    up = [(i, i + 1) for i in range(count - 1)]
    back = [(b, a) for a, b in up]
    from_lower = lax.ppermute(to_upper, "row", back)
    from_upper = lax.ppermute(to_lower, "row", up)

    group = lax.axis_size(("row", "col"))
    grid_s = lambda dtype: pltpu.VMEM((tiles, deep, LANES), dtype)
    *field, sums = pl.pallas_call(
        basis,
        in_specs=[ANY] * 4 + [VMEM] * 4,
        out_specs=[VMEM] * (ITERS + 2),
        out_shape=[jax.ShapeDtypeStruct((tiles, deep, LANES), f32)] * (ITERS + 1)
        + [jax.ShapeDtypeStruct((group, 1, LANES), f32)],
        scratch_shapes=[grid_s(jnp.int32), grid_s(jnp.int32)]
        + [grid_s(f32)] * 6
        + [pltpu.SemaphoreType.DMA((4 * (tiles - 1),))],
        compiler_params=pltpu.CompilerParams(vmem_limit_bytes=32 * 1024 * 1024),
    )(*arrays, from_right, from_left, from_lower, from_upper)

    every = lax.all_to_all(sums, ("row", "col"), 0, 0, tiled=True)

    labeling, residual, flag = pl.pallas_call(
        combine,
        in_specs=[VMEM] * (ITERS + 3),
        out_specs=[VMEM] * 3,
        out_shape=[jax.ShapeDtypeStruct(edges.shape, f32)] * 2
        + [jax.ShapeDtypeStruct((8, LANES), jnp.int32)],
        compiler_params=pltpu.CompilerParams(vmem_limit_bytes=32 * 1024 * 1024),
    )(every, labels, *field)

    def again(carry):
        return (jnp.int32(1), *plain(edges, labels, prior, data_weight))

    _, labeling, residual = lax.while_loop(
        lambda carry: carry[0] == 0, again, (flag[0, 0], labeling, residual)
    )
    return labeling, residual


def solution(mesh):
    spec = P("img", "row", "col")
    return jax.shard_map(
        per_device, mesh=mesh, in_specs=(spec,) * 4, out_specs=(spec,) * 2, check_vma=False
    )
```

```python
import functools
import jax
import jax.numpy as jnp
from jax import lax
from jax.experimental import pallas as pl
from jax.experimental.pallas import tpu as pltpu
from jax.sharding import PartitionSpec as P

ITERS = 8
HALO = 8
LANES = 128
LOW, HIGH = 0.05, 7.5
CENTRE, RADIUS = (HIGH + LOW) / 2, (HIGH - LOW) / 2
AMPLIFICATION = 24.0
VMEM = pl.BlockSpec(memory_space=pltpu.VMEM)
ANY = pl.BlockSpec(memory_space=pl.ANY)


def with_halo(array, sides, width):
    edges = {}
    for axis, dim in sides:
        count, length = (lax.axis_size(axis), array.shape[dim])
        up = [(i, (i + 1) % count) for i in range(count - 1)]
        last = lax.slice_in_dim(array, length - width, length, axis=dim)
        first = lax.slice_in_dim(array, 0, width, axis=dim)
        edges[dim] = (
            lax.ppermute(last, axis, up),
            lax.ppermute(first, axis, [(b, a) for a, b in up]),
        )
    done = []
    for _, dim in sides:
        low, high = edges[dim]
        around = [(width, width) if d in done else (0, 0) for d in range(array.ndim)]
        array = jnp.concatenate([jnp.pad(low, around), array, jnp.pad(high, around)], axis=dim)
        done.append(dim)
    return array


def total(value, axis):
    count = lax.axis_size(axis)
    flat = value.reshape(1, 1, 1)
    every = lax.all_to_all(jnp.broadcast_to(flat, (count, 1, 1)), axis, 0, 0, tiled=True)
    return every.sum()


def neighbours(field, right, left, down, upper):
    padded = with_halo(field, (("row", 1), ("col", 2)), 1)
    return (
        right * padded[:, 1:-1, 2:]
        + left * padded[:, 1:-1, :-2]
        + down * padded[:, 2:, 1:-1]
        + upper * padded[:, :-2, 1:-1]
    )


def plain(edges, labels, prior, data_weight):
    right = (edges % 2).astype(jnp.float32)
    left = (edges // 2 % 2).astype(jnp.float32)
    down = (edges // 4 % 2).astype(jnp.float32)
    upper = (edges // 8 % 2).astype(jnp.float32)
    degree = right + left + down + upper
    free = (labels == 0).astype(jnp.float32)
    anchor = (labels == 1).astype(jnp.float32)
    diag_term = degree + data_weight

    def nearby(field):
        return neighbours(field, right, left, down, upper)

    rhs = free * (data_weight * prior + nearby(anchor))

    def step(_, carry):
        result, residual, direction, norm_now = carry
        image_v = free * (diag_term * direction - nearby(direction))
        alpha = norm_now / total(jnp.sum(direction * image_v), ("row", "col"))
        result = result + alpha * direction
        residual = residual - alpha * image_v
        norm_next = total(jnp.sum(residual * residual), ("row", "col"))
        direction = residual + (norm_next / norm_now) * direction
        return result, residual, direction, norm_next

    start = (jnp.zeros_like(rhs), rhs, rhs, total(jnp.sum(rhs * rhs), ("row", "col")))
    result, residual, _, _ = lax.fori_loop(0, ITERS, step, start)
    return anchor + result, residual


WIDTH = HALO + 1
LINES = 40
TOP_OF = ((0, 0, 8), (2, 8, 8), (3, 16, 8), (1, 24, 16))


def lane_ids(rows):
    return lax.broadcasted_iota(jnp.int32, (rows, LANES), 1)


def turn(x, by):
    return pltpu.roll(x, by % LANES, 1) if by % LANES else x


def col_pack(edges, labels, prior, weight, to_left, to_right, ints, floats, sem):
    arrays = (edges, labels, prior, weight)
    rows, cols = edges.shape[1], edges.shape[2]
    lane = lane_ids(LANES)

    def copy(side, a, chunk):
        at = pl.ds(chunk * LANES, LANES)
        dst = (ints if a < 2 else floats).at[side, a % 2, at, :]
        return pltpu.make_async_copy(
            arrays[a].at[0, at, pl.ds(side * (cols - LANES), LANES)], dst, sem.at[side, a, chunk]
        )

    chunks = rows // LANES
    for chunk in range(chunks):
        for side in range(2):
            for a in range(4):
                copy(side, a, chunk).start()
    for chunk in range(chunks):
        at = slice(chunk * LANES, (chunk + 1) * LANES)
        for side, out, base in ((0, to_left, 0), (1, to_right, LANES - WIDTH)):
            packed = None
            for a in range(4):
                copy(side, a, chunk).wait()
                x = (ints if a < 2 else floats)[side, a % 2, at, :].astype(jnp.float32)
                x = turn(x, a * WIDTH - base)
                packed = x if packed is None else jnp.where(lane < a * WIDTH, packed, x)
            out[:, at] = jnp.swapaxes(packed, 0, 1)[:LINES]


def load(edges, labels, prior, weight, code_t, lab_t, prior_t, weight_t, sem):
    rows = edges.shape[1]
    tiles = code_t.shape[0]
    copies = []
    for a, (src, dst, at) in enumerate(
        ((edges, code_t, 0), (labels, lab_t, HALO), (prior, prior_t, 0), (weight, weight_t, 0))
    ):
        for j in range(tiles):
            copies.append(
                pltpu.make_async_copy(
                    src.at[0, :, pl.ds(j * LANES, LANES)],
                    dst.at[j, pl.ds(at, rows), :],
                    sem.at[a, j],
                )
            )
    for copy in copies:
        copy.start()
    seeds = jnp.full((HALO, LANES), 2, jnp.int32)
    for j in range(tiles):
        lab_t[j, :HALO, :] = seeds
        lab_t[j, HALO + rows :, :] = seeds
    for copy in copies:
        copy.wait()


def side_tiles(from_right, from_left, at):
    pad = jnp.zeros((LANES - LINES, LANES), jnp.float32)
    r = jnp.swapaxes(jnp.concatenate([from_right[:, at : at + LANES], pad], 0), 0, 1)
    l = jnp.swapaxes(jnp.concatenate([from_left[:, at : at + LANES], pad], 0), 0, 1)
    lane = lane_ids(LANES)
    tiles = []
    for a in range(4):
        right = turn(r, -a * WIDTH)
        left = turn(l, LANES - WIDTH - a * WIDTH)
        outside = 2.0 if a == 1 else 0.0
        tiles.append(jnp.where(lane < WIDTH, right, jnp.where(lane >= LANES - WIDTH, left, outside)))
    return tiles


def row_pack(code_t, lab_t, prior_t, weight_t, from_right, from_left, to_upper, to_lower):
    tiles, rows = code_t.shape[0], code_t.shape[1]
    refs = (code_t, lab_t, prior_t, weight_t)
    for out, at in ((to_upper, 0), (to_lower, rows - LANES)):
        side = side_tiles(from_right, from_left, at)
        for a, line, n in TOP_OF:
            first = 0 if at == 0 else rows - n
            skip = HALO if a == 1 else 0
            for j in range(tiles):
                x = refs[a][j, skip + first : skip + first + n, :].astype(jnp.float32)
                out[line : line + n, j * LANES : (j + 1) * LANES] = x
            out[line : line + n, tiles * LANES :] = side[a][first - at : first - at + n]


def shifted(tiles, lane, by):
    count = len(tiles)
    turned = [turn(t, by) for t in tiles]
    if by > 0:
        return [jnp.where(lane == 0, turned[j - 1], turned[j]) for j in range(count)]
    return [jnp.where(lane == LANES - 1, turned[(j + 1) % count], turned[j]) for j in range(count)]


SCALE = 2.0 / RADIUS


def decode(lane, code, lab, lab_d, lab_u, prior, weight):
    lab_r, lab_l = shifted(lab, lane, -1), shifted(lab, lane, 1)
    er, ed, eu, diag, rhs = [], [], [], [], []
    for j in range(len(code)):
        r = (code[j] & 1).astype(jnp.float32)
        l = ((code[j] >> 1) & 1).astype(jnp.float32)
        d = ((code[j] >> 2) & 1).astype(jnp.float32)
        u = ((code[j] >> 3) & 1).astype(jnp.float32)
        free = lab[j] == 0
        one = jnp.where(free, SCALE, 0.0)
        er.append(jnp.where(lab_r[j] == 0, one, 0.0) * r)
        ed.append(one * d)
        eu.append(one * u)
        diag.append(SCALE * ((r + l + d + u) + weight[j] - CENTRE))
        near = (
            jnp.where(lab_r[j] == 1, r, 0.0)
            + jnp.where(lab_l[j] == 1, l, 0.0)
            + jnp.where(lab_d[j] == 1, d, 0.0)
            + jnp.where(lab_u[j] == 1, u, 0.0)
        )
        rhs.append(jnp.where(free, weight[j] * prior[j] + near, 0.0))
    return er, ed, eu, diag, rhs


def recurrence(lane, k, v, v_d, v_u, before, er, ed, eu, diag):
    v_r = shifted(v, lane, -1)
    g = shifted([er[j] * v[j] for j in range(len(v))], lane, 1)
    new = []
    for j in range(len(v)):
        x = diag[j] * v[j] - (er[j] * v_r[j] + g[j])
        x = x - (ed[j] * v_d[j] + eu[j] * v_u[j])
        new.append(0.5 * x if k == 0 else x - before[j])
    return new


def summed(a, b):
    t = [x * y for x, y in zip(a, b)]
    while len(t) > 1:
        t = [t[q] + t[q + 1] for q in range(0, len(t) - 1, 2)] + ([t[-1]] if len(t) % 2 else [])
    return t[0]


def interior(code_t, lab_t, prior_t, weight_t, from_right, from_left, *refs):
    n = ITERS + 1
    field, (er_t, ed_t, eu_t, diag_t, side_lab, sums) = refs[:n], refs[n : n + 6]
    side_code, side_prior, side_weight = refs[n + 6 :]
    inner, rows = code_t.shape[0], code_t.shape[1]
    tiles = inner + 1
    lane = lane_ids(8)
    for at in range(0, rows, LANES):
        side = side_tiles(from_right, from_left, at)
        side_code[at : at + LANES, :] = side[0].astype(jnp.int32)
        side_lab[HALO + at : HALO + at + LANES, :] = side[1].astype(jnp.int32)
        side_prior[at : at + LANES, :] = side[2]
        side_weight[at : at + LANES, :] = side[3]
    seeds = jnp.full((HALO, LANES), 2, jnp.int32)
    side_lab[:HALO, :] = seeds
    side_lab[HALO + rows :, :] = seeds
    zero = jnp.zeros((8, LANES), jnp.float32)
    for k in range(1, ITERS):
        for j in range(tiles):
            field[k][j, :8, :] = zero
            field[k][j, rows - 8 :, :] = zero

    def read(ref, side, s):
        return [ref[j, pl.ds(s, 8), :] for j in range(inner)] + [side[pl.ds(s, 8), :]]

    def prepare(i, _):
        s = pl.multiple_of(8 * i, 8)
        here = pl.ds(s, 8)
        done = decode(
            lane,
            read(code_t, side_code, s),
            read(lab_t, side_lab, pl.multiple_of(s + HALO, 8)),
            read(lab_t, side_lab, s + HALO + 1),
            read(lab_t, side_lab, s + HALO - 1),
            read(prior_t, side_prior, s),
            read(weight_t, side_weight, s),
        )
        for ref, values in zip((er_t, ed_t, eu_t, diag_t, field[0]), done):
            for j in range(tiles):
                ref[j, here, :] = values[j]
        return 0

    lax.fori_loop(0, rows // 8, prepare, 0, unroll=8)

    def at_rows(ref, s):
        return [ref[j, pl.ds(s, 8), :] for j in range(tiles)]

    def advance(k, s):
        v = at_rows(field[k], s)
        new = recurrence(
            lane, k, v, at_rows(field[k], s + 1), at_rows(field[k], s - 1),
            at_rows(field[k - 1], s) if k else None,
            at_rows(er_t, s), at_rows(ed_t, s), at_rows(eu_t, s), at_rows(diag_t, s),
        )
        for j in range(tiles):
            field[k + 1][j, pl.ds(s, 8), :] = new[j]
        return v[:inner], new[:inner]

    count = 0
    for k in range(ITERS):
        last = k == ITERS - 1

        def body(i, carry, k=k, last=last):
            v, new = advance(k, pl.multiple_of(2 * HALO + 8 * i, 8))
            pairs = [(v, v), (v, new)] + ([(new, new)] if last else [])
            return tuple(acc + summed(a, b) for acc, (a, b) in zip(carry, pairs))

        if not last:
            advance(k, 8)
            advance(k, rows - 16)
        acc = (zero,) * (3 if last else 2)
        acc = lax.fori_loop(0, (rows - 4 * HALO) // 8, body, acc, unroll=15)
        for value in acc:
            sums[count] = value
            count += 1


def band(*refs):
    n = ITERS
    field, (er_t, ed_t, eu_t, diag_t, lab_t, side_lab) = refs[:n], refs[n : n + 6]
    sums, from_upper, from_lower = refs[n + 6 : n + 9]
    out, edge, labs, grid = refs[n + 9 :]
    inner, rows = lab_t.shape[0], er_t.shape[1]
    tiles = inner + 1
    lane = lane_ids(8)
    sub = lax.broadcasted_iota(jnp.int32, (8, LANES), 0)
    zero = jnp.zeros((8, LANES), jnp.float32)

    def lab_own(first):
        return [lab_t[j, HALO + first : HALO + first + 8, :] for j in range(inner)] + [
            side_lab[HALO + first : HALO + first + 8, :]
        ]

    def own(ref, first):
        return [ref[j, first : first + 8, :] for j in range(tiles)]

    terms = []
    for end, (message, first) in enumerate(((from_upper, 0), (from_lower, rows - 8))):
        def line(at, count=8, message=message):
            return [message[at : at + count, j * LANES : (j + 1) * LANES] for j in range(tiles)]

        beyond, mine = (0, 16) if end == 0 else (8, 0)
        for j, (x, y) in enumerate(zip(line(24, 16), lab_own(first))):
            labs[end, j, beyond : beyond + 16, :] = x.astype(jnp.int32)
            labs[end, j, mine : mine + 8, :] = y
        near = lambda at: [labs[end, j, at : at + 8, :] for j in range(tiles)]
        *halo, rhs = decode(
            lane, [x.astype(jnp.int32) for x in line(0)], near(8), near(9), near(7), line(8), line(16)
        )
        if end == 0:
            add = [jnp.where((sub == 0) & (x == 1) & (c > 0.0), 1.0, 0.0) for x, c in zip(near(15), own(eu_t, 0))]
        else:
            add = [jnp.where((sub == 7) & (x == 1) & (c > 0.0), 1.0, 0.0) for x, c in zip(near(1), own(ed_t, first))]
        outer = [x + y for x, y in zip(own(field[0], first), add)]
        step = 8 if end == 0 else -8
        next_in = own(field[0], first + step)
        coefficient = [[own(ref, f) for ref in (er_t, ed_t, eu_t, diag_t)] for f in (first, first + step)]
        trio = [(halo, rhs), (coefficient[0], outer), (coefficient[1], next_in)]
        if end == 1:
            trio.reverse()
        terms.append([t[0] for t in trio])
        for q, (_, start) in enumerate(trio):
            for j in range(tiles):
                grid[end, 0, j, 8 + 8 * q : 16 + 8 * q, :] = start[j]
        guard, inside, take = (0, 32, 16) if end == 0 else (32, 0, rows - 24)
        for k in range(ITERS):
            for j in range(tiles):
                grid[end, k, j, guard : guard + 8, :] = zero
                grid[end, k, j, inside : inside + 8, :] = field[k][j, take : take + 8, :]

    parts = [sums[q] for q in range(2 * ITERS + 1)]
    for k in range(ITERS):
        for end in range(2):
            at = lambda kk, s: [grid[end, kk, j, s : s + 8, :] for j in range(tiles)]
            for q in range(3):
                s = 8 + 8 * q
                v = at(k, s)
                new = recurrence(
                    lane, k, v, at(k, s + 1), at(k, s - 1), at(k - 1, s) if k else None, *terms[end][q]
                )
                for j in range(tiles):
                    grid[end, k + 1, j, s : s + 8, :] = new[j]
                mine = q - 1 if end == 0 else q
                if 0 <= mine < 2:
                    v, new = v[:inner], new[:inner]
                    parts[2 * k] = parts[2 * k] + summed(v, v)
                    parts[2 * k + 1] = parts[2 * k + 1] + summed(v, new)
                    for j in range(inner):
                        edge[k, end, j, 8 * mine : 8 * mine + 8, :] = v[j]
                    if k == ITERS - 1:
                        parts[2 * k + 2] = parts[2 * k + 2] + summed(new, new)
                        for j in range(inner):
                            edge[k + 1, end, j, 8 * mine : 8 * mine + 8, :] = new[j]

    every = jnp.zeros((1, LANES), jnp.float32)
    for q, acc in enumerate(parts):
        one = jnp.sum(jnp.sum(acc, axis=0, keepdims=True), axis=1, keepdims=True)
        every = jnp.where(lane_ids(1) == q, one, every)
    out[...] = jnp.broadcast_to(every[None], out.shape)


def coefficients(dots):
    n = ITERS
    inv = 1.0 / dots[0]
    moment = [jnp.ones_like(dots[0]), dots[1] * inv]
    for k in range(1, n + 1):
        moment.append(2.0 * (dots[2 * k] * inv) - moment[0])
        if k < n:
            moment.append(2.0 * (dots[2 * k + 1] * inv) - moment[1])
    gram = [[0.5 * (moment[i + j] + moment[abs(i - j)]) for j in range(n + 1)] for i in range(n + 1)]

    def image(p):
        q = [CENTRE * x for x in p] + [jnp.zeros_like(p[0])]
        for i, x in enumerate(p):
            if i == 0:
                q[1] = q[1] + RADIUS * x
            else:
                q[i + 1] = q[i + 1] + (RADIUS / 2) * x
                q[i - 1] = q[i - 1] + (RADIUS / 2) * x
        return q

    def product(a, b):
        sums = None
        for i, x in enumerate(a):
            t = gram[i][0] * b[0]
            for j in range(1, len(b)):
                t = t + gram[i][j] * b[j]
            sums = x * t if sums is None else sums + x * t
        return sums

    zero = jnp.zeros_like(inv)
    x, r, p = [], [moment[0]], [moment[0]]
    now = moment[0]
    for _ in range(n):
        q = image(p)
        alpha = now / product(p, q)
        x = [(x[i] if i < len(x) else zero) + alpha * p[i] for i in range(len(p))]
        r = [(r[i] if i < len(r) else zero) - alpha * q[i] for i in range(len(q))]
        following = product(r, r)
        beta = following / now
        p = [r[i] + (beta * p[i] if i < len(p) else zero) for i in range(len(r))]
        now = following
    size = zero
    for i in range(n + 1):
        size = size + jnp.abs(r[i]) * jnp.sqrt(jnp.maximum(gram[i][i], 0.0))
    good = (size * size <= (AMPLIFICATION * AMPLIFICATION) * now) & (now > 0.0)
    return x, r, good


def combine(every, lab_t, edge, *refs):
    n = ITERS + 1
    field, (labeling, residual, flag, sol_s, res_s, sem) = refs[:n], refs[n:]
    inner, rows = field[0].shape[0] - 1, field[0].shape[1]
    g = jnp.sum(every[:, 0, :], axis=0, keepdims=True)
    dots = [jnp.broadcast_to(g[:, q : q + 1], (8, LANES)) for q in range(2 * ITERS + 1)]
    x, r, good = coefficients(dots)
    flag[...] = good.astype(jnp.int32)

    def put(s, source):
        for j in range(inner):
            lanes = slice(j * LANES, (j + 1) * LANES)
            sol = jnp.where(lab_t[j, pl.ds(s + HALO, 8), :] == 1, 1.0, 0.0)
            res = None
            for k in range(n):
                t = source(k, j)
                res = r[k] * t if res is None else res + r[k] * t
                if k < ITERS:
                    sol = sol + x[k] * t
            sol_s[pl.ds(s, 8), lanes] = sol
            res_s[pl.ds(s, 8), lanes] = res

    def body(i, _):
        s = pl.multiple_of(8 * i, 8)
        put(s, lambda k, j: field[k][j, pl.ds(s, 8), :])
        return 0

    copies = []
    chunk = 64
    for c in range(rows // chunk):
        first, last = c * chunk // 8, (c + 1) * chunk // 8
        if c == 0:
            for q in range(2):
                put(8 * q, lambda k, j: edge[k, 0, j, 8 * q : 8 * q + 8, :])
            first += 2
        if (c + 1) * chunk == rows:
            last -= 2
        lax.fori_loop(first, last, body, 0, unroll=2)
        if (c + 1) * chunk == rows:
            for q in range(2):
                put(rows - 16 + 8 * q, lambda k, j: edge[k, 1, j, 8 * q : 8 * q + 8, :])
        at = pl.ds(c * chunk, chunk)
        for q, (src, dst) in enumerate(((sol_s, labeling), (res_s, residual))):
            copy = pltpu.make_async_copy(src.at[at, :], dst.at[0, at, :], sem.at[c, q])
            copy.start()
            copies.append(copy)
    for copy in copies:
        copy.wait()


def both_ways(axis, backward, forward):
    up = [(i, i + 1) for i in range(lax.axis_size(axis) - 1)]
    return (
        lax.ppermute(backward, axis, [(b, a) for a, b in up]),
        lax.ppermute(forward, axis, up),
    )


def call(body, in_specs, outs, scratch, mib, flops, operands, out_specs=None):
    return pl.pallas_call(
        body,
        in_specs=in_specs,
        out_specs=out_specs or [VMEM] * len(outs),
        out_shape=outs,
        scratch_shapes=scratch,
        compiler_params=pltpu.CompilerParams(vmem_limit_bytes=mib * 1024 * 1024),
        cost_estimate=pl.CostEstimate(flops=flops, bytes_accessed=1 << 20, transcendentals=0),
    )(*operands)


def per_device(edges, labels, prior, data_weight):
    arrays = (edges, labels, prior, data_weight)
    _, rows, cols = edges.shape
    f32, i32 = jnp.float32, jnp.int32
    shape = jax.ShapeDtypeStruct
    inner = cols // LANES
    tiles = inner + 1
    dma = pltpu.SemaphoreType.DMA

    to_left, to_right = call(
        col_pack, [ANY] * 4, [shape((LINES, rows), f32)] * 2,
        [
            pltpu.VMEM((2, 2, rows, LANES), i32),
            pltpu.VMEM((2, 2, rows, LANES), f32),
            dma((2, 4, rows // LANES)),
        ],
        6, 1 << 20, arrays,
    )
    from_right, from_left = both_ways("col", to_left, to_right)

    block = call(
        load, [ANY] * 4,
        [
            shape((inner, rows, LANES), i32),
            shape((inner, rows + 2 * HALO, LANES), i32),
            shape((inner, rows, LANES), f32),
            shape((inner, rows, LANES), f32),
        ],
        [dma((4, inner))], 6, 1 << 24, arrays,
    )
    to_upper, to_lower = call(
        row_pack, [VMEM] * 6, [shape((LINES, tiles * LANES), f32)] * 2, [],
        4, 1 << 20, (*block, from_right, from_left),
    )
    from_lower, from_upper = both_ways("row", to_upper, to_lower)

    n = ITERS + 1
    out = call(
        interior, [VMEM] * 6,
        [shape((tiles, rows, LANES), f32)] * (n + 4)
        + [shape((rows + 2 * HALO, LANES), i32), shape((2 * ITERS + 1, 8, LANES), f32)],
        [pltpu.VMEM((rows, LANES), i32), pltpu.VMEM((rows, LANES), f32), pltpu.VMEM((rows, LANES), f32)],
        16, 1 << 26, (*block, from_right, from_left),
    )
    field, terms, side_lab, sums = out[:n], out[n : n + 4], out[n + 4], out[n + 5]
    group = lax.axis_size(("row", "col"))
    sums, edge = call(
        band, [VMEM] * (ITERS + 9),
        [shape((group, 1, LANES), f32), shape((n, 2, inner, 2 * HALO, LANES), f32)],
        [pltpu.VMEM((2, tiles, 24, LANES), i32), pltpu.VMEM((2, n, tiles, 40, LANES), f32)],
        6, 1 << 20, (*field[:ITERS], *terms, block[1], side_lab, sums, from_upper, from_lower),
    )
    every = lax.all_to_all(sums, ("row", "col"), 0, 0, tiled=True)

    labeling, residual, flag = call(
        combine, [VMEM] * (n + 3),
        [shape(edges.shape, f32)] * 2 + [shape((8, LANES), i32)],
        [pltpu.VMEM((rows, cols), f32)] * 2 + [dma((rows // 64, 2))],
        4, 1 << 20, (every, block[1], edge, *field), out_specs=[ANY, ANY, VMEM],
    )

    def again(carry):
        return (jnp.int32(1), *plain(edges, labels, prior, data_weight))

    _, labeling, residual = lax.while_loop(
        lambda carry: carry[0] == 0, again, (flag[0, 0], labeling, residual)
    )
    return labeling, residual


def solution(mesh):
    spec = P("img", "row", "col")
    return jax.shard_map(
        per_device, mesh=mesh, in_specs=(spec,) * 4, out_specs=(spec,) * 2, check_vma=False
    )
```

```python
import functools
import jax
import jax.numpy as jnp
from jax import lax
from jax.experimental import pallas as pl
from jax.experimental.pallas import tpu as pltpu
from jax.sharding import PartitionSpec as P

ITERS = 8
HALO = 8
LANES = 128
LOW, HIGH = 0.05, 7.5
CENTRE, RADIUS = (HIGH + LOW) / 2, (HIGH - LOW) / 2
AMPLIFICATION = 24.0
VMEM = pl.BlockSpec(memory_space=pltpu.VMEM)
ANY = pl.BlockSpec(memory_space=pl.ANY)
HBM = pl.BlockSpec(memory_space=pltpu.HBM)


def with_halo(array, sides, width):
    edges = {}
    for axis, dim in sides:
        count, length = (lax.axis_size(axis), array.shape[dim])
        up = [(i, (i + 1) % count) for i in range(count - 1)]
        last = lax.slice_in_dim(array, length - width, length, axis=dim)
        first = lax.slice_in_dim(array, 0, width, axis=dim)
        edges[dim] = (
            lax.ppermute(last, axis, up),
            lax.ppermute(first, axis, [(b, a) for a, b in up]),
        )
    done = []
    for _, dim in sides:
        low, high = edges[dim]
        around = [(width, width) if d in done else (0, 0) for d in range(array.ndim)]
        array = jnp.concatenate([jnp.pad(low, around), array, jnp.pad(high, around)], axis=dim)
        done.append(dim)
    return array


def total(value, axis):
    count = lax.axis_size(axis)
    flat = value.reshape(1, 1, 1)
    every = lax.all_to_all(jnp.broadcast_to(flat, (count, 1, 1)), axis, 0, 0, tiled=True)
    return every.sum()


def neighbours(field, right, left, down, upper):
    padded = with_halo(field, (("row", 1), ("col", 2)), 1)
    return (
        right * padded[:, 1:-1, 2:]
        + left * padded[:, 1:-1, :-2]
        + down * padded[:, 2:, 1:-1]
        + upper * padded[:, :-2, 1:-1]
    )


def plain(edges, labels, prior, data_weight):
    right = (edges % 2).astype(jnp.float32)
    left = (edges // 2 % 2).astype(jnp.float32)
    down = (edges // 4 % 2).astype(jnp.float32)
    upper = (edges // 8 % 2).astype(jnp.float32)
    degree = right + left + down + upper
    free = (labels == 0).astype(jnp.float32)
    anchor = (labels == 1).astype(jnp.float32)
    diag_term = degree + data_weight

    def nearby(field):
        return neighbours(field, right, left, down, upper)

    rhs = free * (data_weight * prior + nearby(anchor))

    def step(_, carry):
        result, residual, direction, norm_now = carry
        image_v = free * (diag_term * direction - nearby(direction))
        alpha = norm_now / total(jnp.sum(direction * image_v), ("row", "col"))
        result = result + alpha * direction
        residual = residual - alpha * image_v
        norm_next = total(jnp.sum(residual * residual), ("row", "col"))
        direction = residual + (norm_next / norm_now) * direction
        return result, residual, direction, norm_next

    start = (jnp.zeros_like(rhs), rhs, rhs, total(jnp.sum(rhs * rhs), ("row", "col")))
    result, residual, _, _ = lax.fori_loop(0, ITERS, step, start)
    return anchor + result, residual


WIDTH = HALO + 1
LINES = 40
TOP_OF = ((0, 0, 8), (2, 8, 8), (3, 16, 8), (1, 24, 16))


def lane_ids(rows):
    return lax.broadcasted_iota(jnp.int32, (rows, LANES), 1)


def turn(x, by):
    return pltpu.roll(x, by % LANES, 1) if by % LANES else x


def col_pack(edges, labels, prior, weight, first, second, ints, floats, sem):
    arrays = (edges, labels, prior, weight)
    rows, cols = edges.shape[1], edges.shape[2]
    lane = lane_ids(LANES)

    def copy(side, a, chunk):
        at = pl.ds(chunk * LANES, LANES)
        dst = (ints if a < 2 else floats).at[side, a % 2, at, :]
        return pltpu.make_async_copy(
            arrays[a].at[0, at, pl.ds(side * (cols - LANES), LANES)], dst, sem.at[side, a, chunk]
        )

    chunks = rows // LANES
    for chunk in range(chunks):
        for side in range(2):
            for a in range(4):
                copy(side, a, chunk).start()
    for chunk in range(chunks):
        at = slice(chunk * LANES, (chunk + 1) * LANES)
        lines = []
        for side, base in ((0, 0), (1, LANES - WIDTH)):
            packed = None
            for a in range(4):
                copy(side, a, chunk).wait()
                x = (ints if a < 2 else floats)[side, a % 2, at, :].astype(jnp.float32)
                x = turn(x, a * WIDTH - base)
                packed = x if packed is None else jnp.where(lane < a * WIDTH, packed, x)
            lines.append(jnp.swapaxes(packed, 0, 1)[:LINES])
        first[:, at], second[:, at] = ordered("col", *lines)


def ordered(axis, before, after):
    even = lax.axis_index(axis) % 2 == 0
    return jnp.where(even, after, before), jnp.where(even, before, after)


def load(edges, labels, prior, weight, code_t, lab_t, prior_t, weight_t, sem):
    rows = edges.shape[1]
    tiles = code_t.shape[0]
    copies = []
    for a, (src, dst, at) in enumerate(
        ((edges, code_t, 0), (labels, lab_t, HALO), (prior, prior_t, 0), (weight, weight_t, 0))
    ):
        for j in range(tiles):
            copies.append(
                pltpu.make_async_copy(
                    src.at[0, :, pl.ds(j * LANES, LANES)],
                    dst.at[j, pl.ds(at, rows), :],
                    sem.at[a, j],
                )
            )
    for copy in copies:
        copy.start()
    seeds = jnp.full((HALO, LANES), 2, jnp.int32)
    for j in range(tiles):
        lab_t[j, :HALO, :] = seeds
        lab_t[j, HALO + rows :, :] = seeds
    for copy in copies:
        copy.wait()


def side_tiles(first, second, at):
    pad = jnp.zeros((LANES - LINES, LANES), jnp.float32)
    r, l = ordered("col", second[:, at : at + LANES], first[:, at : at + LANES])
    r = jnp.swapaxes(jnp.concatenate([r, pad], 0), 0, 1)
    l = jnp.swapaxes(jnp.concatenate([l, pad], 0), 0, 1)
    lane = lane_ids(LANES)
    tiles = []
    for a in range(4):
        right = turn(r, -a * WIDTH)
        left = turn(l, LANES - WIDTH - a * WIDTH)
        outside = 2.0 if a == 1 else 0.0
        tiles.append(jnp.where(lane < WIDTH, right, jnp.where(lane >= LANES - WIDTH, left, outside)))
    return tiles


def row_pack(code_t, lab_t, prior_t, weight_t, col_first, col_second, first, second):
    tiles, rows = code_t.shape[0], code_t.shape[1]
    refs = (code_t, lab_t, prior_t, weight_t)
    top = side_tiles(col_first, col_second, 0)
    bottom = side_tiles(col_first, col_second, rows - LANES)
    for a, line, n in TOP_OF:
        skip = HALO if a == 1 else 0
        here = slice(line, line + n)
        for j in range(tiles):
            lanes = slice(j * LANES, (j + 1) * LANES)
            up = refs[a][j, skip : skip + n, :].astype(jnp.float32)
            low = refs[a][j, skip + rows - n : skip + rows, :].astype(jnp.float32)
            first[here, lanes], second[here, lanes] = ordered("row", up, low)
        lanes = slice(tiles * LANES, (tiles + 1) * LANES)
        first[here, lanes], second[here, lanes] = ordered("row", top[a][:n], bottom[a][LANES - n :])


def shifted(tiles, lane, by):
    count = len(tiles)
    turned = [turn(t, by) for t in tiles]
    if by > 0:
        return [jnp.where(lane == 0, turned[j - 1], turned[j]) for j in range(count)]
    return [jnp.where(lane == LANES - 1, turned[(j + 1) % count], turned[j]) for j in range(count)]


SCALE = 2.0 / RADIUS


def decode(lane, code, lab, lab_d, lab_u, prior, weight):
    lab_r, lab_l = shifted(lab, lane, -1), shifted(lab, lane, 1)
    er, ed, eu, diag, rhs = [], [], [], [], []
    for j in range(len(code)):
        r = (code[j] & 1).astype(jnp.float32)
        l = ((code[j] >> 1) & 1).astype(jnp.float32)
        d = ((code[j] >> 2) & 1).astype(jnp.float32)
        u = ((code[j] >> 3) & 1).astype(jnp.float32)
        free = lab[j] == 0
        one = jnp.where(free, SCALE, 0.0)
        er.append(jnp.where(lab_r[j] == 0, one, 0.0) * r)
        ed.append(one * d)
        eu.append(one * u)
        diag.append(SCALE * ((r + l + d + u) + weight[j] - CENTRE))
        near = (
            jnp.where(lab_r[j] == 1, r, 0.0)
            + jnp.where(lab_l[j] == 1, l, 0.0)
            + jnp.where(lab_d[j] == 1, d, 0.0)
            + jnp.where(lab_u[j] == 1, u, 0.0)
        )
        rhs.append(jnp.where(free, weight[j] * prior[j] + near, 0.0))
    return er, ed, eu, diag, rhs


def recurrence(lane, k, v, v_d, v_u, before, er, ed, eu, diag):
    v_r = shifted(v, lane, -1)
    g = shifted([er[j] * v[j] for j in range(len(v))], lane, 1)
    new = []
    for j in range(len(v)):
        x = diag[j] * v[j] - (er[j] * v_r[j] + g[j])
        x = x - (ed[j] * v_d[j] + eu[j] * v_u[j])
        new.append(0.5 * x if k == 0 else x - before[j])
    return new


def summed(a, b):
    t = [x * y for x, y in zip(a, b)]
    while len(t) > 1:
        t = [t[q] + t[q + 1] for q in range(0, len(t) - 1, 2)] + ([t[-1]] if len(t) % 2 else [])
    return t[0]


def interior(code_t, lab_t, prior_t, weight_t, col_first, col_second, *refs):
    n = ITERS + 1
    field, (er_t, ed_t, eu_t, diag_t, side_lab, sums) = refs[:n], refs[n : n + 6]
    side_code, side_prior, side_weight = refs[n + 6 :]
    inner, rows = code_t.shape[0], code_t.shape[1]
    tiles = inner + 1
    lane = lane_ids(8)
    for at in range(0, rows, LANES):
        side = side_tiles(col_first, col_second, at)
        side_code[at : at + LANES, :] = side[0].astype(jnp.int32)
        side_lab[HALO + at : HALO + at + LANES, :] = side[1].astype(jnp.int32)
        side_prior[at : at + LANES, :] = side[2]
        side_weight[at : at + LANES, :] = side[3]
    seeds = jnp.full((HALO, LANES), 2, jnp.int32)
    side_lab[:HALO, :] = seeds
    side_lab[HALO + rows :, :] = seeds
    zero = jnp.zeros((8, LANES), jnp.float32)
    for k in range(1, ITERS):
        for j in range(tiles):
            field[k][j, :8, :] = zero
            field[k][j, rows - 8 :, :] = zero

    def read(ref, side, s):
        return [ref[j, pl.ds(s, 8), :] for j in range(inner)] + [side[pl.ds(s, 8), :]]

    def prepare(i, _):
        s = pl.multiple_of(8 * i, 8)
        here = pl.ds(s, 8)
        done = decode(
            lane,
            read(code_t, side_code, s),
            read(lab_t, side_lab, pl.multiple_of(s + HALO, 8)),
            read(lab_t, side_lab, s + HALO + 1),
            read(lab_t, side_lab, s + HALO - 1),
            read(prior_t, side_prior, s),
            read(weight_t, side_weight, s),
        )
        for ref, values in zip((er_t, ed_t, eu_t, diag_t, field[0]), done):
            for j in range(tiles):
                ref[j, here, :] = values[j]
        return 0

    lax.fori_loop(0, rows // 8, prepare, 0, unroll=8)

    def at_rows(ref, s):
        return [ref[j, pl.ds(s, 8), :] for j in range(tiles)]

    def advance(k, s):
        v = at_rows(field[k], s)
        new = recurrence(
            lane, k, v, at_rows(field[k], s + 1), at_rows(field[k], s - 1),
            at_rows(field[k - 1], s) if k else None,
            at_rows(er_t, s), at_rows(ed_t, s), at_rows(eu_t, s), at_rows(diag_t, s),
        )
        for j in range(tiles):
            field[k + 1][j, pl.ds(s, 8), :] = new[j]
        return v[:inner], new[:inner]

    count = 0
    for k in range(ITERS):
        last = k == ITERS - 1

        def body(i, carry, k=k, last=last):
            v, new = advance(k, pl.multiple_of(2 * HALO + 8 * i, 8))
            pairs = [(v, v), (v, new)] + ([(new, new)] if last else [])
            return tuple(acc + summed(a, b) for acc, (a, b) in zip(carry, pairs))

        if not last:
            advance(k, 8)
            advance(k, rows - 16)
        acc = (zero,) * (3 if last else 2)
        acc = lax.fori_loop(0, (rows - 4 * HALO) // 8, body, acc, unroll=15)
        for value in acc:
            sums[count] = value
            count += 1


def band(*refs):
    n = ITERS
    field, (er_t, ed_t, eu_t, diag_t, lab_t, side_lab) = refs[:n], refs[n : n + 6]
    sums, row_first, row_second = refs[n + 6 : n + 9]
    out, edge, labs, grid = refs[n + 9 :]
    inner, rows = lab_t.shape[0], er_t.shape[1]
    tiles = inner + 1
    lane = lane_ids(8)
    sub = lax.broadcasted_iota(jnp.int32, (8, LANES), 0)
    zero = jnp.zeros((8, LANES), jnp.float32)

    def lab_own(first):
        return [lab_t[j, HALO + first : HALO + first + 8, :] for j in range(inner)] + [
            side_lab[HALO + first : HALO + first + 8, :]
        ]

    def own(ref, first):
        return [ref[j, first : first + 8, :] for j in range(tiles)]

    terms = []
    for end, first in enumerate((0, rows - 8)):
        def line(at, count=8, end=end):
            both = [
                ordered("row", row_second[at : at + count, lanes], row_first[at : at + count, lanes])
                for lanes in (slice(j * LANES, (j + 1) * LANES) for j in range(tiles))
            ]
            return [pair[1 - end] for pair in both]

        beyond, mine = (0, 16) if end == 0 else (8, 0)
        for j, (x, y) in enumerate(zip(line(24, 16), lab_own(first))):
            labs[end, j, beyond : beyond + 16, :] = x.astype(jnp.int32)
            labs[end, j, mine : mine + 8, :] = y
        near = lambda at: [labs[end, j, at : at + 8, :] for j in range(tiles)]
        *halo, rhs = decode(
            lane, [x.astype(jnp.int32) for x in line(0)], near(8), near(9), near(7), line(8), line(16)
        )
        if end == 0:
            add = [jnp.where((sub == 0) & (x == 1) & (c > 0.0), 1.0, 0.0) for x, c in zip(near(15), own(eu_t, 0))]
        else:
            add = [jnp.where((sub == 7) & (x == 1) & (c > 0.0), 1.0, 0.0) for x, c in zip(near(1), own(ed_t, first))]
        outer = [x + y for x, y in zip(own(field[0], first), add)]
        step = 8 if end == 0 else -8
        next_in = own(field[0], first + step)
        coefficient = [[own(ref, f) for ref in (er_t, ed_t, eu_t, diag_t)] for f in (first, first + step)]
        trio = [(halo, rhs), (coefficient[0], outer), (coefficient[1], next_in)]
        if end == 1:
            trio.reverse()
        terms.append([t[0] for t in trio])
        for q, (_, start) in enumerate(trio):
            for j in range(tiles):
                grid[end, 0, j, 8 + 8 * q : 16 + 8 * q, :] = start[j]
        guard, inside, take = (0, 32, 16) if end == 0 else (32, 0, rows - 24)
        for k in range(ITERS):
            for j in range(tiles):
                grid[end, k, j, guard : guard + 8, :] = zero
                grid[end, k, j, inside : inside + 8, :] = field[k][j, take : take + 8, :]

    parts = [sums[q] for q in range(2 * ITERS + 1)]
    for k in range(ITERS):
        for end in range(2):
            at = lambda kk, s: [grid[end, kk, j, s : s + 8, :] for j in range(tiles)]
            for q in range(3):
                s = 8 + 8 * q
                v = at(k, s)
                new = recurrence(
                    lane, k, v, at(k, s + 1), at(k, s - 1), at(k - 1, s) if k else None, *terms[end][q]
                )
                for j in range(tiles):
                    grid[end, k + 1, j, s : s + 8, :] = new[j]
                mine = q - 1 if end == 0 else q
                if 0 <= mine < 2:
                    v, new = v[:inner], new[:inner]
                    parts[2 * k] = parts[2 * k] + summed(v, v)
                    parts[2 * k + 1] = parts[2 * k + 1] + summed(v, new)
                    for j in range(inner):
                        edge[k, end, j, 8 * mine : 8 * mine + 8, :] = v[j]
                    if k == ITERS - 1:
                        parts[2 * k + 2] = parts[2 * k + 2] + summed(new, new)
                        for j in range(inner):
                            edge[k + 1, end, j, 8 * mine : 8 * mine + 8, :] = new[j]

    every = jnp.zeros((1, LANES), jnp.float32)
    for q, acc in enumerate(parts):
        one = jnp.sum(jnp.sum(acc, axis=0, keepdims=True), axis=1, keepdims=True)
        every = jnp.where(lane_ids(1) == q, one, every)
    out[...] = jnp.broadcast_to(every[None], out.shape)


def coefficients(dots):
    n = ITERS
    inv = 1.0 / dots[0]
    moment = [jnp.ones_like(dots[0]), dots[1] * inv]
    for k in range(1, n + 1):
        moment.append(2.0 * (dots[2 * k] * inv) - moment[0])
        if k < n:
            moment.append(2.0 * (dots[2 * k + 1] * inv) - moment[1])
    gram = [[0.5 * (moment[i + j] + moment[abs(i - j)]) for j in range(n + 1)] for i in range(n + 1)]

    def image(p):
        q = [CENTRE * x for x in p] + [jnp.zeros_like(p[0])]
        for i, x in enumerate(p):
            if i == 0:
                q[1] = q[1] + RADIUS * x
            else:
                q[i + 1] = q[i + 1] + (RADIUS / 2) * x
                q[i - 1] = q[i - 1] + (RADIUS / 2) * x
        return q

    def product(a, b):
        sums = None
        for i, x in enumerate(a):
            t = gram[i][0] * b[0]
            for j in range(1, len(b)):
                t = t + gram[i][j] * b[j]
            sums = x * t if sums is None else sums + x * t
        return sums

    zero = jnp.zeros_like(inv)
    x, r, p = [], [moment[0]], [moment[0]]
    now = moment[0]
    for _ in range(n):
        q = image(p)
        alpha = now / product(p, q)
        x = [(x[i] if i < len(x) else zero) + alpha * p[i] for i in range(len(p))]
        r = [(r[i] if i < len(r) else zero) - alpha * q[i] for i in range(len(q))]
        following = product(r, r)
        beta = following / now
        p = [r[i] + (beta * p[i] if i < len(p) else zero) for i in range(len(r))]
        now = following
    size = zero
    for i in range(n + 1):
        size = size + jnp.abs(r[i]) * jnp.sqrt(jnp.maximum(gram[i][i], 0.0))
    good = (size * size <= (AMPLIFICATION * AMPLIFICATION) * now) & (now > 0.0)
    return x, r, good


def combine(every, lab_t, edge, *refs):
    n = ITERS + 1
    field, (labeling, residual, flag, sol_s, res_s, sem) = refs[:n], refs[n:]
    inner, rows = field[0].shape[0] - 1, field[0].shape[1]
    g = jnp.sum(every[:, 0, :], axis=0, keepdims=True)
    dots = [jnp.broadcast_to(g[:, q : q + 1], (8, LANES)) for q in range(2 * ITERS + 1)]
    x, r, good = coefficients(dots)
    flag[...] = good.astype(jnp.int32)

    def put(s, source):
        for j in range(inner):
            lanes = slice(j * LANES, (j + 1) * LANES)
            sol = jnp.where(lab_t[j, pl.ds(s + HALO, 8), :] == 1, 1.0, 0.0)
            res = None
            for k in range(n):
                t = source(k, j)
                res = r[k] * t if res is None else res + r[k] * t
                if k < ITERS:
                    sol = sol + x[k] * t
            sol_s[pl.ds(s, 8), lanes] = sol
            res_s[pl.ds(s, 8), lanes] = res

    def body(i, _):
        s = pl.multiple_of(8 * i, 8)
        put(s, lambda k, j: field[k][j, pl.ds(s, 8), :])
        return 0

    copies = []
    chunk = 64
    for c in range(rows // chunk):
        first, last = c * chunk // 8, (c + 1) * chunk // 8
        if c == 0:
            for q in range(2):
                put(8 * q, lambda k, j: edge[k, 0, j, 8 * q : 8 * q + 8, :])
            first += 2
        if (c + 1) * chunk == rows:
            last -= 2
        lax.fori_loop(first, last, body, 0, unroll=2)
        if (c + 1) * chunk == rows:
            for q in range(2):
                put(rows - 16 + 8 * q, lambda k, j: edge[k, 1, j, 8 * q : 8 * q + 8, :])
        at = pl.ds(c * chunk, chunk)
        for q, (src, dst) in enumerate(((sol_s, labeling), (res_s, residual))):
            copy = pltpu.make_async_copy(src.at[at, :], dst.at[0, at, :], sem.at[c, q])
            copy.start()
            copies.append(copy)
    for copy in copies:
        copy.wait()


def swaps(axis, first, second, around):
    count = lax.axis_size(axis)
    pairs = [(i, i + 1) for i in range(0, count - 1, 2)]
    others = [(i, i + 1) for i in range(1, count - 1, 2)] + ([(count - 1, 0)] if around else [])
    both = lambda p: [(a, b) for a, b in p] + [(b, a) for a, b in p]
    return lax.ppermute(first, axis, both(pairs)), lax.ppermute(second, axis, both(others))


def call(body, in_specs, outs, scratch, mib, flops, operands, out_specs=None):
    return pl.pallas_call(
        body,
        in_specs=in_specs,
        out_specs=out_specs or [VMEM] * len(outs),
        out_shape=outs,
        scratch_shapes=scratch,
        compiler_params=pltpu.CompilerParams(vmem_limit_bytes=mib * 1024 * 1024),
        cost_estimate=pl.CostEstimate(flops=flops, bytes_accessed=1 << 20, transcendentals=0),
    )(*operands)


def per_device(edges, labels, prior, data_weight):
    arrays = (edges, labels, prior, data_weight)
    _, rows, cols = edges.shape
    f32, i32 = jnp.float32, jnp.int32
    shape = jax.ShapeDtypeStruct
    inner = cols // LANES
    tiles = inner + 1
    dma = pltpu.SemaphoreType.DMA

    col_messages = call(
        col_pack, [HBM] * 4, [shape((LINES, rows), f32)] * 2,
        [
            pltpu.VMEM((2, 2, rows, LANES), i32),
            pltpu.VMEM((2, 2, rows, LANES), f32),
            dma((2, 4, rows // LANES)),
        ],
        6, 1 << 20, arrays,
    )
    col_first, col_second = swaps("col", *col_messages, True)

    block = call(
        load, [HBM] * 4,
        [
            shape((inner, rows, LANES), i32),
            shape((inner, rows + 2 * HALO, LANES), i32),
            shape((inner, rows, LANES), f32),
            shape((inner, rows, LANES), f32),
        ],
        [dma((4, inner))], 6, 1 << 24, arrays,
    )
    row_messages = call(
        row_pack, [VMEM] * 6, [shape((LINES, tiles * LANES), f32)] * 2, [],
        4, 1 << 20, (*block, col_first, col_second),
    )
    row_first, row_second = swaps("row", *row_messages, False)

    n = ITERS + 1
    out = call(
        interior, [VMEM] * 6,
        [shape((tiles, rows, LANES), f32)] * (n + 4)
        + [shape((rows + 2 * HALO, LANES), i32), shape((2 * ITERS + 1, 8, LANES), f32)],
        [pltpu.VMEM((rows, LANES), i32), pltpu.VMEM((rows, LANES), f32), pltpu.VMEM((rows, LANES), f32)],
        16, 1 << 26, (*block, col_first, col_second),
    )
    field, terms, side_lab, sums = out[:n], out[n : n + 4], out[n + 4], out[n + 5]
    group = lax.axis_size(("row", "col"))
    sums, edge = call(
        band, [VMEM] * (ITERS + 9),
        [shape((group, 1, LANES), f32), shape((n, 2, inner, 2 * HALO, LANES), f32)],
        [pltpu.VMEM((2, tiles, 24, LANES), i32), pltpu.VMEM((2, n, tiles, 40, LANES), f32)],
        6, 1 << 20, (*field[:ITERS], *terms, block[1], side_lab, sums, row_first, row_second),
    )
    every = lax.all_to_all(sums, ("row", "col"), 0, 0, tiled=True)

    labeling, residual, flag = call(
        combine, [VMEM] * (n + 3),
        [shape(edges.shape, f32)] * 2 + [shape((8, LANES), i32)],
        [pltpu.VMEM((rows, cols), f32)] * 2 + [dma((rows // 64, 2))],
        4, 1 << 20, (every, block[1], edge, *field), out_specs=[ANY, ANY, VMEM],
    )

    def again(carry):
        return (jnp.int32(1), *plain(edges, labels, prior, data_weight))

    _, labeling, residual = lax.while_loop(
        lambda carry: carry[0] == 0, again, (flag[0, 0], labeling, residual)
    )
    return labeling, residual


def solution(mesh):
    spec = P("img", "row", "col")
    return jax.shard_map(
        per_device, mesh=mesh, in_specs=(spec,) * 4, out_specs=(spec,) * 2, check_vma=False
    )
```

```python
import functools
import jax
import jax.numpy as jnp
from jax import lax
from jax.experimental import pallas as pl
from jax.experimental.pallas import tpu as pltpu
from jax.sharding import PartitionSpec as P

ITERS = 8
HALO = 8
LANES = 128
LOW, HIGH = 0.05, 7.5
CENTRE, RADIUS = (HIGH + LOW) / 2, (HIGH - LOW) / 2
AMPLIFICATION = 24.0
VMEM = pl.BlockSpec(memory_space=pltpu.VMEM)
ANY = pl.BlockSpec(memory_space=pl.ANY)
HBM = pl.BlockSpec(memory_space=pltpu.HBM)


def with_halo(array, sides, width):
    edges = {}
    for axis, dim in sides:
        count, length = (lax.axis_size(axis), array.shape[dim])
        up = [(i, (i + 1) % count) for i in range(count - 1)]
        last = lax.slice_in_dim(array, length - width, length, axis=dim)
        first = lax.slice_in_dim(array, 0, width, axis=dim)
        edges[dim] = (
            lax.ppermute(last, axis, up),
            lax.ppermute(first, axis, [(b, a) for a, b in up]),
        )
    done = []
    for _, dim in sides:
        low, high = edges[dim]
        around = [(width, width) if d in done else (0, 0) for d in range(array.ndim)]
        array = jnp.concatenate([jnp.pad(low, around), array, jnp.pad(high, around)], axis=dim)
        done.append(dim)
    return array


def total(value, axis):
    count = lax.axis_size(axis)
    flat = value.reshape(1, 1, 1)
    every = lax.all_to_all(jnp.broadcast_to(flat, (count, 1, 1)), axis, 0, 0, tiled=True)
    return every.sum()


def neighbours(field, right, left, down, upper):
    padded = with_halo(field, (("row", 1), ("col", 2)), 1)
    return (
        right * padded[:, 1:-1, 2:]
        + left * padded[:, 1:-1, :-2]
        + down * padded[:, 2:, 1:-1]
        + upper * padded[:, :-2, 1:-1]
    )


def plain(edges, labels, prior, data_weight):
    right = (edges % 2).astype(jnp.float32)
    left = (edges // 2 % 2).astype(jnp.float32)
    down = (edges // 4 % 2).astype(jnp.float32)
    upper = (edges // 8 % 2).astype(jnp.float32)
    degree = right + left + down + upper
    free = (labels == 0).astype(jnp.float32)
    anchor = (labels == 1).astype(jnp.float32)
    diag_term = degree + data_weight

    def nearby(field):
        return neighbours(field, right, left, down, upper)

    rhs = free * (data_weight * prior + nearby(anchor))

    def step(_, carry):
        result, residual, direction, norm_now = carry
        image_v = free * (diag_term * direction - nearby(direction))
        alpha = norm_now / total(jnp.sum(direction * image_v), ("row", "col"))
        result = result + alpha * direction
        residual = residual - alpha * image_v
        norm_next = total(jnp.sum(residual * residual), ("row", "col"))
        direction = residual + (norm_next / norm_now) * direction
        return result, residual, direction, norm_next

    start = (jnp.zeros_like(rhs), rhs, rhs, total(jnp.sum(rhs * rhs), ("row", "col")))
    result, residual, _, _ = lax.fori_loop(0, ITERS, step, start)
    return anchor + result, residual


WIDTH = HALO + 1
LINES = 40
TOP_OF = ((0, 0, 8), (2, 8, 8), (3, 16, 8), (1, 24, 16))


def lane_ids(rows):
    return lax.broadcasted_iota(jnp.int32, (rows, LANES), 1)


def turn(x, by):
    return pltpu.roll(x, by % LANES, 1) if by % LANES else x


def col_pack(edges, labels, prior, weight, first, second, ints, floats, sem):
    arrays = (edges, labels, prior, weight)
    rows, cols = edges.shape[1], edges.shape[2]
    lane = lane_ids(LANES)
    held = [(ints if a < 2 else floats).at[:, a % 2] for a in range(4)]
    copies = []
    for side in range(2):
        for a, ref in enumerate(arrays):
            src = ref.at[0, :, pl.ds(side * (cols - LANES), LANES)]
            copies.append(pltpu.make_async_copy(src, held[a].at[side], sem.at[side, a]))
    for copy in copies:
        copy.start()
    for copy in copies:
        copy.wait()
    for chunk in range(rows // LANES):
        at = slice(chunk * LANES, (chunk + 1) * LANES)
        lines = []
        for side, base in ((0, 0), (1, LANES - WIDTH)):
            packed = None
            for a in range(4):
                x = turn(held[a][side, at, :].astype(jnp.float32), a * WIDTH - base)
                packed = x if packed is None else jnp.where(lane < a * WIDTH, packed, x)
            lines.append(jnp.swapaxes(packed, 0, 1)[:LINES])
        first[:, at], second[:, at] = ordered("col", *lines)


def ordered(axis, before, after):
    even = lax.axis_index(axis) % 2 == 0
    return jnp.where(even, after, before), jnp.where(even, before, after)


def side_tiles(first, second, at):
    pad = jnp.zeros((LANES - LINES, LANES), jnp.float32)
    r, l = ordered("col", second[:, at : at + LANES], first[:, at : at + LANES])
    r = jnp.swapaxes(jnp.concatenate([r, pad], 0), 0, 1)
    l = jnp.swapaxes(jnp.concatenate([l, pad], 0), 0, 1)
    lane = lane_ids(LANES)
    tiles = []
    for a in range(4):
        right = turn(r, -a * WIDTH)
        left = turn(l, LANES - WIDTH - a * WIDTH)
        outside = 2.0 if a == 1 else 0.0
        tiles.append(jnp.where(lane < WIDTH, right, jnp.where(lane >= LANES - WIDTH, left, outside)))
    return tiles


def row_pack(edges, lab_t, prior, weight, col_first, col_second, first, second):
    rows, cols = edges.shape[1], edges.shape[2]
    tiles = cols // LANES
    refs = (edges, None, prior, weight)
    top = side_tiles(col_first, col_second, 0)
    bottom = side_tiles(col_first, col_second, rows - LANES)
    for a, line, n in TOP_OF:
        here = slice(line, line + n)
        for j in range(tiles):
            lanes = slice(j * LANES, (j + 1) * LANES)
            if a == 1:
                up, low = lab_t[j, HALO : HALO + n, :], lab_t[j, HALO + rows - n : HALO + rows, :]
            else:
                up, low = refs[a][0, :n, lanes], refs[a][0, rows - n :, lanes]
            up, low = up.astype(jnp.float32), low.astype(jnp.float32)
            first[here, lanes], second[here, lanes] = ordered("row", up, low)
        lanes = slice(tiles * LANES, (tiles + 1) * LANES)
        first[here, lanes], second[here, lanes] = ordered("row", top[a][:n], bottom[a][LANES - n :])


def shifted(tiles, lane, by):
    count = len(tiles)
    turned = [turn(t, by) for t in tiles]
    if by > 0:
        return [jnp.where(lane == 0, turned[j - 1], turned[j]) for j in range(count)]
    return [jnp.where(lane == LANES - 1, turned[(j + 1) % count], turned[j]) for j in range(count)]


SCALE = 2.0 / RADIUS


def decode(code, lab, lab_r, lab_l, lab_d, lab_u, prior, weight):
    r = (code & 1).astype(jnp.float32)
    l = ((code >> 1) & 1).astype(jnp.float32)
    d = ((code >> 2) & 1).astype(jnp.float32)
    u = ((code >> 3) & 1).astype(jnp.float32)
    free = lab == 0
    one = jnp.where(free, SCALE, 0.0)
    near = (
        jnp.where(lab_r == 1, r, 0.0)
        + jnp.where(lab_l == 1, l, 0.0)
        + jnp.where(lab_d == 1, d, 0.0)
        + jnp.where(lab_u == 1, u, 0.0)
    )
    return (
        jnp.where(lab_r == 0, one, 0.0) * r,
        one * d,
        one * u,
        SCALE * ((r + l + d + u) + weight - CENTRE),
        jnp.where(free, weight * prior + near, 0.0),
    )


def decode_row(lane, code, lab, lab_d, lab_u, prior, weight):
    lab_r, lab_l = shifted(lab, lane, -1), shifted(lab, lane, 1)
    return list(zip(*map(decode, code, lab, lab_r, lab_l, lab_d, lab_u, prior, weight)))


def prepare(edges, labels, prior, weight, lab_t, *terms):
    rows, cols = edges.shape[1], edges.shape[2]
    tiles = cols // LANES
    lane = lane_ids(8)
    seeds = jnp.full((8, LANES), 2, jnp.int32)
    for j in range(tiles):
        lab_t[j, :HALO, :] = seeds
        lab_t[j, HALO + rows :, :] = seeds

    def lay(i, _):
        s = pl.multiple_of(8 * i, 8)
        for j in range(tiles):
            lab_t[j, pl.ds(s + HALO, 8), :] = labels[0, pl.ds(s, 8), j * LANES : (j + 1) * LANES]
        return 0

    lax.fori_loop(0, rows // 8, lay, 0, unroll=16)

    def body(i, _):
        s = pl.multiple_of(8 * i, 8)
        read = lambda ref: [ref[0, pl.ds(s, 8), j * LANES : (j + 1) * LANES] for j in range(tiles)]
        near = lambda at: [lab_t[j, pl.ds(at, 8), :] for j in range(tiles)]
        lab = near(pl.multiple_of(s + HALO, 8))
        lab_r, lab_l = (shifted(lab + [seeds], lane, by)[:tiles] for by in (-1, 1))
        done = map(
            decode, read(edges), lab, lab_r, lab_l, near(s + HALO + 1), near(s + HALO - 1),
            read(prior), read(weight),
        )
        for j, values in enumerate(done):
            for ref, value in zip(terms, values):
                ref[j, pl.ds(s, 8), :] = value
        return 0

    lax.fori_loop(0, rows // 8, body, 0, unroll=8)


def recurrence(lane, k, v, v_d, v_u, before, er, ed, eu, diag):
    v_r = shifted(v, lane, -1)
    g = shifted([er[j] * v[j] for j in range(len(v))], lane, 1)
    new = []
    for j in range(len(v)):
        x = diag[j] * v[j] - (er[j] * v_r[j] + g[j])
        x = x - (ed[j] * v_d[j] + eu[j] * v_u[j])
        new.append(0.5 * x if k == 0 else x - before[j])
    return new


def summed(a, b):
    t = [x * y for x, y in zip(a, b)]
    while len(t) > 1:
        t = [t[q] + t[q + 1] for q in range(0, len(t) - 1, 2)] + ([t[-1]] if len(t) % 2 else [])
    return t[0]


def interior(edges, lab_t, col_first, col_second, *refs):
    refs = refs[5:]
    (er_t, ed_t, eu_t, diag_t), field, side_lab, sums = refs[:4], refs[4:13], refs[13], refs[14]
    side_code, side_prior, side_weight = refs[15:]
    rows = edges.shape[1]
    inner = lab_t.shape[0]
    tiles = inner + 1
    lane = lane_ids(8)
    for at in range(0, rows, LANES):
        side = side_tiles(col_first, col_second, at)
        side_code[at : at + LANES, :] = side[0].astype(jnp.int32)
        side_lab[HALO + at : HALO + at + LANES, :] = side[1].astype(jnp.int32)
        side_prior[at : at + LANES, :] = side[2]
        side_weight[at : at + LANES, :] = side[3]
    seeds = jnp.full((HALO, LANES), 2, jnp.int32)
    side_lab[:HALO, :] = seeds
    side_lab[HALO + rows :, :] = seeds
    zero = jnp.zeros((8, LANES), jnp.float32)
    for k in range(1, ITERS):
        for j in range(tiles):
            field[k][j, :8, :] = zero
            field[k][j, rows - 8 :, :] = zero
    end = inner - 1

    def sides(i, _):
        s = pl.multiple_of(8 * i, 8)
        here, there = pl.ds(s, 8), pl.ds(pl.multiple_of(s + HALO, 8), 8)
        lab, lab_0, lab_end = side_lab[there, :], lab_t[0, there, :], lab_t[end, there, :]
        lab_r, lab_l = turn(lab, -1), turn(lab, 1)
        values = decode(
            side_code[here, :], lab,
            jnp.where(lane == LANES - 1, turn(lab_0, -1), lab_r),
            jnp.where(lane == 0, turn(lab_end, 1), lab_l),
            side_lab[pl.ds(s + HALO + 1, 8), :], side_lab[pl.ds(s + HALO - 1, 8), :],
            side_prior[here, :], side_weight[here, :],
        )
        for ref, value in zip((er_t, ed_t, eu_t, diag_t, field[0]), values):
            ref[inner, here, :] = value
        left = (lane == 0) & (lab_0 == 0) & ((edges[0, here, :LANES] & 2) != 0)
        field[0][0, here, :] += jnp.where(left & (lab_l == 1), 1.0, 0.0)
        right = (lane == LANES - 1) & (lab_end == 0) & ((edges[0, here, end * LANES :] & 1) != 0)
        field[0][end, here, :] += jnp.where(right & (lab_r == 1), 1.0, 0.0)
        er_t[end, here, :] += jnp.where(right & (lab_r == 0), SCALE, 0.0)
        return 0

    lax.fori_loop(0, rows // 8, sides, 0, unroll=16)

    def at_rows(ref, s):
        return [ref[j, pl.ds(s, 8), :] for j in range(tiles)]

    def advance(k, s):
        v = at_rows(field[k], s)
        new = recurrence(
            lane, k, v, at_rows(field[k], s + 1), at_rows(field[k], s - 1),
            at_rows(field[k - 1], s) if k else None,
            at_rows(er_t, s), at_rows(ed_t, s), at_rows(eu_t, s), at_rows(diag_t, s),
        )
        for j in range(tiles):
            field[k + 1][j, pl.ds(s, 8), :] = new[j]
        return v[:inner], new[:inner]

    count = 0
    for k in range(ITERS):
        last = k == ITERS - 1

        def body(i, carry, k=k, last=last):
            v, new = advance(k, pl.multiple_of(2 * HALO + 8 * i, 8))
            pairs = [(v, v), (v, new)] + ([(new, new)] if last else [])
            return tuple(acc + summed(a, b) for acc, (a, b) in zip(carry, pairs))

        if not last:
            advance(k, 8)
            advance(k, rows - 16)
        acc = (zero,) * (3 if last else 2)
        acc = lax.fori_loop(0, (rows - 4 * HALO) // 8, body, acc, unroll=60)
        for value in acc:
            sums[count] = value
            count += 1


def band(*refs):
    n = ITERS
    field, (er_t, ed_t, eu_t, diag_t, lab_t, side_lab) = refs[:n], refs[n : n + 6]
    sums, row_first, row_second = refs[n + 6 : n + 9]
    out, edge, labs, grid = refs[n + 9 :]
    inner, rows = lab_t.shape[0], er_t.shape[1]
    tiles = inner + 1
    lane = lane_ids(8)
    sub = lax.broadcasted_iota(jnp.int32, (8, LANES), 0)
    zero = jnp.zeros((8, LANES), jnp.float32)

    def lab_own(first):
        return [lab_t[j, HALO + first : HALO + first + 8, :] for j in range(inner)] + [
            side_lab[HALO + first : HALO + first + 8, :]
        ]

    def own(ref, first):
        return [ref[j, first : first + 8, :] for j in range(tiles)]

    terms = []
    for end, first in enumerate((0, rows - 8)):
        def line(at, count=8, end=end):
            both = [
                ordered("row", row_second[at : at + count, lanes], row_first[at : at + count, lanes])
                for lanes in (slice(j * LANES, (j + 1) * LANES) for j in range(tiles))
            ]
            return [pair[1 - end] for pair in both]

        beyond, mine = (0, 16) if end == 0 else (8, 0)
        for j, (x, y) in enumerate(zip(line(24, 16), lab_own(first))):
            labs[end, j, beyond : beyond + 16, :] = x.astype(jnp.int32)
            labs[end, j, mine : mine + 8, :] = y
        near = lambda at: [labs[end, j, at : at + 8, :] for j in range(tiles)]
        *halo, rhs = decode_row(
            lane, [x.astype(jnp.int32) for x in line(0)], near(8), near(9), near(7), line(8), line(16)
        )
        if end == 0:
            add = [jnp.where((sub == 0) & (x == 1) & (c > 0.0), 1.0, 0.0) for x, c in zip(near(15), own(eu_t, 0))]
        else:
            add = [jnp.where((sub == 7) & (x == 1) & (c > 0.0), 1.0, 0.0) for x, c in zip(near(1), own(ed_t, first))]
        outer = [x + y for x, y in zip(own(field[0], first), add)]
        step = 8 if end == 0 else -8
        next_in = own(field[0], first + step)
        coefficient = [[own(ref, f) for ref in (er_t, ed_t, eu_t, diag_t)] for f in (first, first + step)]
        trio = [(halo, rhs), (coefficient[0], outer), (coefficient[1], next_in)]
        if end == 1:
            trio.reverse()
        terms.append([t[0] for t in trio])
        for q, (_, start) in enumerate(trio):
            for j in range(tiles):
                grid[end, 0, j, 8 + 8 * q : 16 + 8 * q, :] = start[j]
        guard, inside, take = (0, 32, 16) if end == 0 else (32, 0, rows - 24)
        for k in range(ITERS):
            for j in range(tiles):
                grid[end, k, j, guard : guard + 8, :] = zero
                grid[end, k, j, inside : inside + 8, :] = field[k][j, take : take + 8, :]

    parts = [sums[q] for q in range(2 * ITERS + 1)]
    for k in range(ITERS):
        for end in range(2):
            at = lambda kk, s: [grid[end, kk, j, s : s + 8, :] for j in range(tiles)]
            for q in range(3):
                s = 8 + 8 * q
                v = at(k, s)
                new = recurrence(
                    lane, k, v, at(k, s + 1), at(k, s - 1), at(k - 1, s) if k else None, *terms[end][q]
                )
                for j in range(tiles):
                    grid[end, k + 1, j, s : s + 8, :] = new[j]
                mine = q - 1 if end == 0 else q
                if 0 <= mine < 2:
                    v, new = v[:inner], new[:inner]
                    parts[2 * k] = parts[2 * k] + summed(v, v)
                    parts[2 * k + 1] = parts[2 * k + 1] + summed(v, new)
                    for j in range(inner):
                        edge[k, end, j, 8 * mine : 8 * mine + 8, :] = v[j]
                    if k == ITERS - 1:
                        parts[2 * k + 2] = parts[2 * k + 2] + summed(new, new)
                        for j in range(inner):
                            edge[k + 1, end, j, 8 * mine : 8 * mine + 8, :] = new[j]

    every = jnp.zeros((1, LANES), jnp.float32)
    for q, acc in enumerate(parts):
        one = jnp.sum(jnp.sum(acc, axis=0, keepdims=True), axis=1, keepdims=True)
        every = jnp.where(lane_ids(1) == q, one, every)
    out[...] = jnp.broadcast_to(every[None], out.shape)


def coefficients(dots):
    n = ITERS
    inv = 1.0 / dots[0]
    moment = [jnp.ones_like(dots[0]), dots[1] * inv]
    for k in range(1, n + 1):
        moment.append(2.0 * (dots[2 * k] * inv) - moment[0])
        if k < n:
            moment.append(2.0 * (dots[2 * k + 1] * inv) - moment[1])
    gram = [[0.5 * (moment[i + j] + moment[abs(i - j)]) for j in range(n + 1)] for i in range(n + 1)]

    def image(p):
        q = [CENTRE * x for x in p] + [jnp.zeros_like(p[0])]
        for i, x in enumerate(p):
            if i == 0:
                q[1] = q[1] + RADIUS * x
            else:
                q[i + 1] = q[i + 1] + (RADIUS / 2) * x
                q[i - 1] = q[i - 1] + (RADIUS / 2) * x
        return q

    def product(a, b):
        sums = None
        for i, x in enumerate(a):
            t = gram[i][0] * b[0]
            for j in range(1, len(b)):
                t = t + gram[i][j] * b[j]
            sums = x * t if sums is None else sums + x * t
        return sums

    zero = jnp.zeros_like(inv)
    x, r, p = [], [moment[0]], [moment[0]]
    now = moment[0]
    for _ in range(n):
        q = image(p)
        alpha = now / product(p, q)
        x = [(x[i] if i < len(x) else zero) + alpha * p[i] for i in range(len(p))]
        r = [(r[i] if i < len(r) else zero) - alpha * q[i] for i in range(len(q))]
        following = product(r, r)
        beta = following / now
        p = [r[i] + (beta * p[i] if i < len(p) else zero) for i in range(len(r))]
        now = following
    size = zero
    for i in range(n + 1):
        size = size + jnp.abs(r[i]) * jnp.sqrt(jnp.maximum(gram[i][i], 0.0))
    good = (size * size <= (AMPLIFICATION * AMPLIFICATION) * now) & (now > 0.0)
    return x, r, good


def combine(every, lab_t, edge, *refs):
    n = ITERS + 1
    field, (labeling, residual, flag, sol_s, res_s, sem) = refs[:n], refs[n:]
    inner, rows = field[0].shape[0] - 1, field[0].shape[1]
    g = jnp.sum(every[:, 0, :], axis=0, keepdims=True)
    dots = [jnp.broadcast_to(g[:, q : q + 1], (8, LANES)) for q in range(2 * ITERS + 1)]
    x, r, good = coefficients(dots)
    flag[0, 0] = jnp.min(good.astype(jnp.int32))

    def put(s, source):
        for j in range(inner):
            lanes = slice(j * LANES, (j + 1) * LANES)
            sol = jnp.where(lab_t[j, pl.ds(s + HALO, 8), :] == 1, 1.0, 0.0)
            res = None
            for k in range(n):
                t = source(k, j)
                res = r[k] * t if res is None else res + r[k] * t
                if k < ITERS:
                    sol = sol + x[k] * t
            sol_s[pl.ds(s, 8), lanes] = sol
            res_s[pl.ds(s, 8), lanes] = res

    def body(i, _):
        s = pl.multiple_of(8 * i, 8)
        put(s, lambda k, j: field[k][j, pl.ds(s, 8), :])
        return 0

    copies = []
    chunk = 128
    for c in range(rows // chunk):
        first, last = c * chunk // 8, (c + 1) * chunk // 8
        if c == 0:
            for q in range(2):
                put(8 * q, lambda k, j: edge[k, 0, j, 8 * q : 8 * q + 8, :])
            first += 2
        if (c + 1) * chunk == rows:
            last -= 2
        lax.fori_loop(first, last, body, 0, unroll=(last - first) // 2)
        if (c + 1) * chunk == rows:
            for q in range(2):
                put(rows - 16 + 8 * q, lambda k, j: edge[k, 1, j, 8 * q : 8 * q + 8, :])
        at = pl.ds(c * chunk, chunk)
        for q, (src, dst) in enumerate(((sol_s, labeling), (res_s, residual))):
            copy = pltpu.make_async_copy(src.at[at, :], dst.at[0, at, :], sem.at[c, q])
            copy.start()
            copies.append(copy)
    for copy in copies:
        copy.wait()


def swaps(axis, first, second, around):
    count = lax.axis_size(axis)
    pairs = [(i, i + 1) for i in range(0, count - 1, 2)]
    others = [(i, i + 1) for i in range(1, count - 1, 2)] + ([(count - 1, 0)] if around else [])
    both = lambda p: [(a, b) for a, b in p] + [(b, a) for a, b in p]
    return lax.ppermute(first, axis, both(pairs)), lax.ppermute(second, axis, both(others))


def call(body, in_specs, outs, scratch, mib, flops, operands, out_specs=None, aliases={}):
    return pl.pallas_call(
        body,
        in_specs=in_specs,
        out_specs=out_specs or [VMEM] * len(outs),
        out_shape=outs,
        scratch_shapes=scratch,
        input_output_aliases=aliases,
        compiler_params=pltpu.CompilerParams(vmem_limit_bytes=mib * 1024 * 1024),
        cost_estimate=pl.CostEstimate(flops=flops, bytes_accessed=1 << 20, transcendentals=0),
    )(*operands)


def per_device(edges, labels, prior, data_weight):
    arrays = (edges, labels, prior, data_weight)
    _, rows, cols = edges.shape
    f32, i32 = jnp.float32, jnp.int32
    shape = jax.ShapeDtypeStruct
    inner = cols // LANES
    tiles = inner + 1
    dma = pltpu.SemaphoreType.DMA

    col_messages = call(
        col_pack, [HBM] * 4, [shape((LINES, rows), f32)] * 2,
        [
            pltpu.VMEM((2, 2, rows, LANES), i32),
            pltpu.VMEM((2, 2, rows, LANES), f32),
            dma((2, 4)),
        ],
        6, 1 << 20, arrays,
    )
    col_first, col_second = swaps("col", *col_messages, True)

    n = ITERS + 1
    whole = shape((tiles, rows, LANES), f32)
    lab_t, *terms = call(
        prepare, [VMEM] * 4, [shape((inner, rows + 2 * HALO, LANES), i32)] + [whole] * 5, [],
        6, 1 << 24, arrays,
    )
    row_messages = call(
        row_pack, [VMEM] * 6, [shape((LINES, tiles * LANES), f32)] * 2, [],
        4, 1 << 20, (edges, lab_t, prior, data_weight, col_first, col_second),
    )
    row_first, row_second = swaps("row", *row_messages, False)

    out = call(
        interior, [VMEM] * 9,
        [whole] * (4 + n)
        + [shape((rows + 2 * HALO, LANES), i32), shape((2 * ITERS + 1, 8, LANES), f32)],
        [pltpu.VMEM((rows, LANES), i32), pltpu.VMEM((rows, LANES), f32), pltpu.VMEM((rows, LANES), f32)],
        16, 1 << 26, (edges, lab_t, col_first, col_second, *terms),
        aliases={4 + q: q for q in range(5)},
    )
    terms, field, side_lab, sums = out[:4], out[4 : 4 + n], out[4 + n], out[5 + n]
    group = lax.axis_size(("row", "col"))
    sums, edge = call(
        band, [VMEM] * (ITERS + 9),
        [shape((group, 1, LANES), f32), shape((n, 2, inner, 2 * HALO, LANES), f32)],
        [pltpu.VMEM((2, tiles, 24, LANES), i32), pltpu.VMEM((2, n, tiles, 40, LANES), f32)],
        6, 1 << 20, (*field[:ITERS], *terms, lab_t, side_lab, sums, row_first, row_second),
    )
    every = lax.all_to_all(sums, ("row", "col"), 0, 0, tiled=True)

    labeling, residual, flag = call(
        combine, [VMEM] * (n + 3),
        [shape(edges.shape, f32)] * 2 + [shape((1, 1), i32)],
        [pltpu.VMEM((rows, cols), f32)] * 2 + [dma((rows // 128, 2))],
        4, 1 << 20, (every, lab_t, edge, *field), out_specs=[ANY, ANY, pl.BlockSpec(memory_space=pltpu.SMEM)],
    )

    def again(carry):
        return (jnp.int32(1), *plain(edges, labels, prior, data_weight))

    _, labeling, residual = lax.while_loop(
        lambda carry: carry[0] == 0, again, (flag[0, 0], labeling, residual)
    )
    return labeling, residual


def solution(mesh):
    spec = P("img", "row", "col")
    return jax.shard_map(
        per_device, mesh=mesh, in_specs=(spec,) * 4, out_specs=(spec,) * 2, check_vma=False
    )
```

```python
import functools
import jax
import jax.numpy as jnp
from jax import lax
from jax.experimental import pallas as pl
from jax.experimental.pallas import tpu as pltpu
from jax.sharding import PartitionSpec as P

ITERS = 8
HALO = 8
LANES = 128
LOW, HIGH = 0.05, 7.5
CENTRE, RADIUS = (HIGH + LOW) / 2, (HIGH - LOW) / 2
AMPLIFICATION = 24.0
VMEM = pl.BlockSpec(memory_space=pltpu.VMEM)
ANY = pl.BlockSpec(memory_space=pl.ANY)
HBM = pl.BlockSpec(memory_space=pltpu.HBM)


def with_halo(array, sides, width):
    edges = {}
    for axis, dim in sides:
        count, length = (lax.axis_size(axis), array.shape[dim])
        up = [(i, (i + 1) % count) for i in range(count - 1)]
        last = lax.slice_in_dim(array, length - width, length, axis=dim)
        first = lax.slice_in_dim(array, 0, width, axis=dim)
        edges[dim] = (
            lax.ppermute(last, axis, up),
            lax.ppermute(first, axis, [(b, a) for a, b in up]),
        )
    done = []
    for _, dim in sides:
        low, high = edges[dim]
        around = [(width, width) if d in done else (0, 0) for d in range(array.ndim)]
        array = jnp.concatenate([jnp.pad(low, around), array, jnp.pad(high, around)], axis=dim)
        done.append(dim)
    return array


def total(value, axis):
    count = lax.axis_size(axis)
    flat = value.reshape(1, 1, 1)
    every = lax.all_to_all(jnp.broadcast_to(flat, (count, 1, 1)), axis, 0, 0, tiled=True)
    return every.sum()


def neighbours(field, right, left, down, upper):
    padded = with_halo(field, (("row", 1), ("col", 2)), 1)
    return (
        right * padded[:, 1:-1, 2:]
        + left * padded[:, 1:-1, :-2]
        + down * padded[:, 2:, 1:-1]
        + upper * padded[:, :-2, 1:-1]
    )


def plain(edges, labels, prior, data_weight):
    right = (edges % 2).astype(jnp.float32)
    left = (edges // 2 % 2).astype(jnp.float32)
    down = (edges // 4 % 2).astype(jnp.float32)
    upper = (edges // 8 % 2).astype(jnp.float32)
    degree = right + left + down + upper
    free = (labels == 0).astype(jnp.float32)
    anchor = (labels == 1).astype(jnp.float32)
    diag_term = degree + data_weight

    def nearby(field):
        return neighbours(field, right, left, down, upper)

    rhs = free * (data_weight * prior + nearby(anchor))

    def step(_, carry):
        result, residual, direction, norm_now = carry
        image_v = free * (diag_term * direction - nearby(direction))
        alpha = norm_now / total(jnp.sum(direction * image_v), ("row", "col"))
        result = result + alpha * direction
        residual = residual - alpha * image_v
        norm_next = total(jnp.sum(residual * residual), ("row", "col"))
        direction = residual + (norm_next / norm_now) * direction
        return result, residual, direction, norm_next

    start = (jnp.zeros_like(rhs), rhs, rhs, total(jnp.sum(rhs * rhs), ("row", "col")))
    result, residual, _, _ = lax.fori_loop(0, ITERS, step, start)
    return anchor + result, residual


WIDTH = HALO + 1
LINES = 40
SLOTS = ((0, 0, 8), (2, 8, 8), (3, 16, 8), (1, 24, 16))


def lane_ids(rows):
    return lax.broadcasted_iota(jnp.int32, (rows, LANES), 1)


def turn(x, by):
    return pltpu.roll(x, by % LANES, 1) if by % LANES else x


def col_pack(edges, labels, prior, weight, first, second, lab_t, ints, floats, sem):
    rows, cols = edges.shape[1], edges.shape[2]
    tiles = cols // LANES
    lane = lane_ids(LANES)
    pairs = []
    for side in range(2):
        at = pl.ds(side * (cols - LANES), LANES)
        pairs.append((edges.at[0, :, at], ints.at[side]))
        pairs.append((prior.at[0, :, at], floats.at[side, 0]))
        pairs.append((weight.at[0, :, at], floats.at[side, 1]))
    for j in (0, tiles - 1, *range(1, tiles - 1)):
        pairs.append((labels.at[0, :, pl.ds(j * LANES, LANES)], lab_t.at[j, pl.ds(HALO, rows), :]))
    copies = [pltpu.make_async_copy(*pair, sem.at[q]) for q, pair in enumerate(pairs)]
    for copy in copies:
        copy.start()
    seeds = jnp.full((HALO, LANES), 2, jnp.int32)
    for j in range(tiles):
        lab_t[j, :HALO, :] = seeds
        lab_t[j, HALO + rows :, :] = seeds
    for copy in copies[:8]:
        copy.wait()
    for chunk in range(rows // LANES):
        at = slice(chunk * LANES, (chunk + 1) * LANES)
        lines = []
        for side in range(2):
            labs = lab_t[side * (tiles - 1), HALO + chunk * LANES : HALO + (chunk + 1) * LANES, :]
            packed = None
            for x, (_, line, n) in zip((ints[side, at, :], floats[side, 0, at, :], floats[side, 1, at, :], labs), SLOTS):
                x = turn(x.astype(jnp.float32), line + side * n)
                packed = x if packed is None else jnp.where(lane < line, packed, x)
            lines.append(jnp.swapaxes(packed, 0, 1)[:LINES])
        first[:, at], second[:, at] = ordered("col", *lines)
    for copy in copies[8:]:
        copy.wait()


def ordered(axis, before, after):
    even = lax.axis_index(axis) % 2 == 0
    return jnp.where(even, after, before), jnp.where(even, before, after)


def side_tiles(first, second, at):
    right, left = ordered("col", second[:, at : at + LANES], first[:, at : at + LANES])
    both = []
    for _, line, n in SLOTS:
        both += [left[line : line + n], right[line : line + n]]
    both.append(jnp.zeros((LANES - 2 * LINES, LANES), jnp.float32))
    both = jnp.swapaxes(jnp.concatenate(both, 0), 0, 1)
    lane = lane_ids(LANES)
    tiles = {}
    for a, line, n in SLOTS:
        width, outside = (WIDTH, 2.0) if a == 1 else (HALO, 0.0)
        inside = (lane < width) | (lane >= LANES - width)
        tiles[a] = jnp.where(inside, turn(both, -(2 * line + n)), outside)
    return tiles


def row_pack(edges, lab_t, prior, weight, col_first, col_second, after, first, second):
    del after
    rows, cols = edges.shape[1], edges.shape[2]
    tiles = cols // LANES
    refs = (edges, None, prior, weight)
    top = side_tiles(col_first, col_second, 0)
    bottom = side_tiles(col_first, col_second, rows - LANES)
    for a, line, n in SLOTS:
        here = slice(line, line + n)
        for j in range(tiles):
            lanes = slice(j * LANES, (j + 1) * LANES)
            if a == 1:
                up, low = lab_t[j, HALO : HALO + n, :], lab_t[j, HALO + rows - n : HALO + rows, :]
            else:
                up, low = refs[a][0, :n, lanes], refs[a][0, rows - n :, lanes]
            up, low = up.astype(jnp.float32), low.astype(jnp.float32)
            first[here, lanes], second[here, lanes] = ordered("row", up, low)
        lanes = slice(tiles * LANES, (tiles + 1) * LANES)
        first[here, lanes], second[here, lanes] = ordered("row", top[a][:n], bottom[a][LANES - n :])


def shifted(tiles, lane, by):
    count = len(tiles)
    turned = [turn(t, by) for t in tiles]
    if by > 0:
        return [jnp.where(lane == 0, turned[j - 1], turned[j]) for j in range(count)]
    return [jnp.where(lane == LANES - 1, turned[(j + 1) % count], turned[j]) for j in range(count)]


SCALE = 2.0 / RADIUS


def decode(code, lab, lab_r, lab_l, lab_d, lab_u, prior, weight):
    r = (code & 1).astype(jnp.float32)
    l = ((code >> 1) & 1).astype(jnp.float32)
    d = ((code >> 2) & 1).astype(jnp.float32)
    u = ((code >> 3) & 1).astype(jnp.float32)
    free = lab == 0
    one = jnp.where(free, SCALE, 0.0)
    near = (
        jnp.where(lab_r == 1, r, 0.0)
        + jnp.where(lab_l == 1, l, 0.0)
        + jnp.where(lab_d == 1, d, 0.0)
        + jnp.where(lab_u == 1, u, 0.0)
    )
    return (
        jnp.where(lab_r == 0, one, 0.0) * r,
        one * d,
        one * u,
        SCALE * ((r + l + d + u) + weight - CENTRE),
        jnp.where(free, weight * prior + near, 0.0),
    )


def decode_row(lane, code, lab, lab_d, lab_u, prior, weight):
    lab_r, lab_l = shifted(lab, lane, -1), shifted(lab, lane, 1)
    return list(zip(*map(decode, code, lab, lab_r, lab_l, lab_d, lab_u, prior, weight)))


def prepare(edges, lab_t, prior, weight, *terms):
    rows, cols = edges.shape[1], edges.shape[2]
    tiles = cols // LANES
    lane = lane_ids(8)
    seeds = jnp.full((8, LANES), 2, jnp.int32)

    def body(i, _):
        s = pl.multiple_of(8 * i, 8)
        read = lambda ref: [ref[0, pl.ds(s, 8), j * LANES : (j + 1) * LANES] for j in range(tiles)]
        near = lambda at: [lab_t[j, pl.ds(at, 8), :] for j in range(tiles)]
        lab = near(pl.multiple_of(s + HALO, 8))
        lab_r, lab_l = (shifted(lab + [seeds], lane, by)[:tiles] for by in (-1, 1))
        done = map(
            decode, read(edges), lab, lab_r, lab_l, near(s + HALO + 1), near(s + HALO - 1),
            read(prior), read(weight),
        )
        for j, values in enumerate(done):
            for ref, value in zip(terms, values):
                ref[j, pl.ds(s, 8), :] = value
        return 0

    lax.fori_loop(0, rows // 8, body, 0, unroll=8)


def recurrence(lane, k, v, v_d, v_u, before, er, ed, eu, diag):
    v_r = shifted(v, lane, -1)
    g = shifted([er[j] * v[j] for j in range(len(v))], lane, 1)
    new = []
    for j in range(len(v)):
        x = diag[j] * v[j] - (er[j] * v_r[j] + g[j])
        x = x - (ed[j] * v_d[j] + eu[j] * v_u[j])
        new.append(0.5 * x if k == 0 else x - before[j])
    return new


def summed(a, b):
    t = [x * y for x, y in zip(a, b)]
    while len(t) > 1:
        t = [t[q] + t[q + 1] for q in range(0, len(t) - 1, 2)] + ([t[-1]] if len(t) % 2 else [])
    return t[0]


def interior(edges, lab_t, col_first, col_second, *refs):
    refs = refs[5:]
    (er_t, ed_t, eu_t, diag_t), field, side_lab, sums = refs[:4], refs[4:13], refs[13], refs[14]
    side_code, side_prior, side_weight = refs[15:]
    rows = edges.shape[1]
    inner = lab_t.shape[0]
    tiles = inner + 1
    lane = lane_ids(8)
    for at in range(0, rows, LANES):
        side = side_tiles(col_first, col_second, at)
        side_code[at : at + LANES, :] = side[0].astype(jnp.int32)
        side_lab[HALO + at : HALO + at + LANES, :] = side[1].astype(jnp.int32)
        side_prior[at : at + LANES, :] = side[2]
        side_weight[at : at + LANES, :] = side[3]
    seeds = jnp.full((HALO, LANES), 2, jnp.int32)
    side_lab[:HALO, :] = seeds
    side_lab[HALO + rows :, :] = seeds
    zero = jnp.zeros((8, LANES), jnp.float32)
    for k in range(1, ITERS):
        for j in range(tiles):
            field[k][j, :8, :] = zero
            field[k][j, rows - 8 :, :] = zero
    end = inner - 1

    def sides(i, _):
        s = pl.multiple_of(8 * i, 8)
        here, there = pl.ds(s, 8), pl.ds(pl.multiple_of(s + HALO, 8), 8)
        lab, lab_0, lab_end = side_lab[there, :], lab_t[0, there, :], lab_t[end, there, :]
        lab_r, lab_l = turn(lab, -1), turn(lab, 1)
        values = decode(
            side_code[here, :], lab,
            jnp.where(lane == LANES - 1, turn(lab_0, -1), lab_r),
            jnp.where(lane == 0, turn(lab_end, 1), lab_l),
            side_lab[pl.ds(s + HALO + 1, 8), :], side_lab[pl.ds(s + HALO - 1, 8), :],
            side_prior[here, :], side_weight[here, :],
        )
        for ref, value in zip((er_t, ed_t, eu_t, diag_t, field[0]), values):
            ref[inner, here, :] = value
        left = (lane == 0) & (lab_0 == 0) & ((edges[0, here, :LANES] & 2) != 0)
        field[0][0, here, :] += jnp.where(left & (lab_l == 1), 1.0, 0.0)
        right = (lane == LANES - 1) & (lab_end == 0) & ((edges[0, here, end * LANES :] & 1) != 0)
        field[0][end, here, :] += jnp.where(right & (lab_r == 1), 1.0, 0.0)
        er_t[end, here, :] += jnp.where(right & (lab_r == 0), SCALE, 0.0)
        return 0

    lax.fori_loop(0, rows // 8, sides, 0, unroll=16)

    def at_rows(ref, s):
        return [ref[j, pl.ds(s, 8), :] for j in range(tiles)]

    def advance(k, s):
        v = at_rows(field[k], s)
        new = recurrence(
            lane, k, v, at_rows(field[k], s + 1), at_rows(field[k], s - 1),
            at_rows(field[k - 1], s) if k else None,
            at_rows(er_t, s), at_rows(ed_t, s), at_rows(eu_t, s), at_rows(diag_t, s),
        )
        for j in range(tiles):
            field[k + 1][j, pl.ds(s, 8), :] = new[j]
        return v[:inner], new[:inner]

    count = 0
    for k in range(ITERS):
        last = k == ITERS - 1

        def body(i, carry, k=k, last=last):
            v, new = advance(k, pl.multiple_of(2 * HALO + 8 * i, 8))
            pairs = [(v, v), (v, new)] + ([(new, new)] if last else [])
            return tuple(acc + summed(a, b) for acc, (a, b) in zip(carry, pairs))

        if not last:
            advance(k, 8)
            advance(k, rows - 16)
        acc = (zero,) * (3 if last else 2)
        acc = lax.fori_loop(0, (rows - 4 * HALO) // 8, body, acc, unroll=60)
        for value in acc:
            sums[count] = value
            count += 1


def band(*refs):
    n = ITERS
    field, (er_t, ed_t, eu_t, diag_t, lab_t, side_lab) = refs[:n], refs[n : n + 6]
    sums, row_first, row_second = refs[n + 6 : n + 9]
    out, edge, labs, grid = refs[n + 9 :]
    inner, rows = lab_t.shape[0], er_t.shape[1]
    tiles = inner + 1
    lane = lane_ids(8)
    sub = lax.broadcasted_iota(jnp.int32, (8, LANES), 0)
    zero = jnp.zeros((8, LANES), jnp.float32)

    def lab_own(first):
        return [lab_t[j, HALO + first : HALO + first + 8, :] for j in range(inner)] + [
            side_lab[HALO + first : HALO + first + 8, :]
        ]

    def own(ref, first):
        return [ref[j, first : first + 8, :] for j in range(tiles)]

    terms = []
    for end, first in enumerate((0, rows - 8)):
        def line(at, count=8, end=end):
            both = [
                ordered("row", row_second[at : at + count, lanes], row_first[at : at + count, lanes])
                for lanes in (slice(j * LANES, (j + 1) * LANES) for j in range(tiles))
            ]
            return [pair[1 - end] for pair in both]

        beyond, mine = (0, 16) if end == 0 else (8, 0)
        for j, (x, y) in enumerate(zip(line(24, 16), lab_own(first))):
            labs[end, j, beyond : beyond + 16, :] = x.astype(jnp.int32)
            labs[end, j, mine : mine + 8, :] = y
        near = lambda at: [labs[end, j, at : at + 8, :] for j in range(tiles)]
        *halo, rhs = decode_row(
            lane, [x.astype(jnp.int32) for x in line(0)], near(8), near(9), near(7), line(8), line(16)
        )
        if end == 0:
            add = [jnp.where((sub == 0) & (x == 1) & (c > 0.0), 1.0, 0.0) for x, c in zip(near(15), own(eu_t, 0))]
        else:
            add = [jnp.where((sub == 7) & (x == 1) & (c > 0.0), 1.0, 0.0) for x, c in zip(near(1), own(ed_t, first))]
        outer = [x + y for x, y in zip(own(field[0], first), add)]
        step = 8 if end == 0 else -8
        next_in = own(field[0], first + step)
        coefficient = [[own(ref, f) for ref in (er_t, ed_t, eu_t, diag_t)] for f in (first, first + step)]
        trio = [(halo, rhs), (coefficient[0], outer), (coefficient[1], next_in)]
        if end == 1:
            trio.reverse()
        terms.append([t[0] for t in trio])
        for q, (_, start) in enumerate(trio):
            for j in range(tiles):
                grid[end, 0, j, 8 + 8 * q : 16 + 8 * q, :] = start[j]
        guard, inside, take = (0, 32, 16) if end == 0 else (32, 0, rows - 24)
        for k in range(ITERS):
            for j in range(tiles):
                grid[end, k, j, guard : guard + 8, :] = zero
                grid[end, k, j, inside : inside + 8, :] = field[k][j, take : take + 8, :]

    parts = [sums[q] for q in range(2 * ITERS + 1)]
    for k in range(ITERS):
        for end in range(2):
            at = lambda kk, s: [grid[end, kk, j, s : s + 8, :] for j in range(tiles)]
            for q in range(3):
                s = 8 + 8 * q
                v = at(k, s)
                new = recurrence(
                    lane, k, v, at(k, s + 1), at(k, s - 1), at(k - 1, s) if k else None, *terms[end][q]
                )
                for j in range(tiles):
                    grid[end, k + 1, j, s : s + 8, :] = new[j]
                mine = q - 1 if end == 0 else q
                if 0 <= mine < 2:
                    v, new = v[:inner], new[:inner]
                    parts[2 * k] = parts[2 * k] + summed(v, v)
                    parts[2 * k + 1] = parts[2 * k + 1] + summed(v, new)
                    for j in range(inner):
                        edge[k, end, j, 8 * mine : 8 * mine + 8, :] = v[j]
                    if k == ITERS - 1:
                        parts[2 * k + 2] = parts[2 * k + 2] + summed(new, new)
                        for j in range(inner):
                            edge[k + 1, end, j, 8 * mine : 8 * mine + 8, :] = new[j]

    every = jnp.zeros((1, LANES), jnp.float32)
    for q, acc in enumerate(parts):
        one = jnp.sum(jnp.sum(acc, axis=0, keepdims=True), axis=1, keepdims=True)
        every = jnp.where(lane_ids(1) == q, one, every)
    out[...] = jnp.broadcast_to(every[None], out.shape)


def coefficients(dots):
    n = ITERS
    inv = 1.0 / dots[0]
    moment = [jnp.ones_like(dots[0]), dots[1] * inv]
    for k in range(1, n + 1):
        moment.append(2.0 * (dots[2 * k] * inv) - moment[0])
        if k < n:
            moment.append(2.0 * (dots[2 * k + 1] * inv) - moment[1])
    gram = [[0.5 * (moment[i + j] + moment[abs(i - j)]) for j in range(n + 1)] for i in range(n + 1)]

    def image(p):
        q = [CENTRE * x for x in p] + [jnp.zeros_like(p[0])]
        for i, x in enumerate(p):
            if i == 0:
                q[1] = q[1] + RADIUS * x
            else:
                q[i + 1] = q[i + 1] + (RADIUS / 2) * x
                q[i - 1] = q[i - 1] + (RADIUS / 2) * x
        return q

    def product(a, b):
        sums = None
        for i, x in enumerate(a):
            t = gram[i][0] * b[0]
            for j in range(1, len(b)):
                t = t + gram[i][j] * b[j]
            sums = x * t if sums is None else sums + x * t
        return sums

    zero = jnp.zeros_like(inv)
    x, r, p = [], [moment[0]], [moment[0]]
    now = moment[0]
    for _ in range(n):
        q = image(p)
        alpha = now / product(p, q)
        x = [(x[i] if i < len(x) else zero) + alpha * p[i] for i in range(len(p))]
        r = [(r[i] if i < len(r) else zero) - alpha * q[i] for i in range(len(q))]
        following = product(r, r)
        beta = following / now
        p = [r[i] + (beta * p[i] if i < len(p) else zero) for i in range(len(r))]
        now = following
    size = zero
    for i in range(n + 1):
        size = size + jnp.abs(r[i]) * jnp.sqrt(jnp.maximum(gram[i][i], 0.0))
    good = (size * size <= (AMPLIFICATION * AMPLIFICATION) * now) & (now > 0.0)
    return x, r, good


def combine(every, lab_t, edge, *refs):
    n = ITERS + 1
    field, (labeling, residual, flag, sol_s, res_s, sem) = refs[:n], refs[n:]
    inner, rows = field[0].shape[0] - 1, field[0].shape[1]
    g = jnp.sum(every[:, 0, :], axis=0, keepdims=True)
    dots = [jnp.broadcast_to(g[:, q : q + 1], (8, LANES)) for q in range(2 * ITERS + 1)]
    x, r, good = coefficients(dots)
    flag[0, 0] = jnp.min(good.astype(jnp.int32))

    def put(s, source):
        for j in range(inner):
            lanes = slice(j * LANES, (j + 1) * LANES)
            sol = jnp.where(lab_t[j, pl.ds(s + HALO, 8), :] == 1, 1.0, 0.0)
            res = None
            for k in range(n):
                t = source(k, j)
                res = r[k] * t if res is None else res + r[k] * t
                if k < ITERS:
                    sol = sol + x[k] * t
            sol_s[pl.ds(s, 8), lanes] = sol
            res_s[pl.ds(s, 8), lanes] = res

    def body(i, _):
        s = pl.multiple_of(8 * i, 8)
        put(s, lambda k, j: field[k][j, pl.ds(s, 8), :])
        return 0

    copies = []
    chunk = 128
    for c in range(rows // chunk):
        first, last = c * chunk // 8, (c + 1) * chunk // 8
        if c == 0:
            for q in range(2):
                put(8 * q, lambda k, j: edge[k, 0, j, 8 * q : 8 * q + 8, :])
            first += 2
        if (c + 1) * chunk == rows:
            last -= 2
        lax.fori_loop(first, last, body, 0, unroll=(last - first) // 2)
        if (c + 1) * chunk == rows:
            for q in range(2):
                put(rows - 16 + 8 * q, lambda k, j: edge[k, 1, j, 8 * q : 8 * q + 8, :])
        at = pl.ds(c * chunk, chunk)
        for q, (src, dst) in enumerate(((sol_s, labeling), (res_s, residual))):
            copy = pltpu.make_async_copy(src.at[at, :], dst.at[0, at, :], sem.at[c, q])
            copy.start()
            copies.append(copy)
    for copy in copies:
        copy.wait()


def swaps(axis, first, second, around):
    count = lax.axis_size(axis)
    pairs = [(i, i + 1) for i in range(0, count - 1, 2)]
    others = [(i, i + 1) for i in range(1, count - 1, 2)] + ([(count - 1, 0)] if around else [])
    both = lambda p: [(a, b) for a, b in p] + [(b, a) for a, b in p]
    return lax.ppermute(first, axis, both(pairs)), lax.ppermute(second, axis, both(others))


def call(body, in_specs, outs, scratch, mib, flops, operands, out_specs=None, aliases={}):
    return pl.pallas_call(
        body,
        in_specs=in_specs,
        out_specs=out_specs or [VMEM] * len(outs),
        out_shape=outs,
        scratch_shapes=scratch,
        input_output_aliases=aliases,
        compiler_params=pltpu.CompilerParams(vmem_limit_bytes=mib * 1024 * 1024),
        cost_estimate=pl.CostEstimate(flops=flops, bytes_accessed=1 << 20, transcendentals=0),
    )(*operands)


def per_device(edges, labels, prior, data_weight):
    arrays = (edges, labels, prior, data_weight)
    _, rows, cols = edges.shape
    f32, i32 = jnp.float32, jnp.int32
    shape = jax.ShapeDtypeStruct
    inner = cols // LANES
    tiles = inner + 1
    dma = pltpu.SemaphoreType.DMA

    *col_messages, lab_t = call(
        col_pack, [HBM] * 4,
        [shape((LINES, rows), f32)] * 2 + [shape((inner, rows + 2 * HALO, LANES), i32)],
        [
            pltpu.VMEM((2, rows, LANES), i32),
            pltpu.VMEM((2, 2, rows, LANES), f32),
            dma((6 + inner,)),
        ],
        6, 1 << 20, arrays,
    )
    col_first, col_second = swaps("col", *col_messages, True)

    n = ITERS + 1
    whole = shape((tiles, rows, LANES), f32)
    terms = call(
        prepare, [VMEM] * 4, [whole] * 5, [], 6, 1 << 24, (edges, lab_t, prior, data_weight),
    )
    row_messages = call(
        row_pack, [VMEM] * 7, [shape((LINES, tiles * LANES), f32)] * 2, [],
        4, 1 << 20, (edges, lab_t, prior, data_weight, col_first, col_second, terms[1]),
    )
    row_first, row_second = swaps("row", *row_messages, False)

    out = call(
        interior, [VMEM] * 9,
        [whole] * (4 + n)
        + [shape((rows + 2 * HALO, LANES), i32), shape((2 * ITERS + 1, 8, LANES), f32)],
        [pltpu.VMEM((rows, LANES), i32), pltpu.VMEM((rows, LANES), f32), pltpu.VMEM((rows, LANES), f32)],
        16, 1 << 26, (edges, lab_t, col_first, col_second, *terms),
        aliases={4 + q: q for q in range(5)},
    )
    terms, field, side_lab, sums = out[:4], out[4 : 4 + n], out[4 + n], out[5 + n]
    group = lax.axis_size(("row", "col"))
    sums, edge = call(
        band, [VMEM] * (ITERS + 9),
        [shape((group, 1, LANES), f32), shape((n, 2, inner, 2 * HALO, LANES), f32)],
        [pltpu.VMEM((2, tiles, 24, LANES), i32), pltpu.VMEM((2, n, tiles, 40, LANES), f32)],
        6, 1 << 20, (*field[:ITERS], *terms, lab_t, side_lab, sums, row_first, row_second),
    )
    every = lax.all_to_all(sums, ("row", "col"), 0, 0, tiled=True)

    labeling, residual, flag = call(
        combine, [VMEM] * (n + 3),
        [shape(edges.shape, f32)] * 2 + [shape((1, 1), i32)],
        [pltpu.VMEM((rows, cols), f32)] * 2 + [dma((rows // 128, 2))],
        4, 1 << 20, (every, lab_t, edge, *field), out_specs=[ANY, ANY, pl.BlockSpec(memory_space=pltpu.SMEM)],
    )

    def again(carry):
        return (jnp.int32(1), *plain(edges, labels, prior, data_weight))

    _, labeling, residual = lax.while_loop(
        lambda carry: carry[0] == 0, again, (flag[0, 0], labeling, residual)
    )
    return labeling, residual


def solution(mesh):
    spec = P("img", "row", "col")
    return jax.shard_map(
        per_device, mesh=mesh, in_specs=(spec,) * 4, out_specs=(spec,) * 2, check_vma=False
    )
```

```python
import functools
import jax
import jax.numpy as jnp
from jax import lax
from jax.experimental import pallas as pl
from jax.experimental.pallas import tpu as pltpu
from jax.sharding import PartitionSpec as P

ITERS = 8
HALO = 8
LANES = 128
LOW, HIGH = 0.05, 7.5
CENTRE, RADIUS = (HIGH + LOW) / 2, (HIGH - LOW) / 2
AMPLIFICATION = 24.0
VMEM = pl.BlockSpec(memory_space=pltpu.VMEM)
ANY = pl.BlockSpec(memory_space=pl.ANY)
HBM = pl.BlockSpec(memory_space=pltpu.HBM)


def with_halo(array, sides, width):
    edges = {}
    for axis, dim in sides:
        count, length = (lax.axis_size(axis), array.shape[dim])
        up = [(i, (i + 1) % count) for i in range(count - 1)]
        last = lax.slice_in_dim(array, length - width, length, axis=dim)
        first = lax.slice_in_dim(array, 0, width, axis=dim)
        edges[dim] = (
            lax.ppermute(last, axis, up),
            lax.ppermute(first, axis, [(b, a) for a, b in up]),
        )
    done = []
    for _, dim in sides:
        low, high = edges[dim]
        around = [(width, width) if d in done else (0, 0) for d in range(array.ndim)]
        array = jnp.concatenate([jnp.pad(low, around), array, jnp.pad(high, around)], axis=dim)
        done.append(dim)
    return array


def total(value, axis):
    count = lax.axis_size(axis)
    flat = value.reshape(1, 1, 1)
    every = lax.all_to_all(jnp.broadcast_to(flat, (count, 1, 1)), axis, 0, 0, tiled=True)
    return every.sum()


def neighbours(field, right, left, down, upper):
    padded = with_halo(field, (("row", 1), ("col", 2)), 1)
    return (
        right * padded[:, 1:-1, 2:]
        + left * padded[:, 1:-1, :-2]
        + down * padded[:, 2:, 1:-1]
        + upper * padded[:, :-2, 1:-1]
    )


def plain(edges, labels, prior, data_weight):
    right = (edges % 2).astype(jnp.float32)
    left = (edges // 2 % 2).astype(jnp.float32)
    down = (edges // 4 % 2).astype(jnp.float32)
    upper = (edges // 8 % 2).astype(jnp.float32)
    degree = right + left + down + upper
    free = (labels == 0).astype(jnp.float32)
    anchor = (labels == 1).astype(jnp.float32)
    diag_term = degree + data_weight

    def nearby(field):
        return neighbours(field, right, left, down, upper)

    rhs = free * (data_weight * prior + nearby(anchor))

    def step(_, carry):
        result, residual, direction, norm_now = carry
        image_v = free * (diag_term * direction - nearby(direction))
        alpha = norm_now / total(jnp.sum(direction * image_v), ("row", "col"))
        result = result + alpha * direction
        residual = residual - alpha * image_v
        norm_next = total(jnp.sum(residual * residual), ("row", "col"))
        direction = residual + (norm_next / norm_now) * direction
        return result, residual, direction, norm_next

    start = (jnp.zeros_like(rhs), rhs, rhs, total(jnp.sum(rhs * rhs), ("row", "col")))
    result, residual, _, _ = lax.fori_loop(0, ITERS, step, start)
    return anchor + result, residual


WIDTH = HALO + 1
LINES = 40
SLOTS = ((0, 0, 8), (2, 8, 8), (3, 16, 8), (1, 24, 16))


def lane_ids(rows):
    return lax.broadcasted_iota(jnp.int32, (rows, LANES), 1)


def turn(x, by):
    return pltpu.roll(x, by % LANES, 1) if by % LANES else x


def col_pack(edges, labels, prior, weight, first, second, lab_t, ints, floats, sem):
    rows, cols = edges.shape[1], edges.shape[2]
    tiles = cols // LANES
    lane = lane_ids(LANES)
    pairs = []
    for side in range(2):
        at = pl.ds(side * (cols - LANES), LANES)
        pairs.append((edges.at[0, :, at], ints.at[side]))
        pairs.append((prior.at[0, :, at], floats.at[side, 0]))
        pairs.append((weight.at[0, :, at], floats.at[side, 1]))
    for j in (0, tiles - 1, *range(1, tiles - 1)):
        pairs.append((labels.at[0, :, pl.ds(j * LANES, LANES)], lab_t.at[j, pl.ds(HALO, rows), :]))
    copies = [pltpu.make_async_copy(*pair, sem.at[q]) for q, pair in enumerate(pairs)]
    for copy in copies:
        copy.start()
    seeds = jnp.full((HALO, LANES), 2, jnp.int32)
    for j in range(tiles):
        lab_t[j, :HALO, :] = seeds
        lab_t[j, HALO + rows :, :] = seeds
    for copy in copies[:8]:
        copy.wait()
    for chunk in range(rows // LANES):
        at = slice(chunk * LANES, (chunk + 1) * LANES)
        lines = []
        for side in range(2):
            labs = lab_t[side * (tiles - 1), HALO + chunk * LANES : HALO + (chunk + 1) * LANES, :]
            packed = None
            for x, (_, line, n) in zip((ints[side, at, :], floats[side, 0, at, :], floats[side, 1, at, :], labs), SLOTS):
                x = turn(x.astype(jnp.float32), line + side * n)
                packed = x if packed is None else jnp.where(lane < line, packed, x)
            lines.append(jnp.swapaxes(packed, 0, 1)[:LINES])
        first[:, at], second[:, at] = ordered("col", *lines)
    for copy in copies[8:]:
        copy.wait()


def ordered(axis, before, after):
    even = lax.axis_index(axis) % 2 == 0
    return jnp.where(even, after, before), jnp.where(even, before, after)


def side_tiles(first, second, at):
    right, left = ordered("col", second[:, at : at + LANES], first[:, at : at + LANES])
    both = []
    for _, line, n in SLOTS:
        both += [left[line : line + n], right[line : line + n]]
    both.append(jnp.zeros((LANES - 2 * LINES, LANES), jnp.float32))
    both = jnp.swapaxes(jnp.concatenate(both, 0), 0, 1)
    lane = lane_ids(LANES)
    tiles = {}
    for a, line, n in SLOTS:
        width, outside = (WIDTH, 2.0) if a == 1 else (HALO, 0.0)
        inside = (lane < width) | (lane >= LANES - width)
        tiles[a] = jnp.where(inside, turn(both, -(2 * line + n)), outside)
    return tiles


def row_pack(edges, lab_t, prior, weight, col_first, col_second, after, first, second):
    del after
    rows, cols = edges.shape[1], edges.shape[2]
    tiles = cols // LANES
    refs = (edges, None, prior, weight)
    top = side_tiles(col_first, col_second, 0)
    bottom = side_tiles(col_first, col_second, rows - LANES)
    for a, line, n in SLOTS:
        here = slice(line, line + n)
        for j in range(tiles):
            lanes = slice(j * LANES, (j + 1) * LANES)
            if a == 1:
                up, low = lab_t[j, HALO : HALO + n, :], lab_t[j, HALO + rows - n : HALO + rows, :]
            else:
                up, low = refs[a][0, :n, lanes], refs[a][0, rows - n :, lanes]
            up, low = up.astype(jnp.float32), low.astype(jnp.float32)
            first[here, lanes], second[here, lanes] = ordered("row", up, low)
        lanes = slice(tiles * LANES, (tiles + 1) * LANES)
        first[here, lanes], second[here, lanes] = ordered("row", top[a][:n], bottom[a][LANES - n :])


def shifted(tiles, lane, by):
    count = len(tiles)
    turned = [turn(t, by) for t in tiles]
    if by > 0:
        return [jnp.where(lane == 0, turned[j - 1], turned[j]) for j in range(count)]
    return [jnp.where(lane == LANES - 1, turned[(j + 1) % count], turned[j]) for j in range(count)]


SCALE = 2.0 / RADIUS
SPARE = 24


def decode(code, lab, lab_r, lab_l, lab_d, lab_u, prior, weight):
    r = (code & 1).astype(jnp.float32)
    l = ((code >> 1) & 1).astype(jnp.float32)
    d = ((code >> 2) & 1).astype(jnp.float32)
    u = ((code >> 3) & 1).astype(jnp.float32)
    free = lab == 0
    one = jnp.where(free, SCALE, 0.0)
    near = (
        jnp.where(lab_r == 1, r, 0.0)
        + jnp.where(lab_l == 1, l, 0.0)
        + jnp.where(lab_d == 1, d, 0.0)
        + jnp.where(lab_u == 1, u, 0.0)
    )
    return (
        jnp.where(lab_r == 0, one, 0.0) * r,
        one * d,
        one * u,
        SCALE * ((r + l + d + u) + weight - CENTRE),
        jnp.where(free, weight * prior + near, 0.0),
    )


def decode_row(lane, code, lab, lab_d, lab_u, prior, weight):
    lab_r, lab_l = shifted(lab, lane, -1), shifted(lab, lane, 1)
    return list(zip(*map(decode, code, lab, lab_r, lab_l, lab_d, lab_u, prior, weight)))


def prepare(edges, lab_t, prior, weight, *terms):
    rows, cols = edges.shape[1], edges.shape[2]
    tiles = cols // LANES
    lane = lane_ids(8)
    seeds = jnp.full((8, LANES), 2, jnp.int32)

    def body(i, _):
        s = pl.multiple_of(8 * i, 8)
        read = lambda ref: [ref[0, pl.ds(s, 8), j * LANES : (j + 1) * LANES] for j in range(tiles)]
        near = lambda at: [lab_t[j, pl.ds(at, 8), :] for j in range(tiles)]
        lab = near(pl.multiple_of(s + HALO, 8))
        lab_r, lab_l = (shifted(lab + [seeds], lane, by)[:tiles] for by in (-1, 1))
        done = map(
            decode, read(edges), lab, lab_r, lab_l, near(s + HALO + 1), near(s + HALO - 1),
            read(prior), read(weight),
        )
        for j, values in enumerate(done):
            for ref, value in zip(terms, values):
                ref[j, pl.ds(s, 8), :] = value
        return 0

    lax.fori_loop(0, rows // 8, body, 0, unroll=8)


def recurrence(lane, k, v, v_d, v_u, before, er, ed, eu, diag):
    v_r = shifted(v, lane, -1)
    g = shifted([er[j] * v[j] for j in range(len(v))], lane, 1)
    new = []
    for j in range(len(v)):
        x = diag[j] * v[j] - (er[j] * v_r[j] + g[j])
        x = x - (ed[j] * v_d[j] + eu[j] * v_u[j])
        new.append(0.5 * x if k == 0 else x - before[j])
    return new


def summed(a, b):
    t = [x * y for x, y in zip(a, b)]
    while len(t) > 1:
        t = [t[q] + t[q + 1] for q in range(0, len(t) - 1, 2)] + ([t[-1]] if len(t) % 2 else [])
    return t[0]


def interior(edges, lab_t, col_first, col_second, *refs):
    refs = refs[5:]
    (er_t, ed_t, eu_t, diag_t), field, side_lab, sums = refs[:4], refs[4:13], refs[13], refs[14]
    side_code, side_prior, side_weight = refs[15:]
    rows = edges.shape[1]
    inner = lab_t.shape[0]
    tiles = inner + 1
    lane = lane_ids(8)
    for at in range(0, rows, LANES):
        side = side_tiles(col_first, col_second, at)
        side_code[at : at + LANES, :] = side[0].astype(jnp.int32)
        side_lab[HALO + at : HALO + at + LANES, :] = side[1].astype(jnp.int32)
        side_prior[at : at + LANES, :] = side[2]
        side_weight[at : at + LANES, :] = side[3]
    seeds = jnp.full((HALO, LANES), 2, jnp.int32)
    side_lab[:HALO, :] = seeds
    side_lab[HALO + rows :, :] = seeds
    zero = jnp.zeros((8, LANES), jnp.float32)
    for k in range(1, ITERS):
        for j in range(tiles):
            field[k][j, :8, :] = zero
            field[k][j, rows - 8 : rows, :] = zero
    end = inner - 1

    def sides(i, _):
        s = pl.multiple_of(8 * i, 8)
        here, there = pl.ds(s, 8), pl.ds(pl.multiple_of(s + HALO, 8), 8)
        lab, lab_0, lab_end = side_lab[there, :], lab_t[0, there, :], lab_t[end, there, :]
        lab_r, lab_l = turn(lab, -1), turn(lab, 1)
        values = decode(
            side_code[here, :], lab,
            jnp.where(lane == LANES - 1, turn(lab_0, -1), lab_r),
            jnp.where(lane == 0, turn(lab_end, 1), lab_l),
            side_lab[pl.ds(s + HALO + 1, 8), :], side_lab[pl.ds(s + HALO - 1, 8), :],
            side_prior[here, :], side_weight[here, :],
        )
        for ref, value in zip((er_t, ed_t, eu_t, diag_t, field[0]), values):
            ref[inner, here, :] = value
        left = (lane == 0) & (lab_0 == 0) & ((edges[0, here, :LANES] & 2) != 0)
        field[0][0, here, :] += jnp.where(left & (lab_l == 1), 1.0, 0.0)
        right = (lane == LANES - 1) & (lab_end == 0) & ((edges[0, here, end * LANES :] & 1) != 0)
        field[0][end, here, :] += jnp.where(right & (lab_r == 1), 1.0, 0.0)
        er_t[end, here, :] += jnp.where(right & (lab_r == 0), SCALE, 0.0)
        return 0

    lax.fori_loop(0, rows // 8, sides, 0, unroll=16)

    def at_rows(ref, s):
        return [ref[j, pl.ds(s, 8), :] for j in range(tiles)]

    def advance(k, s):
        v = at_rows(field[k], s)
        new = recurrence(
            lane, k, v, at_rows(field[k], s + 1), at_rows(field[k], s - 1),
            at_rows(field[k - 1], s) if k else None,
            at_rows(er_t, s), at_rows(ed_t, s), at_rows(eu_t, s), at_rows(diag_t, s),
        )
        for j in range(tiles):
            field[k + 1][j, pl.ds(s, 8), :] = new[j]
        return v[:inner], new[:inner]

    count = 0
    for k in range(ITERS):
        last = k == ITERS - 1

        def body(i, carry, k=k, last=last):
            v, new = advance(k, pl.multiple_of(2 * HALO + 8 * i, 8))
            pairs = [(v, v), (v, new)] + ([(new, new)] if last else [])
            return tuple(acc + summed(a, b) for acc, (a, b) in zip(carry, pairs))

        if not last:
            advance(k, 8)
            advance(k, rows - 16)
        acc = (zero,) * (3 if last else 2)
        acc = lax.fori_loop(0, (rows - 4 * HALO) // 8, body, acc, unroll=60)
        for value in acc:
            sums[count] = value
            count += 1


def band(*refs):
    n = ITERS
    field, (er_t, ed_t, eu_t, diag_t, lab_t, side_lab) = refs[:n], refs[n : n + 6]
    sums, row_first, row_second = refs[n + 6 : n + 9]
    out, edge, labs, grid = refs[n + 9 :]
    inner, rows = lab_t.shape[0], lab_t.shape[1] - 2 * HALO
    tiles = inner + 1
    lane = lane_ids(8)
    sub = lax.broadcasted_iota(jnp.int32, (8, LANES), 0)
    zero = jnp.zeros((8, LANES), jnp.float32)

    def lab_own(first):
        return [lab_t[j, HALO + first : HALO + first + 8, :] for j in range(inner)] + [
            side_lab[HALO + first : HALO + first + 8, :]
        ]

    def own(ref, first):
        return [ref[j, first : first + 8, :] for j in range(tiles)]

    terms = []
    for end, first in enumerate((0, rows - 8)):
        def line(at, count=8, end=end):
            both = [
                ordered("row", row_second[at : at + count, lanes], row_first[at : at + count, lanes])
                for lanes in (slice(j * LANES, (j + 1) * LANES) for j in range(tiles))
            ]
            return [pair[1 - end] for pair in both]

        beyond, mine = (0, 16) if end == 0 else (8, 0)
        for j, (x, y) in enumerate(zip(line(24, 16), lab_own(first))):
            labs[end, j, beyond : beyond + 16, :] = x.astype(jnp.int32)
            labs[end, j, mine : mine + 8, :] = y
        near = lambda at: [labs[end, j, at : at + 8, :] for j in range(tiles)]
        *halo, rhs = decode_row(
            lane, [x.astype(jnp.int32) for x in line(0)], near(8), near(9), near(7), line(8), line(16)
        )
        if end == 0:
            add = [jnp.where((sub == 0) & (x == 1) & (c > 0.0), 1.0, 0.0) for x, c in zip(near(15), own(eu_t, 0))]
        else:
            add = [jnp.where((sub == 7) & (x == 1) & (c > 0.0), 1.0, 0.0) for x, c in zip(near(1), own(ed_t, first))]
        outer = [x + y for x, y in zip(own(field[0], first), add)]
        step = 8 if end == 0 else -8
        next_in = own(field[0], first + step)
        coefficient = [[own(ref, f) for ref in (er_t, ed_t, eu_t, diag_t)] for f in (first, first + step)]
        trio = [(halo, rhs), (coefficient[0], outer), (coefficient[1], next_in)]
        if end == 1:
            trio.reverse()
        terms.append([t[0] for t in trio])
        for q, (_, start) in enumerate(trio):
            for j in range(tiles):
                grid[end, 0, j, 8 + 8 * q : 16 + 8 * q, :] = start[j]
        guard, inside, take = (0, 32, 16) if end == 0 else (32, 0, rows - 24)
        for k in range(ITERS):
            for j in range(tiles):
                grid[end, k, j, guard : guard + 8, :] = zero
                grid[end, k, j, inside : inside + 8, :] = field[k][j, take : take + 8, :]

    parts = [sums[q] for q in range(2 * ITERS + 1)]
    for k in range(ITERS):
        for end in range(2):
            at = lambda kk, s: [grid[end, kk, j, s : s + 8, :] for j in range(tiles)]
            for q in range(3):
                s = 8 + 8 * q
                v = at(k, s)
                new = recurrence(
                    lane, k, v, at(k, s + 1), at(k, s - 1), at(k - 1, s) if k else None, *terms[end][q]
                )
                for j in range(tiles):
                    grid[end, k + 1, j, s : s + 8, :] = new[j]
                mine = q - 1 if end == 0 else q
                if 0 <= mine < 2:
                    v, new = v[:inner], new[:inner]
                    parts[2 * k] = parts[2 * k] + summed(v, v)
                    parts[2 * k + 1] = parts[2 * k + 1] + summed(v, new)
                    for j in range(inner):
                        edge[k, end, j, 8 * mine : 8 * mine + 8, :] = v[j]
                    if k == ITERS - 1:
                        parts[2 * k + 2] = parts[2 * k + 2] + summed(new, new)
                        for j in range(inner):
                            edge[k + 1, end, j, 8 * mine : 8 * mine + 8, :] = new[j]

    every = jnp.zeros((1, LANES), jnp.float32)
    for q, acc in enumerate(parts):
        one = jnp.sum(jnp.sum(acc, axis=0, keepdims=True), axis=1, keepdims=True)
        every = jnp.where(lane_ids(1) == q, one, every)
    out[...] = jnp.broadcast_to(every[None], out.shape)


def coefficients(dots):
    n = ITERS
    inv = 1.0 / dots[0]
    moment = [jnp.ones_like(dots[0]), dots[1] * inv]
    for k in range(1, n + 1):
        moment.append(2.0 * (dots[2 * k] * inv) - moment[0])
        if k < n:
            moment.append(2.0 * (dots[2 * k + 1] * inv) - moment[1])
    gram = [[0.5 * (moment[i + j] + moment[abs(i - j)]) for j in range(n + 1)] for i in range(n + 1)]

    def image(p):
        q = [CENTRE * x for x in p] + [jnp.zeros_like(p[0])]
        for i, x in enumerate(p):
            if i == 0:
                q[1] = q[1] + RADIUS * x
            else:
                q[i + 1] = q[i + 1] + (RADIUS / 2) * x
                q[i - 1] = q[i - 1] + (RADIUS / 2) * x
        return q

    def product(a, b):
        sums = None
        for i, x in enumerate(a):
            t = gram[i][0] * b[0]
            for j in range(1, len(b)):
                t = t + gram[i][j] * b[j]
            sums = x * t if sums is None else sums + x * t
        return sums

    zero = jnp.zeros_like(inv)
    x, r, p = [], [moment[0]], [moment[0]]
    now = moment[0]
    for _ in range(n):
        q = image(p)
        alpha = now / product(p, q)
        x = [(x[i] if i < len(x) else zero) + alpha * p[i] for i in range(len(p))]
        r = [(r[i] if i < len(r) else zero) - alpha * q[i] for i in range(len(q))]
        following = product(r, r)
        beta = following / now
        p = [r[i] + (beta * p[i] if i < len(p) else zero) for i in range(len(r))]
        now = following
    size = zero
    for i in range(n + 1):
        size = size + jnp.abs(r[i]) * jnp.sqrt(jnp.maximum(gram[i][i], 0.0))
    good = (size * size <= (AMPLIFICATION * AMPLIFICATION) * now) & (now > 0.0)
    return x, r, good


def combine(every, lab_t, edge, *refs):
    n = ITERS + 1
    field, (labeling, residual, flag, sol_s, res_s, sem) = refs[:n], refs[n:]
    inner, rows = lab_t.shape[0], lab_t.shape[1] - 2 * HALO
    g = jnp.sum(every[:, 0, :], axis=0, keepdims=True)
    dots = [jnp.broadcast_to(g[:, q : q + 1], (8, LANES)) for q in range(2 * ITERS + 1)]
    x, r, good = coefficients(dots)
    flag[0, 0] = jnp.min(good.astype(jnp.int32))

    def put(s, source):
        for j in range(inner):
            lanes = slice(j * LANES, (j + 1) * LANES)
            sol = jnp.where(lab_t[j, pl.ds(s + HALO, 8), :] == 1, 1.0, 0.0)
            res = None
            for k in range(n):
                t = source(k, j)
                res = r[k] * t if res is None else res + r[k] * t
                if k < ITERS:
                    sol = sol + x[k] * t
            sol_s[pl.ds(s, 8), lanes] = sol
            res_s[pl.ds(s, 8), lanes] = res

    def body(i, _):
        s = pl.multiple_of(8 * i, 8)
        put(s, lambda k, j: field[k][j, pl.ds(s, 8), :])
        return 0

    copies = []
    chunk = 128
    for c in range(rows // chunk):
        first, last = c * chunk // 8, (c + 1) * chunk // 8
        if c == 0:
            for q in range(2):
                put(8 * q, lambda k, j: edge[k, 0, j, 8 * q : 8 * q + 8, :])
            first += 2
        if (c + 1) * chunk == rows:
            last -= 2
        lax.fori_loop(first, last, body, 0, unroll=(last - first) // 2)
        if (c + 1) * chunk == rows:
            for q in range(2):
                put(rows - 16 + 8 * q, lambda k, j: edge[k, 1, j, 8 * q : 8 * q + 8, :])
        at = pl.ds(c * chunk, chunk)
        for q, (src, dst) in enumerate(((sol_s, labeling), (res_s, residual))):
            copy = pltpu.make_async_copy(src.at[at, :], dst.at[0, at, :], sem.at[c, q])
            copy.start()
            copies.append(copy)
    for copy in copies:
        copy.wait()


def swaps(axis, first, second, around):
    count = lax.axis_size(axis)
    pairs = [(i, i + 1) for i in range(0, count - 1, 2)]
    others = [(i, i + 1) for i in range(1, count - 1, 2)] + ([(count - 1, 0)] if around else [])
    both = lambda p: [(a, b) for a, b in p] + [(b, a) for a, b in p]
    return lax.ppermute(first, axis, both(pairs)), lax.ppermute(second, axis, both(others))


def call(body, in_specs, outs, scratch, mib, flops, operands, out_specs=None, aliases={}):
    return pl.pallas_call(
        body,
        in_specs=in_specs,
        out_specs=out_specs or [VMEM] * len(outs),
        out_shape=outs,
        scratch_shapes=scratch,
        input_output_aliases=aliases,
        compiler_params=pltpu.CompilerParams(vmem_limit_bytes=mib * 1024 * 1024),
        cost_estimate=pl.CostEstimate(flops=flops, bytes_accessed=1 << 20, transcendentals=0),
    )(*operands)


def per_device(edges, labels, prior, data_weight):
    arrays = (edges, labels, prior, data_weight)
    _, rows, cols = edges.shape
    f32, i32 = jnp.float32, jnp.int32
    shape = jax.ShapeDtypeStruct
    inner = cols // LANES
    tiles = inner + 1
    dma = pltpu.SemaphoreType.DMA

    *col_messages, lab_t = call(
        col_pack, [HBM] * 4,
        [shape((LINES, rows), f32)] * 2 + [shape((inner, rows + 2 * HALO, LANES), i32)],
        [
            pltpu.VMEM((2, rows, LANES), i32),
            pltpu.VMEM((2, 2, rows, LANES), f32),
            dma((6 + inner,)),
        ],
        6, 1 << 20, arrays,
    )
    col_first, col_second = swaps("col", *col_messages, True)

    n = ITERS + 1
    whole = shape((tiles, rows + SPARE, LANES), f32)
    terms = call(
        prepare, [VMEM] * 4, [whole] * 5, [], 6, 1 << 24, (edges, lab_t, prior, data_weight),
    )
    row_messages = call(
        row_pack, [VMEM] * 7, [shape((LINES, tiles * LANES), f32)] * 2, [],
        4, 1 << 20, (edges, lab_t, prior, data_weight, col_first, col_second, terms[1]),
    )
    row_first, row_second = swaps("row", *row_messages, False)

    out = call(
        interior, [VMEM] * 9,
        [whole] * (4 + n)
        + [shape((rows + 2 * HALO, LANES), i32), shape((2 * ITERS + 1, 8, LANES), f32)],
        [pltpu.VMEM((rows, LANES), i32), pltpu.VMEM((rows, LANES), f32), pltpu.VMEM((rows, LANES), f32)],
        16, 1 << 26, (edges, lab_t, col_first, col_second, *terms),
        aliases={4 + q: q for q in range(5)},
    )
    terms, field, side_lab, sums = out[:4], out[4 : 4 + n], out[4 + n], out[5 + n]
    group = lax.axis_size(("row", "col"))
    sums, edge = call(
        band, [VMEM] * (ITERS + 9),
        [shape((group, 1, LANES), f32), shape((n, 2, inner, 2 * HALO, LANES), f32)],
        [pltpu.VMEM((2, tiles, 24, LANES), i32), pltpu.VMEM((2, n, tiles, 40, LANES), f32)],
        6, 1 << 20, (*field[:ITERS], *terms, lab_t, side_lab, sums, row_first, row_second),
    )
    every = lax.all_to_all(sums, ("row", "col"), 0, 0, tiled=True)

    labeling, residual, flag = call(
        combine, [VMEM] * (n + 3),
        [shape(edges.shape, f32)] * 2 + [shape((1, 1), i32)],
        [pltpu.VMEM((rows, cols), f32)] * 2 + [dma((rows // 128, 2))],
        4, 1 << 20, (every, lab_t, edge, *field), out_specs=[ANY, ANY, pl.BlockSpec(memory_space=pltpu.SMEM)],
    )

    def again(carry):
        return (jnp.int32(1), *plain(edges, labels, prior, data_weight))

    _, labeling, residual = lax.while_loop(
        lambda carry: carry[0] == 0, again, (flag[0, 0], labeling, residual)
    )
    return labeling, residual


def solution(mesh):
    spec = P("img", "row", "col")
    return jax.shard_map(
        per_device, mesh=mesh, in_specs=(spec,) * 4, out_specs=(spec,) * 2, check_vma=False
    )
```

```python
import functools
import jax
import jax.numpy as jnp
from jax import lax
from jax.experimental import pallas as pl
from jax.experimental.pallas import tpu as pltpu
from jax.sharding import PartitionSpec as P

ITERS = 8
HALO = 8
LANES = 128
LOW, HIGH = 0.05, 7.5
CENTRE, RADIUS = (HIGH + LOW) / 2, (HIGH - LOW) / 2
AMPLIFICATION = 24.0
VMEM = pl.BlockSpec(memory_space=pltpu.VMEM)
ANY = pl.BlockSpec(memory_space=pl.ANY)
HBM = pl.BlockSpec(memory_space=pltpu.HBM)


def with_halo(array, sides, width):
    edges = {}
    for axis, dim in sides:
        count, length = (lax.axis_size(axis), array.shape[dim])
        up = [(i, (i + 1) % count) for i in range(count - 1)]
        last = lax.slice_in_dim(array, length - width, length, axis=dim)
        first = lax.slice_in_dim(array, 0, width, axis=dim)
        edges[dim] = (
            lax.ppermute(last, axis, up),
            lax.ppermute(first, axis, [(b, a) for a, b in up]),
        )
    done = []
    for _, dim in sides:
        low, high = edges[dim]
        around = [(width, width) if d in done else (0, 0) for d in range(array.ndim)]
        array = jnp.concatenate([jnp.pad(low, around), array, jnp.pad(high, around)], axis=dim)
        done.append(dim)
    return array


def total(value, axis):
    count = lax.axis_size(axis)
    flat = value.reshape(1, 1, 1)
    every = lax.all_to_all(jnp.broadcast_to(flat, (count, 1, 1)), axis, 0, 0, tiled=True)
    return every.sum()


def neighbours(field, right, left, down, upper):
    padded = with_halo(field, (("row", 1), ("col", 2)), 1)
    return (
        right * padded[:, 1:-1, 2:]
        + left * padded[:, 1:-1, :-2]
        + down * padded[:, 2:, 1:-1]
        + upper * padded[:, :-2, 1:-1]
    )


def plain(edges, labels, prior, data_weight):
    right = (edges % 2).astype(jnp.float32)
    left = (edges // 2 % 2).astype(jnp.float32)
    down = (edges // 4 % 2).astype(jnp.float32)
    upper = (edges // 8 % 2).astype(jnp.float32)
    degree = right + left + down + upper
    free = (labels == 0).astype(jnp.float32)
    anchor = (labels == 1).astype(jnp.float32)
    diag_term = degree + data_weight

    def nearby(field):
        return neighbours(field, right, left, down, upper)

    rhs = free * (data_weight * prior + nearby(anchor))

    def step(_, carry):
        result, residual, direction, norm_now = carry
        image_v = free * (diag_term * direction - nearby(direction))
        alpha = norm_now / total(jnp.sum(direction * image_v), ("row", "col"))
        result = result + alpha * direction
        residual = residual - alpha * image_v
        norm_next = total(jnp.sum(residual * residual), ("row", "col"))
        direction = residual + (norm_next / norm_now) * direction
        return result, residual, direction, norm_next

    start = (jnp.zeros_like(rhs), rhs, rhs, total(jnp.sum(rhs * rhs), ("row", "col")))
    result, residual, _, _ = lax.fori_loop(0, ITERS, step, start)
    return anchor + result, residual


WIDTH = HALO + 1
LINES = 40
SLOTS = ((0, 0, 8), (2, 8, 8), (3, 16, 8), (1, 24, 16))


def lane_ids(rows):
    return lax.broadcasted_iota(jnp.int32, (rows, LANES), 1)


def turn(x, by):
    return pltpu.roll(x, by % LANES, 1) if by % LANES else x


def col_pack(edges, labels, prior, weight, first, second, lab_t, ints, floats, sem):
    rows, cols = edges.shape[1], edges.shape[2]
    tiles = cols // LANES
    lane = lane_ids(LANES)
    pairs = []
    for side in range(2):
        at = pl.ds(side * (cols - LANES), LANES)
        pairs.append((edges.at[0, :, at], ints.at[side]))
        pairs.append((prior.at[0, :, at], floats.at[side, 0]))
        pairs.append((weight.at[0, :, at], floats.at[side, 1]))
    for j in (0, tiles - 1, *range(1, tiles - 1)):
        pairs.append((labels.at[0, :, pl.ds(j * LANES, LANES)], lab_t.at[j, pl.ds(HALO, rows), :]))
    copies = [pltpu.make_async_copy(*pair, sem.at[q]) for q, pair in enumerate(pairs)]
    for copy in copies:
        copy.start()
    seeds = jnp.full((HALO, LANES), 2, jnp.int32)
    for j in range(tiles):
        lab_t[j, :HALO, :] = seeds
        lab_t[j, HALO + rows :, :] = seeds
    for copy in copies[:8]:
        copy.wait()
    for chunk in range(rows // LANES):
        at = slice(chunk * LANES, (chunk + 1) * LANES)
        lines = []
        for side in range(2):
            labs = lab_t[side * (tiles - 1), HALO + chunk * LANES : HALO + (chunk + 1) * LANES, :]
            packed = None
            for x, (_, line, n) in zip((ints[side, at, :], floats[side, 0, at, :], floats[side, 1, at, :], labs), SLOTS):
                x = turn(x.astype(jnp.float32), line + side * n)
                packed = x if packed is None else jnp.where(lane < line, packed, x)
            lines.append(jnp.swapaxes(packed, 0, 1)[:LINES])
        first[:, at], second[:, at] = ordered("col", *lines)
    for copy in copies[8:]:
        copy.wait()


def ordered(axis, before, after):
    even = lax.axis_index(axis) % 2 == 0
    return jnp.where(even, after, before), jnp.where(even, before, after)


def side_tiles(first, second, at):
    right, left = ordered("col", second[:, at : at + LANES], first[:, at : at + LANES])
    both = []
    for _, line, n in SLOTS:
        both += [left[line : line + n], right[line : line + n]]
    both.append(jnp.zeros((LANES - 2 * LINES, LANES), jnp.float32))
    both = jnp.swapaxes(jnp.concatenate(both, 0), 0, 1)
    lane = lane_ids(LANES)
    tiles = {}
    for a, line, n in SLOTS:
        width, outside = (WIDTH, 2.0) if a == 1 else (HALO, 0.0)
        inside = (lane < width) | (lane >= LANES - width)
        tiles[a] = jnp.where(inside, turn(both, -(2 * line + n)), outside)
    return tiles


def row_pack(edges, lab_t, prior, weight, col_first, col_second, after, first, second):
    del after
    rows, cols = edges.shape[1], edges.shape[2]
    tiles = cols // LANES
    refs = (edges, None, prior, weight)
    top = side_tiles(col_first, col_second, 0)
    bottom = side_tiles(col_first, col_second, rows - LANES)
    for a, line, n in SLOTS:
        here = slice(line, line + n)
        for j in range(tiles):
            lanes = slice(j * LANES, (j + 1) * LANES)
            if a == 1:
                up, low = lab_t[j, HALO : HALO + n, :], lab_t[j, HALO + rows - n : HALO + rows, :]
            else:
                up, low = refs[a][0, :n, lanes], refs[a][0, rows - n :, lanes]
            up, low = up.astype(jnp.float32), low.astype(jnp.float32)
            first[here, lanes], second[here, lanes] = ordered("row", up, low)
        lanes = slice(tiles * LANES, (tiles + 1) * LANES)
        first[here, lanes], second[here, lanes] = ordered("row", top[a][:n], bottom[a][LANES - n :])


def shifted(tiles, lane, by):
    count = len(tiles)
    turned = [turn(t, by) for t in tiles]
    if by > 0:
        return [jnp.where(lane == 0, turned[j - 1], turned[j]) for j in range(count)]
    return [jnp.where(lane == LANES - 1, turned[(j + 1) % count], turned[j]) for j in range(count)]


SCALE = 2.0 / RADIUS
SPARE = 24


def decode(code, lab, lab_r, lab_l, lab_d, lab_u, prior, weight):
    r = (code & 1).astype(jnp.float32)
    l = ((code >> 1) & 1).astype(jnp.float32)
    d = ((code >> 2) & 1).astype(jnp.float32)
    u = ((code >> 3) & 1).astype(jnp.float32)
    free = lab == 0
    one = jnp.where(free, SCALE, 0.0)
    near = (
        jnp.where(lab_r == 1, r, 0.0)
        + jnp.where(lab_l == 1, l, 0.0)
        + jnp.where(lab_d == 1, d, 0.0)
        + jnp.where(lab_u == 1, u, 0.0)
    )
    return (
        jnp.where(lab_r == 0, one, 0.0) * r,
        one * d,
        one * u,
        SCALE * ((r + l + d + u) + weight - CENTRE),
        jnp.where(free, weight * prior + near, 0.0),
    )


def decode_row(lane, code, lab, lab_d, lab_u, prior, weight):
    lab_r, lab_l = shifted(lab, lane, -1), shifted(lab, lane, 1)
    return list(zip(*map(decode, code, lab, lab_r, lab_l, lab_d, lab_u, prior, weight)))


def prepare(edges, lab_t, prior, weight, *terms):
    rows, cols = edges.shape[1], edges.shape[2]
    tiles = cols // LANES
    lane = lane_ids(8)
    seeds = jnp.full((8, LANES), 2, jnp.int32)

    def body(i, _):
        s = pl.multiple_of(8 * i, 8)
        read = lambda ref: [ref[0, pl.ds(s, 8), j * LANES : (j + 1) * LANES] for j in range(tiles)]
        near = lambda at: [lab_t[j, pl.ds(at, 8), :] for j in range(tiles)]
        lab = near(pl.multiple_of(s + HALO, 8))
        lab_r, lab_l = (shifted(lab + [seeds], lane, by)[:tiles] for by in (-1, 1))
        done = map(
            decode, read(edges), lab, lab_r, lab_l, near(s + HALO + 1), near(s + HALO - 1),
            read(prior), read(weight),
        )
        for j, values in enumerate(done):
            for ref, value in zip(terms, values):
                ref[j, pl.ds(s, 8), :] = value
        return 0

    lax.fori_loop(0, rows // 8, body, 0, unroll=8)


def recurrence(lane, k, v, v_d, v_u, before, er, ed, eu, diag):
    v_r = shifted(v, lane, -1)
    g = shifted([er[j] * v[j] for j in range(len(v))], lane, 1)
    new = []
    for j in range(len(v)):
        x = diag[j] * v[j] - (er[j] * v_r[j] + g[j])
        x = x - (ed[j] * v_d[j] + eu[j] * v_u[j])
        new.append(0.5 * x if k == 0 else x - before[j])
    return new


def summed(a, b):
    t = [x * y for x, y in zip(a, b)]
    while len(t) > 1:
        t = [t[q] + t[q + 1] for q in range(0, len(t) - 1, 2)] + ([t[-1]] if len(t) % 2 else [])
    return t[0]


def interior(edges, lab_t, col_first, col_second, *refs):
    refs = refs[5:]
    (er_t, ed_t, eu_t, diag_t), field, side_lab, sums = refs[:4], refs[4:13], refs[13], refs[14]
    side_code, side_prior, side_weight = refs[15:]
    rows = edges.shape[1]
    inner = lab_t.shape[0]
    tiles = inner + 1
    lane = lane_ids(8)
    for at in range(0, rows, LANES):
        side = side_tiles(col_first, col_second, at)
        side_code[at : at + LANES, :] = side[0].astype(jnp.int32)
        side_lab[HALO + at : HALO + at + LANES, :] = side[1].astype(jnp.int32)
        side_prior[at : at + LANES, :] = side[2]
        side_weight[at : at + LANES, :] = side[3]
    seeds = jnp.full((HALO, LANES), 2, jnp.int32)
    side_lab[:HALO, :] = seeds
    side_lab[HALO + rows :, :] = seeds
    zero = jnp.zeros((8, LANES), jnp.float32)
    for k in range(1, ITERS):
        for j in range(tiles):
            field[k][j, :8, :] = zero
            field[k][j, rows - 8 : rows, :] = zero
    end = inner - 1

    def sides(i, _):
        s = pl.multiple_of(8 * i, 8)
        here, there = pl.ds(s, 8), pl.ds(pl.multiple_of(s + HALO, 8), 8)
        lab, lab_0, lab_end = side_lab[there, :], lab_t[0, there, :], lab_t[end, there, :]
        lab_r, lab_l = turn(lab, -1), turn(lab, 1)
        values = decode(
            side_code[here, :], lab,
            jnp.where(lane == LANES - 1, turn(lab_0, -1), lab_r),
            jnp.where(lane == 0, turn(lab_end, 1), lab_l),
            side_lab[pl.ds(s + HALO + 1, 8), :], side_lab[pl.ds(s + HALO - 1, 8), :],
            side_prior[here, :], side_weight[here, :],
        )
        for ref, value in zip((er_t, ed_t, eu_t, diag_t, field[0]), values):
            ref[inner, here, :] = value
        left = (lane == 0) & (lab_0 == 0) & ((edges[0, here, :LANES] & 2) != 0)
        field[0][0, here, :] += jnp.where(left & (lab_l == 1), 1.0, 0.0)
        right = (lane == LANES - 1) & (lab_end == 0) & ((edges[0, here, end * LANES :] & 1) != 0)
        field[0][end, here, :] += jnp.where(right & (lab_r == 1), 1.0, 0.0)
        er_t[end, here, :] += jnp.where(right & (lab_r == 0), SCALE, 0.0)
        return 0

    lax.fori_loop(0, rows // 8, sides, 0, unroll=16)

    def at_rows(ref, s):
        return [ref[j, pl.ds(s, 8), :] for j in range(tiles)]

    def advance(k, s):
        v = at_rows(field[k], s)
        new = recurrence(
            lane, k, v, at_rows(field[k], s + 1), at_rows(field[k], s - 1),
            at_rows(field[k - 1], s) if k else None,
            at_rows(er_t, s), at_rows(ed_t, s), at_rows(eu_t, s), at_rows(diag_t, s),
        )
        for j in range(tiles if k + 1 < ITERS else inner):
            field[k + 1][j, pl.ds(s, 8), :] = new[j]
        return v[:inner], new[:inner]

    count = 0
    for k in range(ITERS):
        last = k == ITERS - 1

        def body(i, carry, k=k, last=last):
            v, new = advance(k, pl.multiple_of(2 * HALO + 8 * i, 8))
            pairs = [(v, v), (v, new)] + ([(new, new)] if last else [])
            return tuple(acc + summed(a, b) for acc, (a, b) in zip(carry, pairs))

        if not last:
            advance(k, 8)
            advance(k, rows - 16)
        acc = (zero,) * (3 if last else 2)
        acc = lax.fori_loop(0, (rows - 4 * HALO) // 8, body, acc, unroll=60)
        for value in acc:
            sums[count] = value
            count += 1


def band(*refs):
    n = ITERS
    field, (er_t, ed_t, eu_t, diag_t, lab_t, side_lab) = refs[:n], refs[n : n + 6]
    sums, row_first, row_second = refs[n + 6 : n + 9]
    out, edge, labs, grid = refs[n + 9 :]
    inner, rows = lab_t.shape[0], lab_t.shape[1] - 2 * HALO
    tiles = inner + 1
    lane = lane_ids(8)
    sub = lax.broadcasted_iota(jnp.int32, (8, LANES), 0)
    zero = jnp.zeros((8, LANES), jnp.float32)

    def lab_own(first):
        return [lab_t[j, HALO + first : HALO + first + 8, :] for j in range(inner)] + [
            side_lab[HALO + first : HALO + first + 8, :]
        ]

    def own(ref, first):
        return [ref[j, first : first + 8, :] for j in range(tiles)]

    terms = []
    for end, first in enumerate((0, rows - 8)):
        def line(at, count=8, end=end):
            both = [
                ordered("row", row_second[at : at + count, lanes], row_first[at : at + count, lanes])
                for lanes in (slice(j * LANES, (j + 1) * LANES) for j in range(tiles))
            ]
            return [pair[1 - end] for pair in both]

        beyond, mine = (0, 16) if end == 0 else (8, 0)
        for j, (x, y) in enumerate(zip(line(24, 16), lab_own(first))):
            labs[end, j, beyond : beyond + 16, :] = x.astype(jnp.int32)
            labs[end, j, mine : mine + 8, :] = y
        near = lambda at: [labs[end, j, at : at + 8, :] for j in range(tiles)]
        *halo, rhs = decode_row(
            lane, [x.astype(jnp.int32) for x in line(0)], near(8), near(9), near(7), line(8), line(16)
        )
        if end == 0:
            add = [jnp.where((sub == 0) & (x == 1) & (c > 0.0), 1.0, 0.0) for x, c in zip(near(15), own(eu_t, 0))]
        else:
            add = [jnp.where((sub == 7) & (x == 1) & (c > 0.0), 1.0, 0.0) for x, c in zip(near(1), own(ed_t, first))]
        outer = [x + y for x, y in zip(own(field[0], first), add)]
        step = 8 if end == 0 else -8
        next_in = own(field[0], first + step)
        coefficient = [[own(ref, f) for ref in (er_t, ed_t, eu_t, diag_t)] for f in (first, first + step)]
        trio = [(halo, rhs), (coefficient[0], outer), (coefficient[1], next_in)]
        if end == 1:
            trio.reverse()
        terms.append([t[0] for t in trio])
        for q, (_, start) in enumerate(trio):
            for j in range(tiles):
                grid[end, 0, j, 8 + 8 * q : 16 + 8 * q, :] = start[j]
        guard, inside, take = (0, 32, 16) if end == 0 else (32, 0, rows - 24)
        for k in range(ITERS):
            for j in range(tiles):
                grid[end, k, j, guard : guard + 8, :] = zero
                grid[end, k, j, inside : inside + 8, :] = field[k][j, take : take + 8, :]

    parts = [sums[q] for q in range(2 * ITERS + 1)]
    for k in range(ITERS):
        for end in range(2):
            at = lambda kk, s: [grid[end, kk, j, s : s + 8, :] for j in range(tiles)]
            for q in range(3):
                s = 8 + 8 * q
                v = at(k, s)
                new = recurrence(
                    lane, k, v, at(k, s + 1), at(k, s - 1), at(k - 1, s) if k else None, *terms[end][q]
                )
                for j in range(tiles):
                    grid[end, k + 1, j, s : s + 8, :] = new[j]
                mine = q - 1 if end == 0 else q
                if 0 <= mine < 2:
                    v, new = v[:inner], new[:inner]
                    parts[2 * k] = parts[2 * k] + summed(v, v)
                    parts[2 * k + 1] = parts[2 * k + 1] + summed(v, new)
                    for j in range(inner):
                        edge[k, end, j, 8 * mine : 8 * mine + 8, :] = v[j]
                    if k == ITERS - 1:
                        parts[2 * k + 2] = parts[2 * k + 2] + summed(new, new)
                        for j in range(inner):
                            edge[k + 1, end, j, 8 * mine : 8 * mine + 8, :] = new[j]

    every = jnp.zeros((1, LANES), jnp.float32)
    for q, acc in enumerate(parts):
        one = jnp.sum(jnp.sum(acc, axis=0, keepdims=True), axis=1, keepdims=True)
        every = jnp.where(lane_ids(1) == q, one, every)
    out[...] = jnp.broadcast_to(every[None], out.shape)


def coefficients(dots):
    n = ITERS
    inv = 1.0 / dots[0]
    moment = [jnp.ones_like(dots[0]), dots[1] * inv]
    for k in range(1, n + 1):
        moment.append(2.0 * (dots[2 * k] * inv) - moment[0])
        if k < n:
            moment.append(2.0 * (dots[2 * k + 1] * inv) - moment[1])
    gram = [[0.5 * (moment[i + j] + moment[abs(i - j)]) for j in range(n + 1)] for i in range(n + 1)]

    def image(p):
        q = [CENTRE * x for x in p] + [jnp.zeros_like(p[0])]
        for i, x in enumerate(p):
            if i == 0:
                q[1] = q[1] + RADIUS * x
            else:
                q[i + 1] = q[i + 1] + (RADIUS / 2) * x
                q[i - 1] = q[i - 1] + (RADIUS / 2) * x
        return q

    def product(a, b):
        sums = None
        for i, x in enumerate(a):
            t = gram[i][0] * b[0]
            for j in range(1, len(b)):
                t = t + gram[i][j] * b[j]
            sums = x * t if sums is None else sums + x * t
        return sums

    zero = jnp.zeros_like(inv)
    x, r, p = [], [moment[0]], [moment[0]]
    now = moment[0]
    for _ in range(n):
        q = image(p)
        alpha = now / product(p, q)
        x = [(x[i] if i < len(x) else zero) + alpha * p[i] for i in range(len(p))]
        r = [(r[i] if i < len(r) else zero) - alpha * q[i] for i in range(len(q))]
        following = product(r, r)
        beta = following / now
        p = [r[i] + (beta * p[i] if i < len(p) else zero) for i in range(len(r))]
        now = following
    size = zero
    for i in range(n + 1):
        size = size + jnp.abs(r[i]) * jnp.sqrt(jnp.maximum(gram[i][i], 0.0))
    good = (size * size <= (AMPLIFICATION * AMPLIFICATION) * now) & (now > 0.0)
    return x, r, good


def combine(every, lab_t, edge, *refs):
    n = ITERS + 1
    field, (labeling, residual, flag, sol_s, res_s, sem) = refs[:n], refs[n:]
    inner, rows = lab_t.shape[0], lab_t.shape[1] - 2 * HALO
    g = jnp.sum(every[:, 0, :], axis=0, keepdims=True)
    dots = [jnp.broadcast_to(g[:, q : q + 1], (8, LANES)) for q in range(2 * ITERS + 1)]
    x, r, good = coefficients(dots)
    flag[0, 0] = jnp.min(good.astype(jnp.int32))

    def put(s, source):
        for j in range(inner):
            lanes = slice(j * LANES, (j + 1) * LANES)
            sol = jnp.where(lab_t[j, pl.ds(s + HALO, 8), :] == 1, 1.0, 0.0)
            res = None
            for k in range(n):
                t = source(k, j)
                res = r[k] * t if res is None else res + r[k] * t
                if k < ITERS:
                    sol = sol + x[k] * t
            sol_s[pl.ds(s, 8), lanes] = sol
            res_s[pl.ds(s, 8), lanes] = res

    def body(i, _):
        s = pl.multiple_of(8 * i, 8)
        put(s, lambda k, j: field[k][j, pl.ds(s, 8), :])
        return 0

    copies = []
    chunk = 128
    for c in range(rows // chunk):
        first, last = c * chunk // 8, (c + 1) * chunk // 8
        if c == 0:
            for q in range(2):
                put(8 * q, lambda k, j: edge[k, 0, j, 8 * q : 8 * q + 8, :])
            first += 2
        if (c + 1) * chunk == rows:
            last -= 2
        lax.fori_loop(first, last, body, 0, unroll=(last - first) // 2)
        if (c + 1) * chunk == rows:
            for q in range(2):
                put(rows - 16 + 8 * q, lambda k, j: edge[k, 1, j, 8 * q : 8 * q + 8, :])
        at = pl.ds(c * chunk, chunk)
        for q, (src, dst) in enumerate(((sol_s, labeling), (res_s, residual))):
            copy = pltpu.make_async_copy(src.at[at, :], dst.at[0, at, :], sem.at[c, q])
            copy.start()
            copies.append(copy)
    for copy in copies:
        copy.wait()


def swaps(axis, first, second, around):
    count = lax.axis_size(axis)
    pairs = [(i, i + 1) for i in range(0, count - 1, 2)]
    others = [(i, i + 1) for i in range(1, count - 1, 2)] + ([(count - 1, 0)] if around else [])
    both = lambda p: [(a, b) for a, b in p] + [(b, a) for a, b in p]
    return lax.ppermute(first, axis, both(pairs)), lax.ppermute(second, axis, both(others))


def call(body, in_specs, outs, scratch, mib, flops, operands, out_specs=None, aliases={}):
    return pl.pallas_call(
        body,
        in_specs=in_specs,
        out_specs=out_specs or [VMEM] * len(outs),
        out_shape=outs,
        scratch_shapes=scratch,
        input_output_aliases=aliases,
        compiler_params=pltpu.CompilerParams(vmem_limit_bytes=mib * 1024 * 1024),
        cost_estimate=pl.CostEstimate(flops=flops, bytes_accessed=1 << 20, transcendentals=0),
    )(*operands)


def per_device(edges, labels, prior, data_weight):
    arrays = (edges, labels, prior, data_weight)
    _, rows, cols = edges.shape
    f32, i32 = jnp.float32, jnp.int32
    shape = jax.ShapeDtypeStruct
    inner = cols // LANES
    tiles = inner + 1
    dma = pltpu.SemaphoreType.DMA

    *col_messages, lab_t = call(
        col_pack, [HBM] * 4,
        [shape((LINES, rows), f32)] * 2 + [shape((inner, rows + 2 * HALO, LANES), i32)],
        [
            pltpu.VMEM((2, rows, LANES), i32),
            pltpu.VMEM((2, 2, rows, LANES), f32),
            dma((6 + inner,)),
        ],
        6, 1 << 20, arrays,
    )
    col_first, col_second = swaps("col", *col_messages, True)

    n = ITERS + 1
    whole = shape((tiles, rows + SPARE, LANES), f32)
    terms = call(
        prepare, [VMEM] * 4, [whole] * 5, [], 6, 1 << 24, (edges, lab_t, prior, data_weight),
    )
    row_messages = call(
        row_pack, [VMEM] * 7, [shape((LINES, tiles * LANES), f32)] * 2, [],
        4, 1 << 20, (edges, lab_t, prior, data_weight, col_first, col_second, terms[1]),
    )
    row_first, row_second = swaps("row", *row_messages, False)

    out = call(
        interior, [VMEM] * 9,
        [whole] * (4 + n)
        + [shape((rows + 2 * HALO, LANES), i32), shape((2 * ITERS + 1, 8, LANES), f32)],
        [pltpu.VMEM((rows, LANES), i32), pltpu.VMEM((rows, LANES), f32), pltpu.VMEM((rows, LANES), f32)],
        16, 1 << 26, (edges, lab_t, col_first, col_second, *terms),
        aliases={4 + q: q for q in range(5)},
    )
    terms, field, side_lab, sums = out[:4], out[4 : 4 + n], out[4 + n], out[5 + n]
    group = lax.axis_size(("row", "col"))
    sums, edge = call(
        band, [VMEM] * (ITERS + 9),
        [shape((group, 1, LANES), f32), shape((n, 2, inner, 2 * HALO, LANES), f32)],
        [pltpu.VMEM((2, tiles, 24, LANES), i32), pltpu.VMEM((2, n, tiles, 40, LANES), f32)],
        6, 1 << 20, (*field[:ITERS], *terms, lab_t, side_lab, sums, row_first, row_second),
    )
    every = lax.all_to_all(sums, ("row", "col"), 0, 0, tiled=True)

    labeling, residual, flag = call(
        combine, [VMEM] * (n + 3),
        [shape(edges.shape, f32)] * 2 + [shape((1, 1), i32)],
        [pltpu.VMEM((rows, cols), f32)] * 2 + [dma((rows // 128, 2))],
        4, 1 << 20, (every, lab_t, edge, *field), out_specs=[ANY, ANY, pl.BlockSpec(memory_space=pltpu.SMEM)],
    )

    def again(carry):
        return (jnp.int32(1), *plain(edges, labels, prior, data_weight))

    _, labeling, residual = lax.while_loop(
        lambda carry: carry[0] == 0, again, (flag[0, 0], labeling, residual)
    )
    return labeling, residual


def solution(mesh):
    spec = P("img", "row", "col")
    return jax.shard_map(
        per_device, mesh=mesh, in_specs=(spec,) * 4, out_specs=(spec,) * 2, check_vma=False
    )
```
